128 devices in a mesh: tm: 8 (over y, z_hi), sky: 16 (over x, z_lo, core).
Axes of the slice: x: 4, y: 4, z: 4 (z_hi: 2, z_lo: 2; z = z_hi * 2 + z_lo), core: 2. Of those that a mesh axis runs over, the one named last changes fastest.
Arguments:
- residual: float32 [65536, 128], P(('tm', 'sky')), may hold values from -110 to 110
- obs_weight: float32 [65536, 128], P(('tm', 'sky')), may hold values from 0.5 to 2
- source_partials: float32 [5, 65536, 128], P(None, ('tm', 'sky')), may hold values from -1 to 1
- attitude_partials: float32 [16, 65536, 128], P(None, ('tm', 'sky')), may hold values from -1.5 to 1.5
- source_index: int32 [65536, 128], P(('tm', 'sky')), may hold values from 0 to 127
- tile_pixel: int32 [65536], P(('tm', 'sky')), may hold values from 0 to 2047, as said below
- tile_knot: int32 [65536], P(('tm', 'sky')), may hold values from 0 to 4095, as said below
- pixel_slot: int32 [2048], replicated, may hold values from 0 to 2047, as said below
Outputs:
- final_residual: float32 [65536, 128], P(('tm', 'sky'))
- source_update: float32 [5, 262144], P(None, 'sky')
- attitude_update: float32 [4, 4096], P(None, 'tm')
The draws below stay inside these ranges and needn't reach their ends.
Inputs may be any that keep to these rules, and one draw needn't show every extreme that they name: Tiles come in aligned blocks of 512; with owner = pixel_slot[tile_pixel[t]] // 128, no block holds more than 96 tiles of one owner, and every block holds exactly 96 tiles of some owner. `pixel_slot`: every slot number appears once. `tile_knot`: the tiles of aligned block q of 512 tiles have first knots in [q * 32, (q + 1) * 32).
All inputs are finite; a program needn't handle non-finite values.
Results may differ from the reference program's by a relative error of at most 0.0003.
Values sent between devices are 32-bit elements; how exact they have to be, the bound alone decides.
A program may use at most 128 MiB of HBM per device.

```python
import math
import jax
import jax.numpy as jnp
from jax import lax

OBS_TILE = 128
TILES_DEV = 512
PIX_DEV = 128
SRC_PIX = 128
OWNERS = 16
TIME_SHARDS = 8
CAP = 96
SPAN = 32
PIXELS = 2048
KNOTS = 4096
TILES = 65536


def sky_layout(key):
    slot_of_pixel = jax.random.permutation(jax.random.fold_in(key, 11), PIXELS).astype(jnp.int32)
    pixel_of_slot = jnp.argsort(slot_of_pixel, stable=True).astype(jnp.int32)
    blocks = TILES // TILES_DEV
    crowded_rows = jax.random.randint(jax.random.fold_in(key, 12), (TIME_SHARDS,), 0, OWNERS)
    crowded = crowded_rows[jnp.arange(blocks, dtype=jnp.int32) // OWNERS]
    positions = jnp.arange(TILES_DEV, dtype=jnp.int32)
    remaining = positions - CAP
    plain_owner = (crowded[:, None] + 1 + remaining[None, :] % (OWNERS - 1)) % OWNERS
    owner_ids = jnp.where(positions[None, :] < CAP, crowded[:, None], plain_owner)
    shuffles = jax.vmap(lambda sub: jax.random.permutation(sub, TILES_DEV))(jax.random.split(jax.random.fold_in(key, 13), blocks))
    owner_ids = jnp.take_along_axis(owner_ids, shuffles, axis=1)
    local_pixel = jax.random.randint(jax.random.fold_in(key, 14), (blocks, TILES_DEV), 0, PIX_DEV)
    pixel_ids = pixel_of_slot[(owner_ids * PIX_DEV + local_pixel).reshape(-1)]
    return (slot_of_pixel, pixel_ids.astype(jnp.int32))


def draw_pixel_slot(key, part):
    return sky_layout(key)[0]


def draw_tile_pixel(key, part):
    return sky_layout(key)[1]


def knot_starts(key):
    offset = jax.random.randint(jax.random.fold_in(key, 21), (TILES,), 0, SPAN)
    return (jnp.arange(TILES, dtype=jnp.int32) // TILES_DEV * SPAN + offset).astype(jnp.int32)


def draw_tile_knot(key, part):
    return knot_starts(key)


def attitude_parts(key):
    partials = jnp.clip(0.25 * jax.random.normal(jax.random.fold_in(key, 31), (16, TILES, OBS_TILE), jnp.float32), -1.5, 1.5)
    return partials


def draw_attitude_partials(key, part):
    return attitude_parts(key)


def draw_residual(key, part):
    partials = attitude_parts(key)
    knot_start = knot_starts(key)
    attitude_curve = jnp.clip(jax.random.normal(jax.random.fold_in(key, 32), (4, KNOTS + 3), jnp.float32), -4.0, 4.0)
    signal = jnp.clip(jax.random.normal(jax.random.fold_in(key, 33), (TILES, OBS_TILE), jnp.float32), -6.0, 6.0)
    for segment in range(4):
        values = jnp.take(attitude_curve, knot_start + segment, axis=1)
        for component in range(4):
            signal = signal + partials[4 * segment + component] * values[component][:, None]
    return signal


def with_ends(values, rng, low, high):
    shape = values.shape
    spot = [jax.random.randint(jax.random.fold_in(rng, axis), (), 0, shape[axis]) for axis in range(len(shape))]
    values = values.at[tuple(spot)].set(low)
    longest = shape.index(max(shape))
    spot[longest] = (spot[longest] + 1) % shape[longest]
    return values.at[tuple(spot)].set(high)


def shard_levels(key, extent, cuts, low, top_value):
    gain, own = 1.0, jax.random.fold_in(key, 6)
    for axis_at, blocks in cuts:
        heights = jnp.exp(jax.random.uniform(jax.random.fold_in(own, axis_at), (blocks,), jnp.float32, low / len(cuts), top_value / len(cuts)))
        gain = gain * jnp.repeat(heights, extent[axis_at] // blocks).reshape([-1 if axis == axis_at else 1 for axis in range(len(extent))])
    return gain


def centred(own_key, extent, width, reach, cuts=(), kind=jnp.bfloat16):
    values = width * jax.random.normal(own_key, extent, jnp.float32)
    if cuts:
        values = values * shard_levels(own_key, extent, cuts, -0.22, 0.18)
    return jnp.clip(values, -reach, reach).astype(kind)


def setup_inputs(seed: int = 0) -> dict:
    arg_keys = jax.random.split(jax.random.key(seed), 9)
    return {
        "residual": draw_residual(jax.random.fold_in(arg_keys[8], 71), 0),
        "obs_weight": jnp.clip(jnp.exp(math.log(2.0) - 1.3862944 * jax.random.uniform(arg_keys[1], (TILES, OBS_TILE), jnp.float32) ** shard_levels(arg_keys[1], (TILES, OBS_TILE), ((0, 128),), -0.2, 0.2)), 0.5, 2.0),
        "source_partials": centred(arg_keys[2], (5, TILES, OBS_TILE), 32 ** -0.5, 1.0, ((1, 128),), jnp.float32),
        "attitude_partials": draw_attitude_partials(jax.random.fold_in(arg_keys[8], 71), 0),
        "source_index": with_ends(jax.random.randint(arg_keys[4], (TILES, OBS_TILE), 0, SRC_PIX), jax.random.fold_in(arg_keys[4], 1), 0, SRC_PIX - 1).astype(jnp.int32),
        "tile_pixel": draw_tile_pixel(jax.random.fold_in(arg_keys[8], 71), 0),
        "tile_knot": draw_tile_knot(jax.random.fold_in(arg_keys[8], 71), 0),
        "pixel_slot": draw_pixel_slot(jax.random.fold_in(arg_keys[8], 71), 0),
    }


SOURCE_PAIRS = tuple(((first, second) for first in range(5) for second in range(first, 5)))
KNOT_PAIRS = tuple(((first, second) for first in range(4) for second in range(first, 4)))

def damped_solve(normal, target, order, pairs):
    entries = {}
    for number, couple in enumerate(pairs):
        entries[couple] = normal[number]
    factor = {}
    for column in range(order):
        pivot_value = entries[column, column] + 1.0
        for earlier in range(column):
            pivot_value = pivot_value - factor[column, earlier] * factor[column, earlier]
        pivot_value = jnp.sqrt(pivot_value)
        factor[column, column] = pivot_value
        for below in range(column + 1, order):
            current = entries[column, below]
            for earlier in range(column):
                current = current - factor[below, earlier] * factor[column, earlier]
            factor[below, column] = current / pivot_value
    forward = []
    for column in range(order):
        current = target[column]
        for earlier in range(column):
            current = current - factor[column, earlier] * forward[earlier]
        forward.append(current / factor[column, column])
    answer = [None] * order
    for column in reversed(range(order)):
        current = forward[column]
        for later in range(column + 1, order):
            current = current - factor[later, column] * answer[later]
        answer[column] = current / factor[column, column]
    return jnp.stack(answer)

def source_terms(weights, partials, baseline):
    products = [weights * partials[first] * partials[second] for first, second in SOURCE_PAIRS]
    products = products + [weights * partials[first] * baseline for first in range(5)]
    return products

def knot_terms(weights, partials, baseline):
    result = []
    for segment in range(4):
        portion = partials[4 * segment:4 * segment + 4]
        sums_rows = [lax.optimization_barrier(jnp.sum(weights * portion[first] * portion[second], axis=-1)) for first, second in KNOT_PAIRS]
        sums_rows = sums_rows + [lax.optimization_barrier(jnp.sum(weights * portion[first] * baseline, axis=-1)) for first in range(4)]
        result.append(jnp.stack(sums_rows))
    return result

def correct(baseline, partials, picked):
    accumulated = partials[0] * picked[0]
    for component in range(1, partials.shape[0]):
        accumulated = accumulated + partials[component] * picked[component]
    return baseline - accumulated

def knot_correct(baseline, partials, extended, knot_start):
    accumulated = None
    for segment in range(4):
        values = jnp.take(extended, knot_start + segment, axis=1)
        for component in range(4):
            addend = partials[4 * segment + component] * values[component][:, None]
            accumulated = addend if accumulated is None else accumulated + addend
    return baseline - accumulated

def reference(residual, obs_weight, source_partials, attitude_partials, source_index, tile_pixel, tile_knot, pixel_slot):
    blocks = residual.shape[0] // TILES_DEV
    sources = pixel_slot.shape[0] * SRC_PIX
    source_id = (jnp.take(pixel_slot, tile_pixel)[:, None] * SRC_PIX + source_index).astype(jnp.int32)

    def add_block(running, number):
        offset = (number * TILES_DEV).astype(jnp.int32)
        baseline = lax.dynamic_slice_in_dim(residual, offset, TILES_DEV, 0)
        weights = lax.dynamic_slice_in_dim(obs_weight, offset, TILES_DEV, 0)
        partials = lax.dynamic_slice_in_dim(source_partials, offset, TILES_DEV, 1)
        indices = lax.dynamic_slice_in_dim(source_id, offset, TILES_DEV, 0)
        stacked = jnp.stack(source_terms(weights, partials, baseline), axis=-1).reshape(-1, 20)
        return (running + jax.ops.segment_sum(stacked, indices.reshape(-1), num_segments=sources), None)
    normals, _ = lax.scan(add_block, jnp.zeros((sources, 20), jnp.float32), jnp.arange(blocks, dtype=jnp.int32))
    normals = normals.T
    source_update = damped_solve(normals[:15], normals[15:], 5, SOURCE_PAIRS)
    picked = jnp.take(source_update, source_id, axis=1)
    settled = correct(residual, source_partials, picked)
    knots = KNOTS
    accumulated = jnp.zeros((14, knots + 3), jnp.float32)
    for segment, tile_sums in enumerate(knot_terms(obs_weight, attitude_partials, settled)):
        accumulated = accumulated + jax.ops.segment_sum(tile_sums.T, tile_knot + segment, num_segments=knots + 3).T
    attitude_update = damped_solve(accumulated[:10, :knots], accumulated[10:, :knots], 4, KNOT_PAIRS)
    extended = jnp.concatenate([attitude_update, jnp.zeros((4, 3), jnp.float32)], axis=1)
    final_residual = knot_correct(settled, attitude_partials, extended, tile_knot)
    return (final_residual, source_update, attitude_update)
```

```python
import jax
import jax.numpy as jnp
from jax import lax
from jax.experimental import pallas as pl
from jax.experimental.pallas import tpu as pltpu
from jax.sharding import PartitionSpec as P

TILES = 512
OWNERS = 16
TIMES = 8
CAP = 96
PIX = 128
SRC = 128
FIELDS = 7
BLOCK_ROWS = CAP * FIELDS + 8
SPAN = 32
TERMS = 20
PART_ROWS = (PIX // TIMES) * TERMS
KNOT_PAIRS = tuple((c, e) for c in range(4) for e in range(c, 4))
TERM_ROW = {
    (0, 0): 0, (1, 1): 1, (2, 2): 2, (3, 3): 3, (4, 4): 4, (0, 5): 5,
    (0, 1): 6, (1, 2): 7, (2, 3): 8, (3, 4): 9, (4, 5): 10, (0, 4): 11, (1, 5): 12,
    (0, 2): 13, (1, 3): 14, (2, 4): 15, (3, 5): 16, (0, 3): 17, (1, 4): 18, (2, 5): 19,
}
VMEM = pl.BlockSpec(memory_space=pltpu.VMEM)
SMEM = pl.BlockSpec(memory_space=pltpu.SMEM)
F32 = jnp.float32
BF16 = jnp.bfloat16


def params(**kw):
    return pltpu.CompilerParams(vmem_limit_bytes=60 * 1024 * 1024, **kw)


def pack_kernel(pixel_ref, slot_ref, res_ref, w_ref, part_ref, idx_ref,
                out_ref, where_ref, pix_ref, count_ref, stage_ref):
    def clear(i, _):
        for o in range(OWNERS):
            pix_ref[o, i] = PIX
        return 0

    lax.fori_loop(0, 128, clear, 0)
    for o in range(OWNERS):
        count_ref[o] = 0

    def scale(g, _):
        rows = pl.ds(pl.multiple_of(g * 8, 8), 8)
        root = jnp.sqrt(w_ref[rows, :])
        for a in range(5):
            stage_ref[a, rows, :] = part_ref[a, rows, :] * root
        stage_ref[5, rows, :] = res_ref[rows, :] * root
        stage_ref[6, rows, :] = idx_ref[rows, :].astype(F32)
        return 0

    lax.fori_loop(0, TILES // 8, scale, 0, unroll=4)

    def place(g, _):
        for j in range(8):
            t = g * 8 + j
            seat = slot_ref[pixel_ref[t]]
            owner = lax.shift_right_logical(seat, 7)
            position = count_ref[owner]
            count_ref[owner] = position + 1
            where_ref[t] = owner * CAP + position
            pix_ref[owner, position] = lax.bitwise_and(seat, 127)
            base = owner * BLOCK_ROWS + position * FIELDS
            for f in range(FIELDS):
                out_ref[pl.ds(base + f, 1), :] = stage_ref[f, pl.ds(t, 1), :]
        return 0

    lax.fori_loop(0, TILES // 8, place, 0)
    for o in range(OWNERS):
        pix_ref[o, 127] = count_ref[o]


def pack(tile_pixel, pixel_slot, residual, weight, partials, index):
    return pl.pallas_call(
        pack_kernel,
        out_shape=(
            jax.ShapeDtypeStruct((OWNERS * BLOCK_ROWS, 128), F32),
            jax.ShapeDtypeStruct((TILES,), jnp.int32),
            jax.ShapeDtypeStruct((OWNERS, 128), jnp.int32),
        ),
        in_specs=[SMEM, SMEM, VMEM, VMEM, VMEM, VMEM],
        out_specs=(VMEM, SMEM, SMEM),
        scratch_shapes=[pltpu.SMEM((OWNERS,), jnp.int32), pltpu.VMEM((FIELDS, TILES, 128), F32)],
        compiler_params=params(),
        name="pack",
    )(tile_pixel, pixel_slot, residual, weight, partials, index)


def pair_products(v, row):
    low5, low4 = row < 5, row < 4
    one = pltpu.roll(v, 1, 0)
    first = jnp.where(low5, v, pltpu.roll(v, 5, 0))
    second = jnp.where(low5, pltpu.roll(v, 7, 0), one)
    third = jnp.where(low4, v, pltpu.roll(v, 4, 0))
    fourth = jnp.where(low4, pltpu.roll(v, 6, 0), one)
    return jnp.concatenate([first * v, first * second, third * fourth], axis=0)


def tile_sums(v, row, sources):
    products = pair_products(v, row)
    high = products.astype(BF16).astype(F32)
    left = jnp.concatenate([high, products - high], axis=0).astype(BF16)
    hits = (v[6:7, :].astype(BF16) == sources).astype(BF16)
    out = lax.dot_general(left, hits, (((1,), (1,)), ((), ())), preferred_element_type=F32)
    return out[:24] + out[24:]


def normals_kernel(pix_ref, in_ref, out_ref, acc_ref):
    zero = jnp.zeros((24, 128), F32)

    def clear(p, _):
        acc_ref[p] = zero
        return 0

    lax.fori_loop(0, PIX + 1, clear, 0, unroll=8)
    row = lax.broadcasted_iota(jnp.int32, (8, 128), 0)
    sources = lax.broadcasted_iota(jnp.int32, (128, 128), 0).astype(F32).astype(BF16)

    def sender(b, _):
        count = pix_ref[b, 127]

        def group(g, _):
            sums = []
            for j in range(8):
                start = b * BLOCK_ROWS + (g * 8 + j) * FIELDS
                sums.append(tile_sums(in_ref[pl.ds(start, 8), :], row, sources))
            for j in range(8):
                p = pix_ref[b, g * 8 + j]
                acc_ref[p] = acc_ref[p] + sums[j]
            return 0

        lax.fori_loop(0, lax.shift_right_logical(count + 7, 3), group, 0)
        return 0

    lax.fori_loop(0, OWNERS, sender, 0)

    def write(p, _):
        base = p * TERMS
        out_ref[pl.ds(base, 8), :] = acc_ref[p, 0:8]
        out_ref[pl.ds(base + 6, 8), :] = acc_ref[p, 8:16]
        out_ref[pl.ds(base + 13, 7), :] = acc_ref[p, 16:23]
        return 0

    lax.fori_loop(0, PIX, write, 0, unroll=4)


def normals_of(pix, arrived):
    return pl.pallas_call(
        normals_kernel,
        out_shape=jax.ShapeDtypeStruct((PIX * TERMS, 128), F32),
        in_specs=[SMEM, VMEM],
        out_specs=VMEM,
        scratch_shapes=[pltpu.VMEM((PIX + 1, 24, 128), F32)],
        compiler_params=params(),
        name="normals",
    )(pix, arrived)


def damped_solve(entries, target, order):
    factor = {}
    for column in range(order):
        pivot = entries[column, column] + 1.0
        for earlier in range(column):
            pivot = pivot - factor[column, earlier] * factor[column, earlier]
        pivot = jnp.sqrt(pivot)
        factor[column, column] = pivot
        for below in range(column + 1, order):
            current = entries[column, below]
            for earlier in range(column):
                current = current - factor[below, earlier] * factor[column, earlier]
            factor[below, column] = current / pivot
    forward = []
    for column in range(order):
        current = target[column]
        for earlier in range(column):
            current = current - factor[column, earlier] * forward[earlier]
        forward.append(current / factor[column, column])
    answer = [None] * order
    for column in reversed(range(order)):
        current = forward[column]
        for later in range(column + 1, order):
            current = current - factor[later, column] * answer[later]
        answer[column] = current / factor[column, column]
    return answer


def solve_kernel(in_ref, out_ref):
    count = PIX // TIMES
    sums = []
    for term in range(TERMS):
        total = in_ref[0, pl.ds(term, count, stride=TERMS), :]
        for part in range(1, TIMES):
            total = total + in_ref[part, pl.ds(term, count, stride=TERMS), :]
        sums.append(total)
    entries = {key: sums[at] for key, at in TERM_ROW.items() if key[1] < 5}
    target = [sums[TERM_ROW[a, 5]] for a in range(5)]
    for a, value in enumerate(damped_solve(entries, target, 5)):
        out_ref[pl.ds(a, count, stride=5), :] = value


def solve(parts):
    return pl.pallas_call(
        solve_kernel,
        out_shape=jax.ShapeDtypeStruct((5 * PIX // TIMES, 128), F32),
        in_specs=[VMEM],
        out_specs=VMEM,
        compiler_params=params(),
        name="solve",
    )(parts)


def pick_kernel(pix_ref, in_ref, table_ref, out_ref, update_ref, rows_ref):
    row = lax.broadcasted_iota(jnp.int32, (8, 128), 0)

    def spread(p, _):
        rows_ref[p] = jnp.where(row < 5, table_ref[pl.ds(p * 5, 8), :], -1.0)
        return 0

    lax.fori_loop(0, PIX - 1, spread, 0, unroll=4)
    rows_ref[PIX - 1] = jnp.where(
        row < 5, pltpu.roll(table_ref[pl.ds(PIX * 5 - 8, 8), :], 5, 0), -1.0)
    for p in range(PIX):
        update_ref[:, p * 128:(p + 1) * 128] = rows_ref[p, 0:5]

    def sender(b, _):
        count = pix_ref[b, 127]

        def group(g, _):
            for j in range(8):
                start = b * BLOCK_ROWS + (g * 8 + j) * FIELDS
                v = in_ref[pl.ds(start, 8), :]
                table = rows_ref[jnp.minimum(pix_ref[b, g * 8 + j], PIX - 1)]
                at = jnp.broadcast_to(jnp.clip(v[6:7, :].astype(jnp.int32), 0, 127), (8, 128))
                picked = jnp.take_along_axis(table, at, axis=1)
                terms = jnp.where(row < 6, v * picked, 0.0)
                out_ref[b, pl.ds(g * 8 + j, 1), :] = -jnp.sum(terms, axis=0, keepdims=True)
            return 0

        lax.fori_loop(0, lax.shift_right_logical(count + 7, 3), group, 0)
        return 0

    lax.fori_loop(0, OWNERS, sender, 0)


def pick(pix, arrived, table):
    return pl.pallas_call(
        pick_kernel,
        out_shape=(
            jax.ShapeDtypeStruct((OWNERS, CAP, 128), F32),
            jax.ShapeDtypeStruct((5, PIX * SRC), F32),
        ),
        in_specs=[SMEM, VMEM, VMEM],
        out_specs=(VMEM, VMEM),
        scratch_shapes=[pltpu.VMEM((PIX, 8, 128), F32)],
        compiler_params=params(),
        name="pick",
    )(pix, arrived, table)


def knot_hits(knot_row, first):
    lane = lax.broadcasted_iota(jnp.int32, (SPAN, TILES), 0)
    return (lane == knot_row - first).astype(F32)


def split_dot(hits, value):
    high = value.astype(BF16)
    low = (value - high.astype(F32)).astype(BF16)
    return (jnp.dot(hits, high, preferred_element_type=F32)
            + jnp.dot(hits, low, preferred_element_type=F32))


def quad_kernel(knot_ref, first_ref, w_ref, att_ref, out_ref, hits_ref):
    hits = knot_hits(knot_ref[...], first_ref[0])
    flipped = hits.T
    hits_ref[...] = jnp.concatenate([flipped] * 3 + [jnp.zeros_like(flipped)], axis=1).astype(BF16)
    hits = hits.astype(BF16)
    lane = lax.broadcasted_iota(jnp.int32, (SPAN, 128), 1)
    total = jnp.zeros((SPAN, 128), F32)
    weight = w_ref[...]
    for m in range(4):
        for c in range(4):
            scaled = weight * att_ref[4 * m + c]
            for e in range(c, 4):
                sums = split_dot(hits, scaled * att_ref[4 * m + e])
                at = 14 * m + KNOT_PAIRS.index((c, e))
                total = total + jnp.where(lane == at, jnp.sum(sums, axis=1, keepdims=True), 0.0)
    out_ref[...] = total


def quads(knots, first, weight, attitude):
    return pl.pallas_call(
        quad_kernel,
        out_shape=(jax.ShapeDtypeStruct((SPAN, 128), F32), jax.ShapeDtypeStruct((TILES, 128), BF16)),
        in_specs=[VMEM, SMEM, VMEM, VMEM],
        out_specs=(VMEM, VMEM),
        compiler_params=params(),
        name="quads",
    )(knots, first, weight, attitude)


def linear_kernel(where_ref, knot_ref, first_ref, back_ref, w_ref, att_ref, quad_ref,
                  settled_ref, sums_ref, halo_ref):
    def fetch(g, _):
        for j in range(8):
            t = g * 8 + j
            settled_ref[pl.ds(t, 1), :] = back_ref[pl.ds(where_ref[t], 1), :]
        return 0

    lax.fori_loop(0, TILES // 8, fetch, 0)
    weight = w_ref[...]
    root = jnp.sqrt(weight)
    settled = settled_ref[...] / root
    settled_ref[...] = settled
    hits = knot_hits(knot_ref[...], first_ref[0]).astype(BF16)
    lane = lax.broadcasted_iota(jnp.int32, (SPAN, 128), 1)
    total = quad_ref[...]
    scaled = weight * settled
    for m in range(4):
        for c in range(4):
            sums = split_dot(hits, scaled * att_ref[4 * m + c])
            at = 14 * m + 10 + c
            total = total + jnp.where(lane == at, jnp.sum(sums, axis=1, keepdims=True), 0.0)
    lane40 = lax.broadcasted_iota(jnp.int32, (SPAN + 8, 128), 1)
    padded = jnp.concatenate([total, jnp.zeros((8, 128), F32)], axis=0)
    moved = jnp.where(lane40 < 14, padded, 0.0)
    for m in range(1, 4):
        shifted = pltpu.roll(pltpu.roll(padded, m, 0), 128 - 14 * m, 1)
        moved = moved + jnp.where(lane40 < 14, shifted, 0.0)
    sums_ref[...] = moved[:SPAN]
    halo_ref[...] = moved[SPAN:]


def linear(where, knots, first, back, weight, attitude, quad):
    return pl.pallas_call(
        linear_kernel,
        out_shape=(
            jax.ShapeDtypeStruct((TILES, 128), F32),
            jax.ShapeDtypeStruct((SPAN, 128), F32),
            jax.ShapeDtypeStruct((8, 128), F32),
        ),
        in_specs=[SMEM, VMEM, SMEM, VMEM, VMEM, VMEM, VMEM],
        out_specs=(VMEM, VMEM, VMEM),
        compiler_params=params(),
        name="linear",
    )(where, knots, first, back, weight, attitude, quad)


def knot_solve_kernel(sums_ref, halo_ref, out_ref, head_ref):
    sums = sums_ref[...]
    sums = jnp.concatenate([sums[:8] + halo_ref[...], sums[8:]], axis=0)

    def column(at):
        return jnp.broadcast_to(sums[:, at:at + 1], (SPAN, 128))

    entries = {pair: column(n) for n, pair in enumerate(KNOT_PAIRS)}
    answer = damped_solve(entries, [column(10 + c) for c in range(4)], 4)
    for c in range(4):
        out_ref[c] = answer[c]
        head_ref[c] = answer[c][:8]


def knot_solve(sums, halo):
    return pl.pallas_call(
        knot_solve_kernel,
        out_shape=(jax.ShapeDtypeStruct((4, SPAN, 128), F32), jax.ShapeDtypeStruct((4, 8, 128), F32)),
        in_specs=[VMEM, VMEM],
        out_specs=(VMEM, VMEM),
        compiler_params=params(),
        name="knot_solve",
    )(sums, halo)


def final_kernel(hits_ref, settled_ref, att_ref, own_ref, next_ref, out_ref):
    hits = hits_ref[...]
    total = None
    for m in range(4):
        for c in range(4):
            both = jnp.concatenate([own_ref[c], next_ref[c]], axis=0)
            value = both[m:m + SPAN]
            high = value.astype(BF16)
            rest = value - high.astype(F32)
            middle = rest.astype(BF16)
            low = (rest - middle.astype(F32)).astype(BF16)
            table = jnp.concatenate([high, middle, low, jnp.zeros_like(high)], axis=0)
            term = att_ref[4 * m + c] * jnp.dot(hits, table, preferred_element_type=F32)
            total = term if total is None else total + term
    out_ref[...] = settled_ref[...] - total


def finish(hits, settled, attitude, own, following):
    return pl.pallas_call(
        final_kernel,
        out_shape=jax.ShapeDtypeStruct((TILES, 128), F32),
        in_specs=[VMEM] * 5,
        out_specs=VMEM,
        compiler_params=params(),
        name="finish",
    )(hits, settled, attitude, own, following)


def body(residual, obs_weight, source_partials, attitude_partials, source_index,
         tile_pixel, tile_knot, pixel_slot):
    both = ("tm", "sky")
    block = lax.axis_index("tm") * OWNERS + lax.axis_index("sky")
    first = (block * SPAN).reshape(1)
    knots = tile_knot.reshape(1, TILES)
    packed, where, pix = pack(tile_pixel, pixel_slot, residual, obs_weight, source_partials, source_index)
    arrived = lax.all_to_all(packed.reshape(OWNERS, BLOCK_ROWS, 128), "sky", 0, 0, tiled=True)
    pix = lax.all_to_all(pix, "sky", 0, 0, tiled=True)
    arrived = arrived.reshape(OWNERS * BLOCK_ROWS, 128)
    quad, hits = quads(knots, first, obs_weight, attitude_partials)
    normals = normals_of(pix, arrived)
    parts = lax.all_to_all(normals.reshape(TIMES, PART_ROWS, 128), "tm", 0, 0, tiled=True)
    solved = solve(parts)
    table = lax.all_gather(solved, "tm", axis=0, tiled=True)
    corrected, source_update = pick(pix, arrived, table)
    back = lax.all_to_all(corrected, "sky", 0, 0, tiled=True).reshape(OWNERS * CAP, 128)
    settled, sums, halo = linear(where, knots, first, back, obs_weight, attitude_partials, quad)
    last = TIMES * OWNERS - 1
    halo = lax.ppermute(halo, both, [(q, q + 1) for q in range(last)])
    own, head = knot_solve(sums, halo)
    following = lax.ppermute(head, both, [(q + 1, q) for q in range(last)])
    final = finish(hits, settled, attitude_partials, own, following)
    attitude_update = lax.all_gather(own[:, :, 0], "sky", axis=1, tiled=True)
    return final, source_update, attitude_update


def solution(mesh):
    in_specs = (
        P(("tm", "sky"), None),
        P(("tm", "sky"), None),
        P(None, ("tm", "sky"), None),
        P(None, ("tm", "sky"), None),
        P(("tm", "sky"), None),
        P(("tm", "sky")),
        P(("tm", "sky")),
        P(),
    )
    out_specs = (P(("tm", "sky"), None), P(None, "sky"), P(None, "tm"))
    return jax.shard_map(body, mesh=mesh, in_specs=in_specs, out_specs=out_specs, check_vma=False)
```

```python
import jax
import jax.numpy as jnp
from jax import lax
from jax.experimental import pallas as pl
from jax.experimental.pallas import tpu as pltpu
from jax.sharding import PartitionSpec as P

TILES = 512
OWNERS = 16
TIMES = 8
CAP = 96
PIX = 128
SRC = 128
FIELDS = 7
CLASSES = 4
SEATS = CAP // CLASSES
SLOTS = OWNERS * CLASSES
BLOCK_ROWS = SEATS * FIELDS
ROWS_IN = SLOTS * BLOCK_ROWS + 8
SPAN = 32
TERMS = 20
QUARTER = PIX // 4
HALF = PIX // TIMES
QROWS = QUARTER * TERMS
HROWS = HALF * TERMS
KNOT_PAIRS = tuple((c, e) for c in range(4) for e in range(c, 4))
TERM_ROW = {
    (0, 0): 0, (1, 1): 1, (2, 2): 2, (3, 3): 3, (4, 4): 4, (0, 5): 5,
    (0, 1): 6, (1, 2): 7, (2, 3): 8, (3, 4): 9, (4, 5): 10, (0, 4): 11, (1, 5): 12,
    (0, 2): 13, (1, 3): 14, (2, 4): 15, (3, 5): 16, (0, 3): 17, (1, 4): 18, (2, 5): 19,
}
VMEM = pl.BlockSpec(memory_space=pltpu.VMEM)
SMEM = pl.BlockSpec(memory_space=pltpu.SMEM)
F32 = jnp.float32
BF16 = jnp.bfloat16


def params(**kw):
    return pltpu.CompilerParams(vmem_limit_bytes=60 * 1024 * 1024, **kw)


def pack_kernel(pixel_ref, slot_ref, res_ref, w_ref, part_ref, idx_ref,
                out_ref, where_ref, pix_ref, count_ref, stage_ref):
    def clear(i, _):
        for b in range(SLOTS):
            pix_ref[b, i] = PIX
        return 0

    lax.fori_loop(0, SEATS, clear, 0)
    for o in range(OWNERS):
        count_ref[o] = 0

    def scale(g, _):
        rows = pl.ds(pl.multiple_of(g * 8, 8), 8)
        root = jnp.sqrt(w_ref[rows, :])
        for a in range(5):
            stage_ref[a, rows, :] = part_ref[a, rows, :] * root
        stage_ref[5, rows, :] = res_ref[rows, :] * root
        stage_ref[6, rows, :] = idx_ref[rows, :].astype(F32)
        return 0

    lax.fori_loop(0, TILES // 8, scale, 0, unroll=4)

    def place(g, _):
        for j in range(8):
            t = g * 8 + j
            seat = slot_ref[pixel_ref[t]]
            owner = lax.shift_right_logical(seat, 7)
            rank = count_ref[owner]
            count_ref[owner] = rank + 1
            plan = lax.bitwise_and(rank, 1)
            half = lax.bitwise_and(lax.shift_right_logical(rank, 1), 1)
            position = lax.shift_right_logical(rank, 2)
            block = plan * (2 * OWNERS) + owner * 2 + half
            where_ref[t] = block * SEATS + position
            pix_ref[block, position] = lax.bitwise_and(seat, 127)
            base = block * BLOCK_ROWS + position * FIELDS
            for f in range(FIELDS):
                out_ref[pl.ds(base + f, 1), :] = stage_ref[f, pl.ds(t, 1), :]
        return 0

    lax.fori_loop(0, TILES // 8, place, 0)
    for o in range(OWNERS):
        for plan in range(2):
            for half in range(2):
                left = count_ref[o] + (3 - plan - 2 * half)
                pix_ref[plan * 2 * OWNERS + o * 2 + half, 127] = lax.shift_right_logical(left, 2)


def pack(tile_pixel, pixel_slot, residual, weight, partials, index):
    return pl.pallas_call(
        pack_kernel,
        out_shape=(
            jax.ShapeDtypeStruct((ROWS_IN, 128), F32),
            jax.ShapeDtypeStruct((TILES,), jnp.int32),
            jax.ShapeDtypeStruct((SLOTS, 128), jnp.int32),
        ),
        in_specs=[SMEM, SMEM, VMEM, VMEM, VMEM, VMEM],
        out_specs=(VMEM, SMEM, SMEM),
        scratch_shapes=[pltpu.SMEM((OWNERS,), jnp.int32), pltpu.VMEM((FIELDS, TILES, 128), F32)],
        compiler_params=params(),
        name="pack",
    )(tile_pixel, pixel_slot, residual, weight, partials, index)


def place_of():
    tm, sky = lax.axis_index("tm"), lax.axis_index("sky")
    return tm // 2, tm % 2, sky // 4, (sky // 2) % 2, sky % 2


def device_of(y, zh, x, zl, c):
    return (y * 2 + zh, x * 4 + zl * 2 + c)


def send(src, dst, sent, landed, device):
    copy = pltpu.make_async_remote_copy(
        src_ref=src, dst_ref=dst, send_sem=sent, recv_sem=landed,
        device_id=device, device_id_type=pl.DeviceIdType.MESH)
    copy.start()
    return copy


def greet(devices):
    barrier = pltpu.get_barrier_semaphore()
    for device in devices:
        pl.semaphore_signal(barrier, inc=1, device_id=device, device_id_type=pl.DeviceIdType.MESH)
    pl.semaphore_wait(barrier, len(devices))


MOVES = [(plan, d, dz, dc, h) for d in (2, 1, 3, 0) for dz in (1, 0) for plan in range(2)
         for dc in (1, 0) for h in range(2)]


def exchange_kernel(sizes, *refs):
    n = len(sizes)
    srcs, dsts = refs[:n], refs[n:2 * n]
    bounces = refs[2 * n:3 * n]
    sent, landed, local = refs[3 * n:]
    y, zh, x, zl, c = place_of()
    mine = (x * 4 + zl * 2 + c, y * 4 + zl * 2 + c)
    routes = []
    for plan, d, dz, dc, h in MOVES:
        far = ((y if plan else x) + d) % 4
        zl_to, c_to, zh_to = (zl + dz) % 2, (c + dc) % 2, (zh + dz * h) % 2
        owner = far * 4 + zl_to * 2 + c_to
        to = device_of(far, zh_to, x, zl_to, c_to) if plan else device_of(y, zh_to, far, zl_to, c_to)
        routes.append((plan * 32 + owner * 2 + h, plan * 32 + mine[plan] * 2 + h, to,
                       d == 0 and dz == 0 and dc == 0))
    greet([to for _, _, to, own in routes if not own])
    copies = []
    for k, (block, slot, to, own) in enumerate(routes):
        if not own:
            for i, size in enumerate(sizes):
                copies.append(send(srcs[i].at[pl.ds(block * size, size)], dsts[i].at[pl.ds(slot * size, size)],
                                   sent.at[i, k], landed.at[i, k], to))
    kept = [(block, at) for at, (block, slot, to, own) in enumerate(r for r in routes if r[3])]
    for way in range(2):
        moves = []
        for block, at in kept:
            for i, size in enumerate(sizes):
                ends = (srcs[i].at[pl.ds(block * size, size)], bounces[i].at[pl.ds(at * size, size)])
                if way:
                    ends = (ends[1], dsts[i].at[pl.ds(block * size, size)])
                move = pltpu.make_async_copy(ends[0], ends[1], local.at[i, at])
                move.start()
                moves.append(move)
        for move in moves:
            move.wait()
    for copy in copies:
        copy.wait()


def exchange(arrays, sizes, number):
    n = len(arrays)
    return pl.pallas_call(
        lambda *refs: exchange_kernel(sizes, *refs),
        out_shape=tuple(jax.ShapeDtypeStruct(a.shape, a.dtype) for a in arrays),
        in_specs=[pl.BlockSpec(memory_space=pltpu.HBM)] * n,
        out_specs=tuple(pl.BlockSpec(memory_space=pltpu.HBM) for _ in arrays),
        scratch_shapes=[pltpu.VMEM((4 * size, 128), a.dtype) for a, size in zip(arrays, sizes)] + [
            pltpu.SemaphoreType.DMA((n, len(MOVES))),
            pltpu.SemaphoreType.DMA((n, len(MOVES))),
            pltpu.SemaphoreType.DMA((n, 4)),
        ],
        compiler_params=params(collective_id=number, has_side_effects=True),
        name="exchange" + str(number),
    )(*arrays)


def pair_products(v, row):
    low5, low4 = row < 5, row < 4
    one = pltpu.roll(v, 1, 0)
    first = jnp.where(low5, v, pltpu.roll(v, 5, 0))
    second = jnp.where(low5, pltpu.roll(v, 7, 0), one)
    third = jnp.where(low4, v, pltpu.roll(v, 4, 0))
    fourth = jnp.where(low4, pltpu.roll(v, 6, 0), one)
    return jnp.concatenate([first * v, first * second, third * fourth], axis=0)


def tile_sums(v, row, sources):
    products = pair_products(v, row)
    high = products.astype(BF16).astype(F32)
    left = jnp.concatenate([high, products - high], axis=0).astype(BF16)
    hits = (v[6:7, :].astype(BF16) == sources).astype(BF16)
    out = lax.dot_general(left, hits, (((1,), (1,)), ((), ())), preferred_element_type=F32)
    return out[:24] + out[24:]


def normals_kernel(pix_ref, in_ref, out_ref, acc_ref):
    zero = jnp.zeros((24, 128), F32)

    def clear(p, _):
        acc_ref[p] = zero
        return 0

    lax.fori_loop(0, 2 * (PIX + 1), clear, 0, unroll=6)
    row = lax.broadcasted_iota(jnp.int32, (8, 128), 0)
    sources = lax.broadcasted_iota(jnp.int32, (128, 128), 0).astype(F32).astype(BF16)

    def sender(b, _):
        count = pix_ref[b, 127]
        offset = lax.shift_right_logical(b, 5) * (PIX + 1)

        def group(g, _):
            sums = []
            for j in range(8):
                start = b * BLOCK_ROWS + (g * 8 + j) * FIELDS
                sums.append(tile_sums(in_ref[pl.ds(start, 8), :], row, sources))
            for j in range(8):
                p = offset + pix_ref[b, g * 8 + j]
                acc_ref[p] = acc_ref[p] + sums[j]
            return 0

        lax.fori_loop(0, lax.shift_right_logical(count + 7, 3), group, 0)
        return 0

    lax.fori_loop(0, SLOTS, sender, 0)

    for plan in range(2):
        def write(p, _):
            base = p * TERMS
            at = plan * (PIX + 1) + p
            out_ref[plan, pl.ds(base, 8), :] = acc_ref[at, 0:8]
            out_ref[plan, pl.ds(base + 6, 8), :] = acc_ref[at, 8:16]
            out_ref[plan, pl.ds(base + 13, 7), :] = acc_ref[at, 16:23]
            return 0

        lax.fori_loop(0, PIX, write, 0, unroll=4)


def normals_of(pix, arrived):
    return pl.pallas_call(
        normals_kernel,
        out_shape=jax.ShapeDtypeStruct((2, PIX * TERMS, 128), F32),
        in_specs=[SMEM, VMEM],
        out_specs=VMEM,
        scratch_shapes=[pltpu.VMEM((2 * (PIX + 1), 24, 128), F32)],
        compiler_params=params(),
        name="normals",
    )(pix, arrived)


def damped_solve(entries, target, order):
    factor = {}
    for column in range(order):
        pivot = entries[column, column] + 1.0
        for earlier in range(column):
            pivot = pivot - factor[column, earlier] * factor[column, earlier]
        pivot = jnp.sqrt(pivot)
        factor[column, column] = pivot
        for below in range(column + 1, order):
            current = entries[column, below]
            for earlier in range(column):
                current = current - factor[below, earlier] * factor[column, earlier]
            factor[below, column] = current / pivot
    forward = []
    for column in range(order):
        current = target[column]
        for earlier in range(column):
            current = current - factor[column, earlier] * forward[earlier]
        forward.append(current / factor[column, column])
    answer = [None] * order
    for column in reversed(range(order)):
        current = forward[column]
        for later in range(column + 1, order):
            current = current - factor[later, column] * answer[later]
        answer[column] = current / factor[column, column]
    return answer


def add_rows(out, base, refs, rows):
    def step(g, _):
        at = pl.multiple_of(g * 16, 16)
        total = None
        for ref, start in refs:
            value = ref[pl.ds(start + at, 16), :]
            total = value if total is None else total + value
        out[pl.ds(base + at, 16), :] = total
        return 0

    lax.fori_loop(0, rows // 16, step, 0)


def reduce_kernel(in_ref, table_ref, first_ref, sum_ref, other_ref, whole_ref, own_ref,
                  sent1, landed1, sent2, landed2, sent3, landed3):
    y, zh, x, zl, c = place_of()
    tm = y * 2 + zh
    diagonal = x == y
    greet([device_of((y + dy) % 4, (zh + dz) % 2, (x + dx) % 4, zl, c)
           for dx in range(4) for dy in range(4) for dz in range(2) if (dx, dy, dz) != (0, 0, 0)])
    copies = []
    for d in (2, 1, 3):
        for plan in range(2):
            far = ((x if plan else y) + d) % 4
            to = device_of(y, zh, far, zl, c) if plan else device_of(far, zh, x, zl, c)
            copies.append(send(in_ref.at[plan, pl.ds(far * QROWS, QROWS)], first_ref.at[plan, d - 1],
                               sent1.at[plan, d - 1], landed1.at[plan, d - 1], to))
    for copy in copies:
        copy.wait()
    for plan in range(2):
        near = (x if plan else y) * QROWS
        add_rows(sum_ref.at[plan], 0,
                 [(in_ref.at[plan], near)] + [(first_ref.at[plan, d], 0) for d in range(3)], QROWS)

    @pl.when(diagonal)
    def _():
        add_rows(sum_ref.at[0], 0, [(sum_ref.at[0], 0), (sum_ref.at[1], 0)], QROWS)

    across = send(sum_ref.at[0, pl.ds((1 - zh) * HROWS, HROWS)], other_ref.at[2], sent2.at[2], landed2.at[2],
                  device_of(y, 1 - zh, x, zl, c))

    @pl.when(diagonal)
    def _():
        def clear(g, _):
            other_ref[0, pl.ds(pl.multiple_of(g * 16, 16), 16), :] = jnp.zeros((16, 128), F32)
            other_ref[1, pl.ds(pl.multiple_of(g * 16, 16), 16), :] = jnp.zeros((16, 128), F32)
            return 0

        lax.fori_loop(0, HROWS // 16, clear, 0)

    @pl.when(jnp.logical_not(diagonal))
    def _():
        flips = [send(sum_ref.at[1, pl.ds(z * HROWS, HROWS)], other_ref.at[zh], sent2.at[z], landed2.at[zh],
                      device_of(x, z, y, zl, c)) for z in range(2)]
        for z, flip in enumerate(flips):
            flip.wait_send()
            pltpu.make_async_remote_copy(
                src_ref=sum_ref.at[1, pl.ds(z * HROWS, HROWS)], dst_ref=other_ref.at[z],
                send_sem=sent2.at[z], recv_sem=landed2.at[z], device_id=device_of(x, z, y, zl, c),
                device_id_type=pl.DeviceIdType.MESH).wait_recv()

    across.wait()
    add_rows(whole_ref, 0, [(sum_ref.at[0], zh * HROWS)] + [(other_ref.at[i], 0) for i in range(3)], HROWS)
    sums = [whole_ref[pl.ds(term, HALF, stride=TERMS), :] for term in range(TERMS)]
    entries = {key: sums[at] for key, at in TERM_ROW.items() if key[1] < 5}
    target = [sums[TERM_ROW[a, 5]] for a in range(5)]
    for a, value in enumerate(damped_solve(entries, target, 5)):
        own_ref[pl.ds(a, HALF, stride=5), :] = value
    part = pl.ds(tm * HALF * 5, HALF * 5)
    copies = []
    for d in (2, 1, 3, 0):
        for z in (1, 0):
            if (d, z) != (0, 0):
                copies.append(send(own_ref, table_ref.at[0, part], sent3.at[0, d * 2 + z], landed3.at[0, d * 2 + z],
                                   device_of((y + d) % 4, (zh + z) % 2, x, zl, c)))
    table_ref[0, part, :] = own_ref[...]

    def spread(d, z):
        return pltpu.make_async_remote_copy(
            src_ref=own_ref, dst_ref=table_ref.at[1, part], send_sem=sent3.at[1, d * 2 + z],
            recv_sem=landed3.at[1, tm], device_id=device_of(x, (zh + z) % 2, (x + d) % 4, zl, c),
            device_id_type=pl.DeviceIdType.MESH)

    for d in (2, 1, 3, 0):
        for z in (1, 0):
            if (d, z) != (0, 0):
                spread(d, z).start()

    @pl.when(jnp.logical_not(diagonal))
    def _():
        spread(0, 0).start()

    @pl.when(diagonal)
    def _():
        table_ref[1, part, :] = own_ref[...]

    for copy in copies:
        copy.wait()
    for d in range(4):
        for z in range(2):
            if (d, z) != (0, 0):
                spread(d, z).wait_send()

    @pl.when(jnp.logical_not(diagonal))
    def _():
        spread(0, 0).wait_send()

    for i in range(TIMES):
        arrival = pltpu.make_async_remote_copy(
            src_ref=own_ref, dst_ref=table_ref.at[1, pl.ds(i * HALF * 5, HALF * 5)], send_sem=sent3.at[1, 0],
            recv_sem=landed3.at[1, i], device_id=device_of(i // 2, i % 2, y, zl, c),
            device_id_type=pl.DeviceIdType.MESH)

        @pl.when(jnp.logical_or(jnp.logical_not(diagonal), tm != i))
        def _():
            arrival.wait_recv()


def reduce_and_solve(normals):
    return pl.pallas_call(
        reduce_kernel,
        out_shape=jax.ShapeDtypeStruct((2, PIX * 5, 128), F32),
        in_specs=[VMEM],
        out_specs=VMEM,
        scratch_shapes=[
            pltpu.VMEM((2, 3, QROWS, 128), F32),
            pltpu.VMEM((2, QROWS, 128), F32),
            pltpu.VMEM((3, HROWS, 128), F32),
            pltpu.VMEM((HROWS, 128), F32),
            pltpu.VMEM((HALF * 5, 128), F32),
            pltpu.SemaphoreType.DMA((2, 3)),
            pltpu.SemaphoreType.DMA((2, 3)),
            pltpu.SemaphoreType.DMA((3,)),
            pltpu.SemaphoreType.DMA((3,)),
            pltpu.SemaphoreType.DMA((2, 8)),
            pltpu.SemaphoreType.DMA((2, 8)),
        ],
        compiler_params=params(collective_id=2, has_side_effects=True),
        name="reduce",
    )(normals)


def pick_kernel(pix_ref, in_ref, table_ref, out_ref, update_ref, rows_ref):
    row = lax.broadcasted_iota(jnp.int32, (8, 128), 0)
    for plan in range(2):
        def spread(p, _):
            rows_ref[plan * PIX + p] = jnp.where(row < 5, table_ref[plan, pl.ds(p * 5, 8), :], -1.0)
            return 0

        lax.fori_loop(0, PIX - 1, spread, 0, unroll=4)
        rows_ref[plan * PIX + PIX - 1] = jnp.where(
            row < 5, pltpu.roll(table_ref[plan, pl.ds(PIX * 5 - 8, 8), :], 5, 0), -1.0)
    for p in range(PIX):
        update_ref[:, p * 128:(p + 1) * 128] = rows_ref[p, 0:5]

    def sender(b, _):
        count = pix_ref[b, 127]
        offset = lax.shift_right_logical(b, 5) * PIX

        def group(g, _):
            for j in range(8):
                start = b * BLOCK_ROWS + (g * 8 + j) * FIELDS
                v = in_ref[pl.ds(start, 8), :]
                table = rows_ref[offset + jnp.minimum(pix_ref[b, g * 8 + j], PIX - 1)]
                at = jnp.broadcast_to(jnp.clip(v[6:7, :].astype(jnp.int32), 0, 127), (8, 128))
                picked = jnp.take_along_axis(table, at, axis=1)
                terms = jnp.where(row < 6, v * picked, 0.0)
                out_ref[pl.ds(b * SEATS + g * 8 + j, 1), :] = -jnp.sum(terms, axis=0, keepdims=True)
            return 0

        lax.fori_loop(0, lax.shift_right_logical(count + 7, 3), group, 0)
        return 0

    lax.fori_loop(0, SLOTS, sender, 0)


def pick(pix, arrived, table):
    return pl.pallas_call(
        pick_kernel,
        out_shape=(
            jax.ShapeDtypeStruct((SLOTS * SEATS, 128), F32),
            jax.ShapeDtypeStruct((5, PIX * SRC), F32),
        ),
        in_specs=[SMEM, VMEM, VMEM],
        out_specs=(VMEM, VMEM),
        scratch_shapes=[pltpu.VMEM((2 * PIX, 8, 128), F32)],
        compiler_params=params(),
        name="pick",
    )(pix, arrived, table)


def knot_hits(knot_row, first):
    lane = lax.broadcasted_iota(jnp.int32, (SPAN, TILES), 0)
    return (lane == knot_row - first).astype(F32)


def split_dot(hits, value):
    high = value.astype(BF16)
    low = (value - high.astype(F32)).astype(BF16)
    return (jnp.dot(hits, high, preferred_element_type=F32)
            + jnp.dot(hits, low, preferred_element_type=F32))


def quad_kernel(knot_ref, first_ref, w_ref, att_ref, out_ref, hits_ref):
    hits = knot_hits(knot_ref[...], first_ref[0])
    flipped = hits.T
    hits_ref[...] = jnp.concatenate([flipped] * 3 + [jnp.zeros_like(flipped)], axis=1).astype(BF16)
    hits = hits.astype(BF16)
    lane = lax.broadcasted_iota(jnp.int32, (SPAN, 128), 1)
    total = jnp.zeros((SPAN, 128), F32)
    weight = w_ref[...]
    for m in range(4):
        for c in range(4):
            scaled = weight * att_ref[4 * m + c]
            for e in range(c, 4):
                sums = split_dot(hits, scaled * att_ref[4 * m + e])
                at = 14 * m + KNOT_PAIRS.index((c, e))
                total = total + jnp.where(lane == at, jnp.sum(sums, axis=1, keepdims=True), 0.0)
    out_ref[...] = total


def quads(knots, first, weight, attitude):
    return pl.pallas_call(
        quad_kernel,
        out_shape=(jax.ShapeDtypeStruct((SPAN, 128), F32), jax.ShapeDtypeStruct((TILES, 128), BF16)),
        in_specs=[VMEM, SMEM, VMEM, VMEM],
        out_specs=(VMEM, VMEM),
        compiler_params=params(),
        name="quads",
    )(knots, first, weight, attitude)


def finish_kernel(where_ref, knot_ref, first_ref, back_ref, w_ref, att_ref, quad_ref, hits_ref,
                  out_ref, attitude_ref, settled_ref, edge_ref, head_ref, next_ref, piece_ref, pieces_ref,
                  sent, landed):
    tm, sky = lax.axis_index("tm"), lax.axis_index("sky")
    block = tm * OWNERS + sky
    after = ((block + 1) // OWNERS % TIMES, (block + 1) % OWNERS)
    before = ((block + 127) // OWNERS % TIMES, (block + 127) % OWNERS)
    has_after, has_before = block < TIMES * OWNERS - 1, block > 0
    peers = [(tm, (sky + d) % OWNERS) for d in range(1, OWNERS)]
    barrier = pltpu.get_barrier_semaphore()
    edge_ref[1] = jnp.zeros((8, 128), F32)
    next_ref[...] = jnp.zeros((4, 8, 128), F32)
    for peer in peers + [after, before]:
        pl.semaphore_signal(barrier, inc=1, device_id=peer, device_id_type=pl.DeviceIdType.MESH)

    def fetch(g, _):
        for j in range(8):
            t = g * 8 + j
            settled_ref[pl.ds(t, 1), :] = back_ref[pl.ds(where_ref[t], 1), :]
        return 0

    lax.fori_loop(0, TILES // 8, fetch, 0)
    weight = w_ref[...]
    settled = settled_ref[...] / jnp.sqrt(weight)
    settled_ref[...] = settled
    hits = knot_hits(knot_ref[...], first_ref[0]).astype(BF16)
    lane = lax.broadcasted_iota(jnp.int32, (SPAN, 128), 1)
    total = quad_ref[...]
    scaled = weight * settled
    for m in range(4):
        for c in range(4):
            sums = split_dot(hits, scaled * att_ref[4 * m + c])
            at = 14 * m + 10 + c
            total = total + jnp.where(lane == at, jnp.sum(sums, axis=1, keepdims=True), 0.0)
    lane40 = lax.broadcasted_iota(jnp.int32, (SPAN + 8, 128), 1)
    padded = jnp.concatenate([total, jnp.zeros((8, 128), F32)], axis=0)
    moved = jnp.where(lane40 < 14, padded, 0.0)
    for m in range(1, 4):
        shifted = pltpu.roll(pltpu.roll(padded, m, 0), 128 - 14 * m, 1)
        moved = moved + jnp.where(lane40 < 14, shifted, 0.0)
    edge_ref[0] = moved[SPAN:]
    pl.semaphore_wait(barrier, OWNERS + 1)

    def onward(to):
        return pltpu.make_async_remote_copy(
            src_ref=edge_ref.at[0], dst_ref=edge_ref.at[1], send_sem=sent.at[0], recv_sem=landed.at[0],
            device_id=to, device_id_type=pl.DeviceIdType.MESH)

    def backward(to):
        return pltpu.make_async_remote_copy(
            src_ref=head_ref, dst_ref=next_ref, send_sem=sent.at[1], recv_sem=landed.at[1],
            device_id=to, device_id_type=pl.DeviceIdType.MESH)

    @pl.when(has_after)
    def _():
        onward(after).start()

    @pl.when(has_before)
    def _():
        onward(before).wait_recv()

    sums = jnp.concatenate([moved[:8] + edge_ref[1], moved[8:SPAN]], axis=0)

    def column(at):
        return jnp.broadcast_to(sums[:, at:at + 1], (SPAN, 128))

    entries = {pair: column(n) for n, pair in enumerate(KNOT_PAIRS)}
    answer = damped_solve(entries, [column(10 + c) for c in range(4)], 4)
    for c in range(4):
        head_ref[c] = answer[c][:8]

    @pl.when(has_before)
    def _():
        backward(before).start()

    row32 = lax.broadcasted_iota(jnp.int32, (SPAN, 128), 0)
    row8 = lax.broadcasted_iota(jnp.int32, (8, 128), 0)
    piece = jnp.zeros((8, 128), F32)
    for c in range(4):
        line = jnp.sum(jnp.where(lane == row32 + (sky % 4) * SPAN, answer[c], 0.0), axis=0, keepdims=True)
        piece = jnp.where(row8 == c, line, piece)
    piece_ref[...] = piece
    copies = [send(piece_ref, pieces_ref.at[sky], sent.at[1 + d], landed.at[1 + d], peers[d - 1])
              for d in range(1, OWNERS)]
    pieces_ref[sky] = piece

    @pl.when(has_after)
    def _():
        backward(after).wait_recv()

    fix = None
    for m in range(4):
        for c in range(4):
            both = jnp.concatenate([answer[c], next_ref[c]], axis=0)
            value = both[m:m + SPAN]
            high = value.astype(BF16)
            rest = value - high.astype(F32)
            middle = rest.astype(BF16)
            low = (rest - middle.astype(F32)).astype(BF16)
            table = jnp.concatenate([high, middle, low, jnp.zeros_like(high)], axis=0)
            term = att_ref[4 * m + c] * jnp.dot(hits_ref[...], table, preferred_element_type=F32)
            fix = term if fix is None else fix + term
    out_ref[...] = settled_ref[...] - fix
    for copy in copies:
        copy.wait()
    for j in range(4):
        total = pieces_ref[4 * j]
        for i in range(1, 4):
            total = total + pieces_ref[4 * j + i]
        attitude_ref[:, j * 128:(j + 1) * 128] = total[:4]

    @pl.when(has_after)
    def _():
        onward(after).wait_send()

    @pl.when(has_before)
    def _():
        backward(before).wait_send()


def finish(where, knots, first, back, weight, attitude, quad, hits):
    return pl.pallas_call(
        finish_kernel,
        out_shape=(
            jax.ShapeDtypeStruct((TILES, 128), F32),
            jax.ShapeDtypeStruct((4, SPAN * OWNERS), F32),
        ),
        in_specs=[SMEM, VMEM, SMEM, VMEM, VMEM, VMEM, VMEM, VMEM],
        out_specs=(VMEM, VMEM),
        scratch_shapes=[
            pltpu.VMEM((TILES, 128), F32),
            pltpu.VMEM((2, 8, 128), F32),
            pltpu.VMEM((4, 8, 128), F32),
            pltpu.VMEM((4, 8, 128), F32),
            pltpu.VMEM((8, 128), F32),
            pltpu.VMEM((OWNERS, 8, 128), F32),
            pltpu.SemaphoreType.DMA((OWNERS + 1,)),
            pltpu.SemaphoreType.DMA((OWNERS + 1,)),
        ],
        compiler_params=params(collective_id=4, has_side_effects=True),
        name="finish",
    )(where, knots, first, back, weight, attitude, quad, hits)


def body(residual, obs_weight, source_partials, attitude_partials, source_index,
         tile_pixel, tile_knot, pixel_slot):
    block = lax.axis_index("tm") * OWNERS + lax.axis_index("sky")
    first = (block * SPAN).reshape(1)
    knots = tile_knot.reshape(1, TILES)
    packed, where, pix = pack(tile_pixel, pixel_slot, residual, obs_weight, source_partials, source_index)
    arrived, pix = exchange((packed, pix), (BLOCK_ROWS, 1), 1)
    quad, hits = quads(knots, first, obs_weight, attitude_partials)
    normals = normals_of(pix, arrived)
    table = reduce_and_solve(normals)
    corrected, source_update = pick(pix, arrived, table)
    (back,) = exchange((corrected,), (SEATS,), 3)
    final, attitude_update = finish(
        where, knots, first, back, obs_weight, attitude_partials, quad, hits)
    return final, source_update, attitude_update


def solution(mesh):
    in_specs = (
        P(("tm", "sky"), None),
        P(("tm", "sky"), None),
        P(None, ("tm", "sky"), None),
        P(None, ("tm", "sky"), None),
        P(("tm", "sky"), None),
        P(("tm", "sky")),
        P(("tm", "sky")),
        P(),
    )
    out_specs = (P(("tm", "sky"), None), P(None, "sky"), P(None, "tm"))
    return jax.shard_map(body, mesh=mesh, in_specs=in_specs, out_specs=out_specs, check_vma=False)
```

```python
import jax
import jax.numpy as jnp
from jax import lax
from jax.experimental import pallas as pl
from jax.experimental.pallas import tpu as pltpu
from jax.sharding import PartitionSpec as P

TILES = 512
OWNERS = 16
TIMES = 8
CAP = 96
PIX = 128
SRC = 128
FIELDS = 7
CLASSES = 4
SEATS = CAP // CLASSES
SLOTS = OWNERS * CLASSES
BLOCK_ROWS = SEATS * FIELDS
ROWS_IN = SLOTS * BLOCK_ROWS + 8
SPAN = 32
TERMS = 20
QUARTER = PIX // 4
HALF = PIX // TIMES
QROWS = QUARTER * TERMS
HROWS = HALF * TERMS
KNOT_PAIRS = tuple((c, e) for c in range(4) for e in range(c, 4))
TERM_ROW = {
    (0, 0): 0, (1, 1): 1, (2, 2): 2, (3, 3): 3, (4, 4): 4, (0, 5): 5,
    (0, 1): 6, (1, 2): 7, (2, 3): 8, (3, 4): 9, (4, 5): 10, (0, 4): 11, (1, 5): 12,
    (0, 2): 13, (1, 3): 14, (2, 4): 15, (3, 5): 16, (0, 3): 17, (1, 4): 18, (2, 5): 19,
}
VMEM = pl.BlockSpec(memory_space=pltpu.VMEM)
SMEM = pl.BlockSpec(memory_space=pltpu.SMEM)
F32 = jnp.float32
BF16 = jnp.bfloat16


def params(**kw):
    return pltpu.CompilerParams(vmem_limit_bytes=60 * 1024 * 1024, **kw)


def pack_kernel(pixel_ref, slot_ref, res_ref, w_ref, part_ref, idx_ref,
                out_ref, where_ref, count_ref, stage_ref):
    for o in range(OWNERS):
        count_ref[o] = 0
    nothing = jnp.zeros((SEATS, 128), F32)

    def clear(b, _):
        base = pl.multiple_of(b * BLOCK_ROWS, 8)
        for i in range(FIELDS):
            out_ref[pl.ds(base + i * SEATS, SEATS), :] = nothing
        out_ref[pl.ds(base + 6, SEATS, stride=FIELDS), :] = nothing - 1.0
        return 0

    lax.fori_loop(0, SLOTS, clear, 0)

    def scale(g, _):
        rows = pl.ds(pl.multiple_of(g * 8, 8), 8)
        root = jnp.sqrt(w_ref[rows, :])
        for a in range(5):
            stage_ref[a, rows, :] = part_ref[a, rows, :] * root
        stage_ref[5, rows, :] = res_ref[rows, :] * root
        stage_ref[6, rows, :] = idx_ref[rows, :].astype(F32)
        return 0

    lax.fori_loop(0, TILES // 8, scale, 0, unroll=4)

    def place(g, _):
        for j in range(8):
            t = g * 8 + j
            seat = slot_ref[pixel_ref[t]]
            owner = lax.shift_right_logical(seat, 7)
            rank = count_ref[owner]
            count_ref[owner] = rank + 1
            plan = lax.bitwise_and(rank, 1)
            half = lax.bitwise_and(lax.shift_right_logical(rank, 1), 1)
            position = lax.shift_right_logical(rank, 2)
            block = plan * (2 * OWNERS) + owner * 2 + half
            where_ref[t] = block * SEATS + position
            base = block * BLOCK_ROWS + position * FIELDS
            for f in range(6):
                out_ref[pl.ds(base + f, 1), :] = stage_ref[f, pl.ds(t, 1), :]
            first = (lax.bitwise_and(seat, 127) * SRC).astype(F32)
            out_ref[pl.ds(base + 6, 1), :] = stage_ref[6, pl.ds(t, 1), :] + first
        return 0

    lax.fori_loop(0, TILES // 8, place, 0)


def pack(tile_pixel, pixel_slot, residual, weight, partials, index):
    return pl.pallas_call(
        pack_kernel,
        out_shape=(
            jax.ShapeDtypeStruct((ROWS_IN, 128), F32),
            jax.ShapeDtypeStruct((TILES,), jnp.int32),
        ),
        in_specs=[SMEM, SMEM, VMEM, VMEM, VMEM, VMEM],
        out_specs=(VMEM, SMEM),
        scratch_shapes=[pltpu.SMEM((OWNERS,), jnp.int32), pltpu.VMEM((FIELDS, TILES, 128), F32)],
        compiler_params=params(),
        name="pack",
    )(tile_pixel, pixel_slot, residual, weight, partials, index)


def place_of():
    tm, sky = lax.axis_index("tm"), lax.axis_index("sky")
    return tm // 2, tm % 2, sky // 4, (sky // 2) % 2, sky % 2


def device_of(y, zh, x, zl, c):
    return (y * 2 + zh, x * 4 + zl * 2 + c)


def send(src, dst, sent, landed, device):
    copy = pltpu.make_async_remote_copy(
        src_ref=src, dst_ref=dst, send_sem=sent, recv_sem=landed,
        device_id=device, device_id_type=pl.DeviceIdType.MESH)
    copy.start()
    return copy


def greet(devices):
    barrier = pltpu.get_barrier_semaphore()
    for device in devices:
        pl.semaphore_signal(barrier, inc=1, device_id=device, device_id_type=pl.DeviceIdType.MESH)
    pl.semaphore_wait(barrier, len(devices))


MOVES = [(plan, d, dz, dc, h)
         for d, dz in ((0, 0), (1, 0), (3, 0), (0, 1), (2, 0), (1, 1), (3, 1), (2, 1))
         for plan in range(2) for dc in range(2) for h in range(2)]
OWN = (0, 1, 4, 5)
CHUNK = 4
CHUNKS = SLOTS // CHUNK
PITCH = 136
ROOM = BLOCK_ROWS + 8
HBM = pl.BlockSpec(memory_space=pltpu.HBM)


def routes_of(back):
    y, zh, x, zl, c = place_of()
    sign = -1 if back else 1
    routes = []
    for plan, d, dz, dc, h in MOVES:
        far = ((y if plan else x) + 4 + sign * d) % 4
        zl_to, c_to, zh_to = (zl + dz) % 2, (c + dc) % 2, (zh + dz * h) % 2
        to = device_of(far, zh_to, x, zl_to, c_to) if plan else device_of(y, zh_to, far, zl_to, c_to)
        if back:
            owner = (y if plan else x) * 4 + zl * 2 + c
        else:
            owner = far * 4 + zl_to * 2 + c_to
        routes.append((plan * 2 * OWNERS + owner * 2 + h, to))
    return routes


def pair_products(v, row):
    low5, low4 = row < 5, row < 4
    one = pltpu.roll(v, 1, 0)
    first = jnp.where(low5, v, pltpu.roll(v, 5, 0))
    second = jnp.where(low5, pltpu.roll(v, 7, 0), one)
    third = jnp.where(low4, v, pltpu.roll(v, 4, 0))
    fourth = jnp.where(low4, pltpu.roll(v, 6, 0), one)
    return jnp.concatenate([first * v, first * second, third * fourth], axis=0)


def left_side(v, row):
    products = pair_products(v, row)
    high = products.astype(BF16).astype(F32)
    return jnp.concatenate([high, products - high], axis=0).astype(BF16)


def landing(in_ref, arr_ref, sent, landed, k, to):
    return pltpu.make_async_remote_copy(
        src_ref=in_ref.at[pl.ds(k * BLOCK_ROWS, BLOCK_ROWS)],
        dst_ref=arr_ref.at[pl.ds(k * ROOM, BLOCK_ROWS)], send_sem=sent.at[k], recv_sem=landed.at[k],
        device_id=to, device_id_type=pl.DeviceIdType.MESH)


def gather_kernel(in_ref, att_hbm, w_hbm, knot_ref, first_ref,
                  keep_ref, sums_ref, pix_ref, quad_ref, hits_ref,
                  arr_ref, att_ref, w_ref, spread_ref, sent, landed, local, stored):
    routes = routes_of(False)
    load_att = pltpu.make_async_copy(att_hbm, att_ref, local.at[4])
    load_w = pltpu.make_async_copy(w_hbm, w_ref, local.at[5])
    load_att.start()
    load_w.start()
    greet([to for k, (_, to) in enumerate(routes) if k not in OWN])
    copies = []
    for k, (block, to) in enumerate(routes):
        if k not in OWN:
            copies.append(send(in_ref.at[pl.ds(block * BLOCK_ROWS, BLOCK_ROWS)],
                               arr_ref.at[pl.ds(k * ROOM, BLOCK_ROWS)], sent.at[k], landed.at[k], to))
    kept = []
    for i, k in enumerate(OWN):
        kept.append(pltpu.make_async_copy(in_ref.at[pl.ds(routes[k][0] * BLOCK_ROWS, BLOCK_ROWS)],
                                          arr_ref.at[pl.ds(k * ROOM, BLOCK_ROWS)], local.at[i]))
        kept[-1].start()

    def clear(g, _):
        spread_ref[pl.ds(pl.multiple_of(g * 8, 8), 8), :] = jnp.zeros((8, 128), F32)
        return 0

    lax.fori_loop(0, 24 * PITCH // 8, clear, 0, unroll=4)

    def clear_sums(g, _):
        for plan in range(2):
            sums_ref[plan, pl.ds(pl.multiple_of(g * 16, 16), 16), :] = jnp.zeros((16, 128), F32)
        return 0

    lax.fori_loop(0, PIX * TERMS // 16, clear_sums, 0, unroll=4)
    load_att.wait()
    load_w.wait()
    quad_sums(knot_ref, first_ref, w_ref, att_ref, quad_ref, hits_ref)
    for move in kept:
        move.wait()
    row = lax.broadcasted_iota(jnp.int32, (8, 128), 0)
    sources = lax.broadcasted_iota(jnp.int32, (128, 128), 0).astype(F32)
    pixels = lax.broadcasted_iota(jnp.int32, (SEATS, 128), 1)
    seat_row = lax.broadcasted_iota(jnp.int32, (SEATS, 128), 0)
    blank = jnp.zeros((48, 128), BF16)

    def keep(k):
        return pltpu.make_async_copy(arr_ref.at[pl.ds(k * ROOM, BLOCK_ROWS)],
                                     keep_ref.at[pl.ds(k * BLOCK_ROWS, BLOCK_ROWS)], stored.at[k])

    def chunk_step(chunk, _):
        plan = chunk % 2
        for i in range(CHUNK):
            k = chunk * CHUNK + i
            arrival = landing(in_ref, arr_ref, sent, landed, k, routes[2][1])
            if i < 2:
                @pl.when(chunk >= 2)
                def _():
                    arrival.wait_recv()
            else:
                arrival.wait_recv()
            keep(k).start()

        def group(g, _):
            for j in range(0, 8, 2):
                start = (chunk * CHUNK + g // 3) * ROOM + (g % 3 * 8 + j) * FIELDS
                lefts, hits = [], []
                for i in range(2):
                    v = arr_ref[pl.ds(start + i * FIELDS, 8), :]
                    within = v - jnp.floor(v * (1.0 / SRC)) * SRC
                    lefts.append(left_side(v, row))
                    hits.append((within[6:7, :] == sources).astype(F32).astype(BF16))
                left = jnp.concatenate([jnp.concatenate([lefts[0], blank], axis=1),
                                        jnp.concatenate([blank, lefts[1]], axis=1)], axis=0)
                out = lax.dot_general(left, jnp.concatenate(hits, axis=1), (((1,), (1,)), ((), ())),
                                      preferred_element_type=F32)
                for i in range(2):
                    both = out[48 * i:48 * i + 24] + out[48 * i + 24:48 * i + 48]
                    for n in range(3):
                        spread_ref[pl.ds(8 * n * PITCH + g * 8 + j + i, 8, stride=PITCH), :] = both[8 * n:8 * n + 8]
            return 0

        lax.fori_loop(0, CHUNK * SEATS // 8, group, 0)
        places = []
        for i in range(CHUNK):
            k = chunk * CHUNK + i
            whole = arr_ref[pl.ds(k * ROOM + 6, SEATS, stride=FIELDS), :]
            pixel = jnp.floor(whole * (1.0 / SRC)).astype(jnp.int32)
            places.append((pixel == pixels).astype(F32))
            line = jnp.sum(jnp.where(pixels == seat_row, pixel + plan * PIX, 0), axis=0, keepdims=True)
            count = jnp.sum((pixel >= 0).astype(jnp.int32), axis=0, keepdims=True)
            line = jnp.where(pixels[:1] == 127, count, jnp.where(pixels[:1] < SEATS, line, 0))
            pix_ref[pl.ds(k, 1), :] = jnp.maximum(line, 0)
        places.append(jnp.zeros((128 - CHUNK * SEATS, 128), F32))
        place = jnp.concatenate(places, axis=0).T.astype(BF16)
        place = jnp.concatenate([place, place], axis=1)
        for n in range(TERMS):
            at = n + (2 if n >= 6 else 0) + (1 if n >= 13 else 0)
            value = spread_ref[pl.ds(at * PITCH, 128), :]
            high = value.astype(BF16)
            low = (value - high.astype(F32)).astype(BF16)
            added = jnp.dot(place, jnp.concatenate([high, low], axis=0), preferred_element_type=F32)
            for part in range(TIMES):
                rows = pl.ds(part * HROWS + n * HALF, HALF)
                sums_ref[plan, rows, :] = sums_ref[plan, rows, :] + added[part * HALF:(part + 1) * HALF]
        return 0

    lax.fori_loop(0, CHUNKS, chunk_step, 0)
    for copy in copies:
        copy.wait_send()

    def kept_step(k, _):
        keep(k).wait()
        return 0

    lax.fori_loop(0, SLOTS, kept_step, 0)


def gather_tiles(packed, attitude, weight, knots, first):
    return pl.pallas_call(
        gather_kernel,
        out_shape=(
            jax.ShapeDtypeStruct((ROWS_IN, 128), F32),
            jax.ShapeDtypeStruct((2, PIX * TERMS, 128), F32),
            jax.ShapeDtypeStruct((SLOTS, 128), jnp.int32),
            jax.ShapeDtypeStruct((SPAN, 128), F32),
            jax.ShapeDtypeStruct((TILES, 128), BF16),
        ),
        in_specs=[HBM, HBM, HBM, VMEM, SMEM],
        out_specs=(HBM, VMEM, VMEM, VMEM, VMEM),
        scratch_shapes=[
            pltpu.VMEM((SLOTS * ROOM, 128), F32),
            pltpu.VMEM((16, TILES, 128), F32),
            pltpu.VMEM((TILES, 128), F32),
            pltpu.VMEM((24 * PITCH, 128), F32),
            pltpu.SemaphoreType.DMA((SLOTS,)),
            pltpu.SemaphoreType.DMA((SLOTS,)),
            pltpu.SemaphoreType.DMA((6,)),
            pltpu.SemaphoreType.DMA((SLOTS,)),
        ],
        compiler_params=params(collective_id=1, has_side_effects=True),
        name="gather_tiles",
    )(packed, attitude, weight, knots, first)


def return_kernel(in_ref, out_ref, bounce_ref, sent, landed, local):
    y, zh, x, zl, c = place_of()
    routes = routes_of(True)
    greet([to for k, (_, to) in enumerate(routes) if k not in OWN])
    copies = []
    for k, (block, to) in enumerate(routes):
        if k not in OWN:
            copies.append(send(in_ref.at[pl.ds(k * SEATS, SEATS)], out_ref.at[pl.ds(block * SEATS, SEATS)],
                               sent.at[k], landed.at[k], to))
    for way in range(2):
        moves = []
        for i, k in enumerate(OWN):
            middle = bounce_ref.at[pl.ds(i * SEATS, SEATS)]
            if way:
                move = pltpu.make_async_copy(middle, out_ref.at[pl.ds(routes[k][0] * SEATS, SEATS)], local.at[i])
            else:
                move = pltpu.make_async_copy(in_ref.at[pl.ds(k * SEATS, SEATS)], middle, local.at[i])
            move.start()
            moves.append(move)
        for move in moves:
            move.wait()
    for copy in copies:
        copy.wait()


def return_tiles(corrected):
    return pl.pallas_call(
        return_kernel,
        out_shape=jax.ShapeDtypeStruct(corrected.shape, F32),
        in_specs=[HBM],
        out_specs=HBM,
        scratch_shapes=[
            pltpu.VMEM((4 * SEATS, 128), F32),
            pltpu.SemaphoreType.DMA((SLOTS,)),
            pltpu.SemaphoreType.DMA((SLOTS,)),
            pltpu.SemaphoreType.DMA((4,)),
        ],
        compiler_params=params(collective_id=3, has_side_effects=True),
        name="return_tiles",
    )(corrected)


def damped_solve(entries, target, order):
    factor = {}
    for column in range(order):
        pivot = entries[column, column] + 1.0
        for earlier in range(column):
            pivot = pivot - factor[column, earlier] * factor[column, earlier]
        pivot = jnp.sqrt(pivot)
        factor[column, column] = pivot
        for below in range(column + 1, order):
            current = entries[column, below]
            for earlier in range(column):
                current = current - factor[below, earlier] * factor[column, earlier]
            factor[below, column] = current / pivot
    forward = []
    for column in range(order):
        current = target[column]
        for earlier in range(column):
            current = current - factor[column, earlier] * forward[earlier]
        forward.append(current / factor[column, column])
    answer = [None] * order
    for column in reversed(range(order)):
        current = forward[column]
        for later in range(column + 1, order):
            current = current - factor[later, column] * answer[later]
        answer[column] = current / factor[column, column]
    return answer


def add_rows(out, base, refs, rows):
    def step(g, _):
        at = pl.multiple_of(g * 16, 16)
        total = None
        for ref, start in refs:
            value = ref[pl.ds(start + at, 16), :]
            total = value if total is None else total + value
        out[pl.ds(base + at, 16), :] = total
        return 0

    lax.fori_loop(0, rows // 16, step, 0)


def reduce_kernel(in_ref, table_ref, first_ref, sum_ref, other_ref, whole_ref, own_ref,
                  sent1, landed1, sent2, landed2, sent3, landed3):
    y, zh, x, zl, c = place_of()
    tm = y * 2 + zh
    diagonal = x == y
    greet([device_of((y + dy) % 4, (zh + dz) % 2, (x + dx) % 4, zl, c)
           for dx in range(4) for dy in range(4) for dz in range(2) if (dx, dy, dz) != (0, 0, 0)])
    copies = []
    for d in (2, 1, 3):
        for plan in range(2):
            far = ((x if plan else y) + d) % 4
            to = device_of(y, zh, far, zl, c) if plan else device_of(far, zh, x, zl, c)
            copies.append(send(in_ref.at[plan, pl.ds(far * QROWS, QROWS)], first_ref.at[plan, d - 1],
                               sent1.at[plan, d - 1], landed1.at[plan, d - 1], to))
    for copy in copies:
        copy.wait()
    for plan in range(2):
        near = (x if plan else y) * QROWS
        add_rows(sum_ref.at[plan], 0,
                 [(in_ref.at[plan], near)] + [(first_ref.at[plan, d], 0) for d in range(3)], QROWS)

    @pl.when(diagonal)
    def _():
        add_rows(sum_ref.at[0], 0, [(sum_ref.at[0], 0), (sum_ref.at[1], 0)], QROWS)

    across = send(sum_ref.at[0, pl.ds((1 - zh) * HROWS, HROWS)], other_ref.at[2], sent2.at[2], landed2.at[2],
                  device_of(y, 1 - zh, x, zl, c))

    @pl.when(diagonal)
    def _():
        def clear(g, _):
            other_ref[0, pl.ds(pl.multiple_of(g * 16, 16), 16), :] = jnp.zeros((16, 128), F32)
            other_ref[1, pl.ds(pl.multiple_of(g * 16, 16), 16), :] = jnp.zeros((16, 128), F32)
            return 0

        lax.fori_loop(0, HROWS // 16, clear, 0)

    @pl.when(jnp.logical_not(diagonal))
    def _():
        flips = [send(sum_ref.at[1, pl.ds(z * HROWS, HROWS)], other_ref.at[zh], sent2.at[z], landed2.at[zh],
                      device_of(x, z, y, zl, c)) for z in range(2)]
        for z, flip in enumerate(flips):
            flip.wait_send()
            pltpu.make_async_remote_copy(
                src_ref=sum_ref.at[1, pl.ds(z * HROWS, HROWS)], dst_ref=other_ref.at[z],
                send_sem=sent2.at[z], recv_sem=landed2.at[z], device_id=device_of(x, z, y, zl, c),
                device_id_type=pl.DeviceIdType.MESH).wait_recv()

    across.wait()
    add_rows(whole_ref, 0, [(sum_ref.at[0], zh * HROWS)] + [(other_ref.at[i], 0) for i in range(3)], HROWS)
    sums = [whole_ref[pl.ds(term * HALF, HALF), :] for term in range(TERMS)]
    entries = {key: sums[at] for key, at in TERM_ROW.items() if key[1] < 5}
    target = [sums[TERM_ROW[a, 5]] for a in range(5)]
    for a, value in enumerate(damped_solve(entries, target, 5)):
        own_ref[pl.ds(a, HALF, stride=5), :] = value
    part = [pl.ds(plan * PIX * 5 + tm * HALF * 5, HALF * 5) for plan in range(2)]
    copies = []
    for d in (2, 1, 3, 0):
        for z in (1, 0):
            if (d, z) != (0, 0):
                copies.append(send(own_ref, table_ref.at[part[0]], sent3.at[0, d * 2 + z], landed3.at[0, d * 2 + z],
                                   device_of((y + d) % 4, (zh + z) % 2, x, zl, c)))
    table_ref[part[0], :] = own_ref[...]

    def spread(d, z):
        return pltpu.make_async_remote_copy(
            src_ref=own_ref, dst_ref=table_ref.at[part[1]], send_sem=sent3.at[1, d * 2 + z],
            recv_sem=landed3.at[1, tm], device_id=device_of(x, (zh + z) % 2, (x + d) % 4, zl, c),
            device_id_type=pl.DeviceIdType.MESH)

    for d in (2, 1, 3, 0):
        for z in (1, 0):
            if (d, z) != (0, 0):
                spread(d, z).start()

    @pl.when(jnp.logical_not(diagonal))
    def _():
        spread(0, 0).start()

    @pl.when(diagonal)
    def _():
        table_ref[part[1], :] = own_ref[...]

    for copy in copies:
        copy.wait()
    for d in range(4):
        for z in range(2):
            if (d, z) != (0, 0):
                spread(d, z).wait_send()

    @pl.when(jnp.logical_not(diagonal))
    def _():
        spread(0, 0).wait_send()

    for i in range(TIMES):
        arrival = pltpu.make_async_remote_copy(
            src_ref=own_ref, dst_ref=table_ref.at[pl.ds(PIX * 5 + i * HALF * 5, HALF * 5)], send_sem=sent3.at[1, 0],
            recv_sem=landed3.at[1, i], device_id=device_of(i // 2, i % 2, y, zl, c),
            device_id_type=pl.DeviceIdType.MESH)

        @pl.when(jnp.logical_or(jnp.logical_not(diagonal), tm != i))
        def _():
            arrival.wait_recv()


def reduce_and_solve(normals):
    return pl.pallas_call(
        reduce_kernel,
        out_shape=jax.ShapeDtypeStruct((2 * PIX * 5 + 8, 128), F32),
        in_specs=[VMEM],
        out_specs=VMEM,
        scratch_shapes=[
            pltpu.VMEM((2, 3, QROWS, 128), F32),
            pltpu.VMEM((2, QROWS, 128), F32),
            pltpu.VMEM((3, HROWS, 128), F32),
            pltpu.VMEM((HROWS, 128), F32),
            pltpu.VMEM((HALF * 5, 128), F32),
            pltpu.SemaphoreType.DMA((2, 3)),
            pltpu.SemaphoreType.DMA((2, 3)),
            pltpu.SemaphoreType.DMA((3,)),
            pltpu.SemaphoreType.DMA((3,)),
            pltpu.SemaphoreType.DMA((2, 8)),
            pltpu.SemaphoreType.DMA((2, 8)),
        ],
        compiler_params=params(collective_id=2, has_side_effects=True),
        name="reduce",
    )(normals)


def pick_kernel(pix_ref, in_ref, table_ref, out_ref, update_ref):
    row = lax.broadcasted_iota(jnp.int32, (8, 128), 0)
    for p in range(PIX):
        update_ref[:, p * 128:(p + 1) * 128] = table_ref[p * 5:p * 5 + 5, :]

    def sender(b, _):
        count = pix_ref[b, 127]

        def group(g, _):
            for j in range(8):
                start = b * BLOCK_ROWS + (g * 8 + j) * FIELDS
                v = in_ref[pl.ds(start, 8), :]
                table = table_ref[pl.ds(pix_ref[b, g * 8 + j] * 5, 8), :]
                within = (v - jnp.floor(v * (1.0 / SRC)) * SRC).astype(jnp.int32)
                at = jnp.broadcast_to(lax.bitwise_and(within[6:7, :], 127), (8, 128))
                picked = jnp.take_along_axis(table, at, axis=1)
                terms = jnp.where(row < 5, v * picked, jnp.where(row == 5, -v, 0.0))
                out_ref[pl.ds(b * SEATS + g * 8 + j, 1), :] = -jnp.sum(terms, axis=0, keepdims=True)
            return 0

        lax.fori_loop(0, lax.shift_right_logical(count + 7, 3), group, 0)
        return 0

    lax.fori_loop(0, SLOTS, sender, 0)


def pick(pix, arrived, table):
    return pl.pallas_call(
        pick_kernel,
        out_shape=(
            jax.ShapeDtypeStruct((SLOTS * SEATS, 128), F32),
            jax.ShapeDtypeStruct((5, PIX * SRC), F32),
        ),
        in_specs=[SMEM, VMEM, VMEM],
        out_specs=(VMEM, VMEM),
        compiler_params=params(),
        name="pick",
    )(pix, arrived, table)


def knot_hits(knot_row, first):
    lane = lax.broadcasted_iota(jnp.int32, (SPAN, TILES), 0)
    return (lane == knot_row - first).astype(F32)


def split_dot(hits, value):
    high = value.astype(BF16)
    low = (value - high.astype(F32)).astype(BF16)
    return (jnp.dot(hits, high, preferred_element_type=F32)
            + jnp.dot(hits, low, preferred_element_type=F32))


def quad_sums(knot_ref, first_ref, w_ref, att_ref, out_ref, hits_ref):
    hits = knot_hits(knot_ref[...], first_ref[0])
    flipped = hits.T
    hits_ref[...] = jnp.concatenate([flipped] * 3 + [jnp.zeros_like(flipped)], axis=1).astype(BF16)
    hits = hits.astype(BF16)
    lane = lax.broadcasted_iota(jnp.int32, (SPAN, 128), 1)
    total = jnp.zeros((SPAN, 128), F32)
    weight = w_ref[...]
    for m in range(4):
        for c in range(4):
            scaled = weight * att_ref[4 * m + c]
            for e in range(c, 4):
                sums = split_dot(hits, scaled * att_ref[4 * m + e])
                at = 14 * m + KNOT_PAIRS.index((c, e))
                total = total + jnp.where(lane == at, jnp.sum(sums, axis=1, keepdims=True), 0.0)
    out_ref[...] = total


def finish_kernel(where_ref, knot_ref, first_ref, back_ref, w_ref, att_ref, quad_ref, hits_ref,
                  out_ref, attitude_ref, settled_ref, edge_ref, head_ref, next_ref, piece_ref, pieces_ref,
                  sent, landed):
    tm, sky = lax.axis_index("tm"), lax.axis_index("sky")
    block = tm * OWNERS + sky
    after = ((block + 1) // OWNERS % TIMES, (block + 1) % OWNERS)
    before = ((block + 127) // OWNERS % TIMES, (block + 127) % OWNERS)
    has_after, has_before = block < TIMES * OWNERS - 1, block > 0
    peers = [(tm, (sky + d) % OWNERS) for d in range(1, OWNERS)]
    barrier = pltpu.get_barrier_semaphore()
    edge_ref[1] = jnp.zeros((8, 128), F32)
    next_ref[...] = jnp.zeros((4, 8, 128), F32)
    for peer in peers + [after, before]:
        pl.semaphore_signal(barrier, inc=1, device_id=peer, device_id_type=pl.DeviceIdType.MESH)

    def fetch(g, _):
        for j in range(8):
            t = g * 8 + j
            settled_ref[pl.ds(t, 1), :] = back_ref[pl.ds(where_ref[t], 1), :]
        return 0

    lax.fori_loop(0, TILES // 8, fetch, 0)
    weight = w_ref[...]
    settled = settled_ref[...] / jnp.sqrt(weight)
    settled_ref[...] = settled
    hits = knot_hits(knot_ref[...], first_ref[0]).astype(BF16)
    lane = lax.broadcasted_iota(jnp.int32, (SPAN, 128), 1)
    total = quad_ref[...]
    scaled = weight * settled
    for m in range(4):
        for c in range(4):
            sums = split_dot(hits, scaled * att_ref[4 * m + c])
            at = 14 * m + 10 + c
            total = total + jnp.where(lane == at, jnp.sum(sums, axis=1, keepdims=True), 0.0)
    lane40 = lax.broadcasted_iota(jnp.int32, (SPAN + 8, 128), 1)
    padded = jnp.concatenate([total, jnp.zeros((8, 128), F32)], axis=0)
    moved = jnp.where(lane40 < 14, padded, 0.0)
    for m in range(1, 4):
        shifted = pltpu.roll(pltpu.roll(padded, m, 0), 128 - 14 * m, 1)
        moved = moved + jnp.where(lane40 < 14, shifted, 0.0)
    edge_ref[0] = moved[SPAN:]
    pl.semaphore_wait(barrier, OWNERS + 1)

    def onward(to):
        return pltpu.make_async_remote_copy(
            src_ref=edge_ref.at[0], dst_ref=edge_ref.at[1], send_sem=sent.at[0], recv_sem=landed.at[0],
            device_id=to, device_id_type=pl.DeviceIdType.MESH)

    def backward(to):
        return pltpu.make_async_remote_copy(
            src_ref=head_ref, dst_ref=next_ref, send_sem=sent.at[1], recv_sem=landed.at[1],
            device_id=to, device_id_type=pl.DeviceIdType.MESH)

    @pl.when(has_after)
    def _():
        onward(after).start()

    @pl.when(has_before)
    def _():
        onward(before).wait_recv()

    sums = jnp.concatenate([moved[:8] + edge_ref[1], moved[8:SPAN]], axis=0)

    def column(at):
        return jnp.broadcast_to(sums[:, at:at + 1], (SPAN, 128))

    entries = {pair: column(n) for n, pair in enumerate(KNOT_PAIRS)}
    answer = damped_solve(entries, [column(10 + c) for c in range(4)], 4)
    for c in range(4):
        head_ref[c] = answer[c][:8]

    @pl.when(has_before)
    def _():
        backward(before).start()

    row32 = lax.broadcasted_iota(jnp.int32, (SPAN, 128), 0)
    row8 = lax.broadcasted_iota(jnp.int32, (8, 128), 0)
    piece = jnp.zeros((8, 128), F32)
    for c in range(4):
        line = jnp.sum(jnp.where(lane == row32 + (sky % 4) * SPAN, answer[c], 0.0), axis=0, keepdims=True)
        piece = jnp.where(row8 == c, line, piece)
    piece_ref[...] = piece
    copies = [send(piece_ref, pieces_ref.at[sky], sent.at[1 + d], landed.at[1 + d], peers[d - 1])
              for d in range(1, OWNERS)]
    pieces_ref[sky] = piece

    @pl.when(has_after)
    def _():
        backward(after).wait_recv()

    fix = None
    for m in range(4):
        for c in range(4):
            both = jnp.concatenate([answer[c], next_ref[c]], axis=0)
            value = both[m:m + SPAN]
            high = value.astype(BF16)
            rest = value - high.astype(F32)
            middle = rest.astype(BF16)
            low = (rest - middle.astype(F32)).astype(BF16)
            table = jnp.concatenate([high, middle, low, jnp.zeros_like(high)], axis=0)
            term = att_ref[4 * m + c] * jnp.dot(hits_ref[...], table, preferred_element_type=F32)
            fix = term if fix is None else fix + term
    out_ref[...] = settled_ref[...] - fix
    for copy in copies:
        copy.wait()
    for j in range(4):
        total = pieces_ref[4 * j]
        for i in range(1, 4):
            total = total + pieces_ref[4 * j + i]
        attitude_ref[:, j * 128:(j + 1) * 128] = total[:4]

    @pl.when(has_after)
    def _():
        onward(after).wait_send()

    @pl.when(has_before)
    def _():
        backward(before).wait_send()


def finish(where, knots, first, back, weight, attitude, quad, hits):
    return pl.pallas_call(
        finish_kernel,
        out_shape=(
            jax.ShapeDtypeStruct((TILES, 128), F32),
            jax.ShapeDtypeStruct((4, SPAN * OWNERS), F32),
        ),
        in_specs=[SMEM, VMEM, SMEM, VMEM, VMEM, VMEM, VMEM, VMEM],
        out_specs=(VMEM, VMEM),
        scratch_shapes=[
            pltpu.VMEM((TILES, 128), F32),
            pltpu.VMEM((2, 8, 128), F32),
            pltpu.VMEM((4, 8, 128), F32),
            pltpu.VMEM((4, 8, 128), F32),
            pltpu.VMEM((8, 128), F32),
            pltpu.VMEM((OWNERS, 8, 128), F32),
            pltpu.SemaphoreType.DMA((OWNERS + 1,)),
            pltpu.SemaphoreType.DMA((OWNERS + 1,)),
        ],
        compiler_params=params(collective_id=4, has_side_effects=True),
        name="finish",
    )(where, knots, first, back, weight, attitude, quad, hits)


def body(residual, obs_weight, source_partials, attitude_partials, source_index,
         tile_pixel, tile_knot, pixel_slot):
    block = lax.axis_index("tm") * OWNERS + lax.axis_index("sky")
    first = (block * SPAN).reshape(1)
    knots = tile_knot.reshape(1, TILES)
    packed, where = pack(tile_pixel, pixel_slot, residual, obs_weight, source_partials, source_index)
    arrived, normals, pix, quad, hits = gather_tiles(packed, attitude_partials, obs_weight, knots, first)
    table = reduce_and_solve(normals)
    corrected, source_update = pick(pix, arrived, table)
    back = return_tiles(corrected)
    final, attitude_update = finish(
        where, knots, first, back, obs_weight, attitude_partials, quad, hits)
    return final, source_update, attitude_update


def solution(mesh):
    in_specs = (
        P(("tm", "sky"), None),
        P(("tm", "sky"), None),
        P(None, ("tm", "sky"), None),
        P(None, ("tm", "sky"), None),
        P(("tm", "sky"), None),
        P(("tm", "sky")),
        P(("tm", "sky")),
        P(),
    )
    out_specs = (P(("tm", "sky"), None), P(None, "sky"), P(None, "tm"))
    return jax.shard_map(body, mesh=mesh, in_specs=in_specs, out_specs=out_specs, check_vma=False)
```

```python
import jax
import jax.numpy as jnp
from jax import lax
from jax.experimental import pallas as pl
from jax.experimental.pallas import tpu as pltpu
from jax.sharding import PartitionSpec as P

TILES = 512
OWNERS = 16
TIMES = 8
CAP = 96
PIX = 128
SRC = 128
FIELDS = 7
CLASSES = 4
SEATS = CAP // CLASSES
SLOTS = OWNERS * CLASSES
BLOCK_ROWS = SEATS * FIELDS
ROWS_IN = SLOTS * BLOCK_ROWS + 8
SPAN = 32
TERMS = 20
QUARTER = PIX // 4
HALF = PIX // TIMES
QROWS = QUARTER * TERMS
HROWS = HALF * TERMS
KNOT_PAIRS = tuple((c, e) for c in range(4) for e in range(c, 4))
TERM_ROW = {
    (0, 0): 0, (1, 1): 1, (2, 2): 2, (3, 3): 3, (4, 4): 4, (0, 5): 5,
    (0, 1): 6, (1, 2): 7, (2, 3): 8, (3, 4): 9, (4, 5): 10, (0, 4): 11, (1, 5): 12,
    (0, 2): 13, (1, 3): 14, (2, 4): 15, (3, 5): 16, (0, 3): 17, (1, 4): 18, (2, 5): 19,
}
VMEM = pl.BlockSpec(memory_space=pltpu.VMEM)
SMEM = pl.BlockSpec(memory_space=pltpu.SMEM)
F32 = jnp.float32
BF16 = jnp.bfloat16


def params(**kw):
    return pltpu.CompilerParams(vmem_limit_bytes=60 * 1024 * 1024, **kw)


def pack_kernel(pixel_ref, slot_ref, res_ref, w_ref, part_ref, idx_ref,
                out_ref, where_ref, count_ref, stage_ref):
    for o in range(OWNERS):
        count_ref[o] = 0
    nothing = jnp.zeros((SEATS, 128), F32)

    def clear(b, _):
        base = pl.multiple_of(b * BLOCK_ROWS, 8)
        for i in range(FIELDS):
            out_ref[pl.ds(base + i * SEATS, SEATS), :] = nothing
        out_ref[pl.ds(base + 6, SEATS, stride=FIELDS), :] = nothing - 1.0
        return 0

    lax.fori_loop(0, SLOTS, clear, 0)

    def scale(g, _):
        rows = pl.ds(pl.multiple_of(g * 8, 8), 8)
        root = jnp.sqrt(w_ref[rows, :])
        for a in range(5):
            stage_ref[a, rows, :] = part_ref[a, rows, :] * root
        stage_ref[5, rows, :] = res_ref[rows, :] * root
        stage_ref[6, rows, :] = idx_ref[rows, :].astype(F32)
        return 0

    lax.fori_loop(0, TILES // 8, scale, 0, unroll=4)

    def place(g, _):
        for j in range(8):
            t = g * 8 + j
            seat = slot_ref[pixel_ref[t]]
            owner = lax.shift_right_logical(seat, 7)
            rank = count_ref[owner]
            count_ref[owner] = rank + 1
            plan = lax.bitwise_and(rank, 1)
            half = lax.bitwise_and(lax.shift_right_logical(rank, 1), 1)
            position = lax.shift_right_logical(rank, 2)
            block = plan * (2 * OWNERS) + owner * 2 + half
            where_ref[t] = block * SEATS + position
            base = block * BLOCK_ROWS + position * FIELDS
            for f in range(6):
                out_ref[pl.ds(base + f, 1), :] = stage_ref[f, pl.ds(t, 1), :]
            first = (lax.bitwise_and(seat, 127) * SRC).astype(F32)
            out_ref[pl.ds(base + 6, 1), :] = stage_ref[6, pl.ds(t, 1), :] + first
        return 0

    lax.fori_loop(0, TILES // 8, place, 0)


def pack(tile_pixel, pixel_slot, residual, weight, partials, index):
    return pl.pallas_call(
        pack_kernel,
        out_shape=(
            jax.ShapeDtypeStruct((ROWS_IN, 128), F32),
            jax.ShapeDtypeStruct((TILES,), jnp.int32),
        ),
        in_specs=[SMEM, SMEM, VMEM, VMEM, VMEM, VMEM],
        out_specs=(VMEM, SMEM),
        scratch_shapes=[pltpu.SMEM((OWNERS,), jnp.int32), pltpu.VMEM((FIELDS, TILES, 128), F32)],
        compiler_params=params(),
        name="pack",
    )(tile_pixel, pixel_slot, residual, weight, partials, index)


def place_of():
    tm, sky = lax.axis_index("tm"), lax.axis_index("sky")
    return tm // 2, tm % 2, sky // 4, (sky // 2) % 2, sky % 2


def device_of(y, zh, x, zl, c):
    return (y * 2 + zh, x * 4 + zl * 2 + c)


def send(src, dst, sent, landed, device):
    copy = pltpu.make_async_remote_copy(
        src_ref=src, dst_ref=dst, send_sem=sent, recv_sem=landed,
        device_id=device, device_id_type=pl.DeviceIdType.MESH)
    copy.start()
    return copy


def greet(devices):
    barrier = pltpu.get_barrier_semaphore()
    for device in devices:
        pl.semaphore_signal(barrier, inc=1, device_id=device, device_id_type=pl.DeviceIdType.MESH)
    pl.semaphore_wait(barrier, len(devices))


MOVES = [(plan, m % 4, m // 4, dc, h)
         for m in range(8) for plan in range(2) for dc in range(2) for h in range(2)]
OWN = (0, 1, 4, 5)
CHUNK = 4
CHUNKS = SLOTS // CHUNK
PITCH = 136
ROOM = BLOCK_ROWS + 8
HBM = pl.BlockSpec(memory_space=pltpu.HBM)


def routes_of():
    y, zh, x, zl, c = place_of()
    routes = []
    for plan, d, dz, dc, h in MOVES:
        far = ((y if plan else x) + d) % 4
        zl_to, c_to, zh_to = (zl + dz) % 2, (c + dc) % 2, (zh + dz * h) % 2
        to = device_of(far, zh_to, x, zl_to, c_to) if plan else device_of(y, zh_to, far, zl_to, c_to)
        owner = far * 4 + zl_to * 2 + c_to
        routes.append((plan * 2 * OWNERS + owner * 2 + h, to))
    return routes


def pair_products(v, row):
    low5, low4 = row < 5, row < 4
    one = pltpu.roll(v, 1, 0)
    first = jnp.where(low5, v, pltpu.roll(v, 5, 0))
    second = jnp.where(low5, pltpu.roll(v, 7, 0), one)
    third = jnp.where(low4, v, pltpu.roll(v, 4, 0))
    fourth = jnp.where(low4, pltpu.roll(v, 6, 0), one)
    return jnp.concatenate([first * v, first * second, third * fourth], axis=0)


def left_side(v, row):
    products = pair_products(v, row)
    high = products.astype(BF16).astype(F32)
    return jnp.concatenate([high, products - high], axis=0).astype(BF16)


def landing(in_ref, arr_ref, sent, landed, k, to):
    return pltpu.make_async_remote_copy(
        src_ref=in_ref.at[pl.ds(k * BLOCK_ROWS, BLOCK_ROWS)],
        dst_ref=arr_ref.at[pl.ds(k * ROOM, BLOCK_ROWS)], send_sem=sent.at[k], recv_sem=landed.at[k],
        device_id=to, device_id_type=pl.DeviceIdType.MESH)


def gather_kernel(in_ref, att_hbm, w_hbm, knot_ref, first_ref,
                  keep_ref, sums_ref, pix_ref, quad_ref, hits_ref,
                  arr_ref, att_ref, w_ref, spread_ref, sent, landed, local, stored):
    routes = routes_of()
    load_att = pltpu.make_async_copy(att_hbm, att_ref, local.at[4])
    load_w = pltpu.make_async_copy(w_hbm, w_ref, local.at[5])
    load_att.start()
    load_w.start()
    greet([to for k, (_, to) in enumerate(routes) if k not in OWN])
    copies = []
    for k, (block, to) in enumerate(routes):
        if k not in OWN:
            copies.append(send(in_ref.at[pl.ds(block * BLOCK_ROWS, BLOCK_ROWS)],
                               arr_ref.at[pl.ds(k * ROOM, BLOCK_ROWS)], sent.at[k], landed.at[k], to))
    kept = []
    for i, k in enumerate(OWN):
        kept.append(pltpu.make_async_copy(in_ref.at[pl.ds(routes[k][0] * BLOCK_ROWS, BLOCK_ROWS)],
                                          arr_ref.at[pl.ds(k * ROOM, BLOCK_ROWS)], local.at[i]))
        kept[-1].start()

    def clear(g, _):
        spread_ref[pl.ds(pl.multiple_of(g * 8, 8), 8), :] = jnp.zeros((8, 128), F32)
        return 0

    lax.fori_loop(0, 24 * PITCH // 8, clear, 0, unroll=4)

    def clear_sums(g, _):
        for plan in range(2):
            sums_ref[plan, pl.ds(pl.multiple_of(g * 16, 16), 16), :] = jnp.zeros((16, 128), F32)
        return 0

    lax.fori_loop(0, PIX * TERMS // 16, clear_sums, 0, unroll=4)
    load_att.wait()
    load_w.wait()
    quad_sums(knot_ref, first_ref, w_ref, att_ref, quad_ref, hits_ref)
    for move in kept:
        move.wait()
    row = lax.broadcasted_iota(jnp.int32, (8, 128), 0)
    sources = lax.broadcasted_iota(jnp.int32, (128, 128), 0).astype(F32)
    pixels = lax.broadcasted_iota(jnp.int32, (SEATS, 128), 1)
    seat_row = lax.broadcasted_iota(jnp.int32, (SEATS, 128), 0)
    blank = jnp.zeros((48, 128), BF16)

    def keep(k):
        return pltpu.make_async_copy(arr_ref.at[pl.ds(k * ROOM, BLOCK_ROWS)],
                                     keep_ref.at[pl.ds(k * ROOM, BLOCK_ROWS)], stored.at[k])

    def chunk_step(chunk, _):
        plan = chunk % 2
        for i in range(CHUNK):
            k = chunk * CHUNK + i
            arrival = landing(in_ref, arr_ref, sent, landed, k, routes[2][1])
            if i < 2:
                @pl.when(chunk >= 2)
                def _():
                    arrival.wait_recv()
            else:
                arrival.wait_recv()
            keep(k).start()

        def group(g, _):
            for j in range(0, SEATS, 2):
                start = (chunk * CHUNK + g) * ROOM + j * FIELDS
                lefts, hits = [], []
                for i in range(2):
                    v = arr_ref[pl.ds(start + i * FIELDS, 8), :]
                    within = v - jnp.floor(v * (1.0 / SRC)) * SRC
                    lefts.append(left_side(v, row))
                    hits.append((within[6:7, :] == sources).astype(F32).astype(BF16))
                left = jnp.concatenate([jnp.concatenate([lefts[0], blank], axis=1),
                                        jnp.concatenate([blank, lefts[1]], axis=1)], axis=0)
                out = lax.dot_general(left, jnp.concatenate(hits, axis=1), (((1,), (1,)), ((), ())),
                                      preferred_element_type=F32)
                for i in range(2):
                    both = out[48 * i:48 * i + 24] + out[48 * i + 24:48 * i + 48]
                    for n in range(3):
                        spread_ref[pl.ds(8 * n * PITCH + g * SEATS + j + i, 8, stride=PITCH), :] = both[8 * n:8 * n + 8]
            return 0

        lax.fori_loop(0, CHUNK, group, 0)
        places = []
        for i in range(CHUNK):
            k = chunk * CHUNK + i
            whole = arr_ref[pl.ds(k * ROOM + 6, SEATS, stride=FIELDS), :]
            pixel = jnp.floor(whole * (1.0 / SRC)).astype(jnp.int32)
            places.append((pixel == pixels).astype(F32))
            line = jnp.sum(jnp.where(pixels == seat_row, pixel + plan * PIX, 0), axis=0, keepdims=True)
            count = jnp.sum((pixel >= 0).astype(jnp.int32), axis=0, keepdims=True)
            line = jnp.where(pixels[:1] == 127, count, jnp.where(pixels[:1] < SEATS, line, 0))
            pix_ref[pl.ds(k, 1), :] = jnp.maximum(line, 0)
        places.append(jnp.zeros((128 - CHUNK * SEATS, 128), F32))
        place = jnp.concatenate(places, axis=0).T.astype(BF16)
        place = jnp.concatenate([place, place], axis=1)
        for n in range(TERMS):
            at = n + (2 if n >= 6 else 0) + (1 if n >= 13 else 0)
            value = spread_ref[pl.ds(at * PITCH, 128), :]
            high = value.astype(BF16)
            low = (value - high.astype(F32)).astype(BF16)
            added = jnp.dot(place, jnp.concatenate([high, low], axis=0), preferred_element_type=F32)
            for part in range(TIMES):
                rows = pl.ds(part * HROWS + n * HALF, HALF)
                sums_ref[plan, rows, :] = sums_ref[plan, rows, :] + added[part * HALF:(part + 1) * HALF]
        return 0

    lax.fori_loop(0, CHUNKS, chunk_step, 0)
    for copy in copies:
        copy.wait_send()

    def kept_step(k, _):
        keep(k).wait()
        return 0

    lax.fori_loop(0, SLOTS, kept_step, 0)


def gather_tiles(packed, attitude, weight, knots, first):
    return pl.pallas_call(
        gather_kernel,
        out_shape=(
            jax.ShapeDtypeStruct((SLOTS * ROOM, 128), F32),
            jax.ShapeDtypeStruct((2, PIX * TERMS, 128), F32),
            jax.ShapeDtypeStruct((SLOTS, 128), jnp.int32),
            jax.ShapeDtypeStruct((SPAN, 128), F32),
            jax.ShapeDtypeStruct((TILES, 128), BF16),
        ),
        in_specs=[HBM, HBM, HBM, VMEM, SMEM],
        out_specs=(HBM, VMEM, VMEM, VMEM, VMEM),
        scratch_shapes=[
            pltpu.VMEM((SLOTS * ROOM, 128), F32),
            pltpu.VMEM((16, TILES, 128), F32),
            pltpu.VMEM((TILES, 128), F32),
            pltpu.VMEM((24 * PITCH, 128), F32),
            pltpu.SemaphoreType.DMA((SLOTS,)),
            pltpu.SemaphoreType.DMA((SLOTS,)),
            pltpu.SemaphoreType.DMA((6,)),
            pltpu.SemaphoreType.DMA((SLOTS,)),
        ],
        compiler_params=params(collective_id=1, has_side_effects=True),
        name="gather_tiles",
    )(packed, attitude, weight, knots, first)


def damped_solve(entries, target, order):
    factor = {}
    for column in range(order):
        pivot = entries[column, column] + 1.0
        for earlier in range(column):
            pivot = pivot - factor[column, earlier] * factor[column, earlier]
        pivot = jnp.sqrt(pivot)
        factor[column, column] = pivot
        for below in range(column + 1, order):
            current = entries[column, below]
            for earlier in range(column):
                current = current - factor[below, earlier] * factor[column, earlier]
            factor[below, column] = current / pivot
    forward = []
    for column in range(order):
        current = target[column]
        for earlier in range(column):
            current = current - factor[column, earlier] * forward[earlier]
        forward.append(current / factor[column, column])
    answer = [None] * order
    for column in reversed(range(order)):
        current = forward[column]
        for later in range(column + 1, order):
            current = current - factor[later, column] * answer[later]
        answer[column] = current / factor[column, column]
    return answer


def add_rows(out, base, refs, rows):
    def step(g, _):
        at = pl.multiple_of(g * 16, 16)
        total = None
        for ref, start in refs:
            value = ref[pl.ds(start + at, 16), :]
            total = value if total is None else total + value
        out[pl.ds(base + at, 16), :] = total
        return 0

    lax.fori_loop(0, rows // 16, step, 0)


def reduce_kernel(in_ref, table_ref, first_ref, sum_ref, other_ref, whole_ref, own_ref,
                  sent1, landed1, sent2, landed2, sent3, landed3):
    y, zh, x, zl, c = place_of()
    tm = y * 2 + zh
    diagonal = x == y
    greet([device_of((y + dy) % 4, (zh + dz) % 2, (x + dx) % 4, zl, c)
           for dx in range(4) for dy in range(4) for dz in range(2) if (dx, dy, dz) != (0, 0, 0)])
    copies = []
    for d in (2, 1, 3):
        for plan in range(2):
            far = ((x if plan else y) + d) % 4
            to = device_of(y, zh, far, zl, c) if plan else device_of(far, zh, x, zl, c)
            copies.append(send(in_ref.at[plan, pl.ds(far * QROWS, QROWS)], first_ref.at[plan, d - 1],
                               sent1.at[plan, d - 1], landed1.at[plan, d - 1], to))
    for copy in copies:
        copy.wait()
    for plan in range(2):
        near = (x if plan else y) * QROWS
        add_rows(sum_ref.at[plan], 0,
                 [(in_ref.at[plan], near)] + [(first_ref.at[plan, d], 0) for d in range(3)], QROWS)

    @pl.when(diagonal)
    def _():
        add_rows(sum_ref.at[0], 0, [(sum_ref.at[0], 0), (sum_ref.at[1], 0)], QROWS)

    across = send(sum_ref.at[0, pl.ds((1 - zh) * HROWS, HROWS)], other_ref.at[2], sent2.at[2], landed2.at[2],
                  device_of(y, 1 - zh, x, zl, c))

    @pl.when(diagonal)
    def _():
        def clear(g, _):
            other_ref[0, pl.ds(pl.multiple_of(g * 16, 16), 16), :] = jnp.zeros((16, 128), F32)
            other_ref[1, pl.ds(pl.multiple_of(g * 16, 16), 16), :] = jnp.zeros((16, 128), F32)
            return 0

        lax.fori_loop(0, HROWS // 16, clear, 0)

    @pl.when(jnp.logical_not(diagonal))
    def _():
        flips = [send(sum_ref.at[1, pl.ds(z * HROWS, HROWS)], other_ref.at[zh], sent2.at[z], landed2.at[zh],
                      device_of(x, z, y, zl, c)) for z in range(2)]
        for z, flip in enumerate(flips):
            flip.wait_send()
            pltpu.make_async_remote_copy(
                src_ref=sum_ref.at[1, pl.ds(z * HROWS, HROWS)], dst_ref=other_ref.at[z],
                send_sem=sent2.at[z], recv_sem=landed2.at[z], device_id=device_of(x, z, y, zl, c),
                device_id_type=pl.DeviceIdType.MESH).wait_recv()

    across.wait()
    add_rows(whole_ref, 0, [(sum_ref.at[0], zh * HROWS)] + [(other_ref.at[i], 0) for i in range(3)], HROWS)
    sums = [whole_ref[pl.ds(term * HALF, HALF), :] for term in range(TERMS)]
    entries = {key: sums[at] for key, at in TERM_ROW.items() if key[1] < 5}
    target = [sums[TERM_ROW[a, 5]] for a in range(5)]
    for a, value in enumerate(damped_solve(entries, target, 5)):
        own_ref[pl.ds(a, HALF, stride=5), :] = value
    part = [pl.ds(plan * PIX * 5 + tm * HALF * 5, HALF * 5) for plan in range(2)]
    copies = []
    for d in (2, 1, 3, 0):
        for z in (1, 0):
            if (d, z) != (0, 0):
                copies.append(send(own_ref, table_ref.at[part[0]], sent3.at[0, d * 2 + z], landed3.at[0, d * 2 + z],
                                   device_of((y + d) % 4, (zh + z) % 2, x, zl, c)))
    table_ref[part[0], :] = own_ref[...]

    def spread(d, z):
        return pltpu.make_async_remote_copy(
            src_ref=own_ref, dst_ref=table_ref.at[part[1]], send_sem=sent3.at[1, d * 2 + z],
            recv_sem=landed3.at[1, tm], device_id=device_of(x, (zh + z) % 2, (x + d) % 4, zl, c),
            device_id_type=pl.DeviceIdType.MESH)

    for d in (2, 1, 3, 0):
        for z in (1, 0):
            if (d, z) != (0, 0):
                spread(d, z).start()

    @pl.when(jnp.logical_not(diagonal))
    def _():
        spread(0, 0).start()

    @pl.when(diagonal)
    def _():
        table_ref[part[1], :] = own_ref[...]

    for copy in copies:
        copy.wait()
    for d in range(4):
        for z in range(2):
            if (d, z) != (0, 0):
                spread(d, z).wait_send()

    @pl.when(jnp.logical_not(diagonal))
    def _():
        spread(0, 0).wait_send()

    for i in range(TIMES):
        arrival = pltpu.make_async_remote_copy(
            src_ref=own_ref, dst_ref=table_ref.at[pl.ds(PIX * 5 + i * HALF * 5, HALF * 5)], send_sem=sent3.at[1, 0],
            recv_sem=landed3.at[1, i], device_id=device_of(i // 2, i % 2, y, zl, c),
            device_id_type=pl.DeviceIdType.MESH)

        @pl.when(jnp.logical_or(jnp.logical_not(diagonal), tm != i))
        def _():
            arrival.wait_recv()


def reduce_and_solve(normals):
    return pl.pallas_call(
        reduce_kernel,
        out_shape=jax.ShapeDtypeStruct((2 * PIX * 5 + 8, 128), F32),
        in_specs=[VMEM],
        out_specs=VMEM,
        scratch_shapes=[
            pltpu.VMEM((2, 3, QROWS, 128), F32),
            pltpu.VMEM((2, QROWS, 128), F32),
            pltpu.VMEM((3, HROWS, 128), F32),
            pltpu.VMEM((HROWS, 128), F32),
            pltpu.VMEM((HALF * 5, 128), F32),
            pltpu.SemaphoreType.DMA((2, 3)),
            pltpu.SemaphoreType.DMA((2, 3)),
            pltpu.SemaphoreType.DMA((3,)),
            pltpu.SemaphoreType.DMA((3,)),
            pltpu.SemaphoreType.DMA((2, 8)),
            pltpu.SemaphoreType.DMA((2, 8)),
        ],
        compiler_params=params(collective_id=2, has_side_effects=True),
        name="reduce",
    )(normals)


def knot_hits(knot_row, first):
    lane = lax.broadcasted_iota(jnp.int32, (SPAN, TILES), 0)
    return (lane == knot_row - first).astype(F32)


def split_dot(hits, value):
    high = value.astype(BF16)
    low = (value - high.astype(F32)).astype(BF16)
    return (jnp.dot(hits, high, preferred_element_type=F32)
            + jnp.dot(hits, low, preferred_element_type=F32))


def quad_sums(knot_ref, first_ref, w_ref, att_ref, out_ref, hits_ref):
    hits = knot_hits(knot_ref[...], first_ref[0])
    flipped = hits.T
    hits_ref[...] = jnp.concatenate([flipped] * 3 + [jnp.zeros_like(flipped)], axis=1).astype(BF16)
    hits = hits.astype(BF16)
    lane = lax.broadcasted_iota(jnp.int32, (SPAN, 128), 1)
    total = jnp.zeros((SPAN, 128), F32)
    weight = w_ref[...]
    for m in range(4):
        for c in range(4):
            scaled = weight * att_ref[4 * m + c]
            for e in range(c, 4):
                sums = split_dot(hits, scaled * att_ref[4 * m + e])
                at = 14 * m + KNOT_PAIRS.index((c, e))
                total = total + jnp.where(lane == at, jnp.sum(sums, axis=1, keepdims=True), 0.0)
    out_ref[...] = total


def apply_kernel(pix_ref, where_ref, first_ref, tiles_hbm, table_ref, knot_ref, w_ref, att_hbm, quad_ref, hits_ref,
                 out_ref, attitude_ref, arr_ref, fixed_ref, back_ref, att_ref,
                 settled_ref, edge_ref, head_ref, next_ref, piece_ref, pieces_ref,
                 sent, landed, loaded, given, taken):
    tm, sky = lax.axis_index("tm"), lax.axis_index("sky")
    y, zh, x, zl, c0 = place_of()
    block = tm * OWNERS + sky
    after = ((block + 1) // OWNERS % TIMES, (block + 1) % OWNERS)
    before = ((block + 127) // OWNERS % TIMES, (block + 127) % OWNERS)
    has_after, has_before = block < TIMES * OWNERS - 1, block > 0
    peers = [(tm, (sky + d) % OWNERS) for d in range(1, OWNERS)]
    parts = 8
    size = SLOTS // parts * ROOM

    def load(part):
        rows = pl.ds(part * size, size)
        return pltpu.make_async_copy(tiles_hbm.at[rows], arr_ref.at[rows], loaded.at[part])

    for part in range(parts):
        load(part).start()
    load_att = pltpu.make_async_copy(att_hbm, att_ref, loaded.at[parts])
    load_att.start()
    edge_ref[1] = jnp.zeros((8, 128), F32)
    next_ref[...] = jnp.zeros((4, 8, 128), F32)
    greet(peers + [after, before] + [to for k, (_, to) in enumerate(routes_of()) if k not in OWN])

    def give(k):
        m, plan, dc, h = k // 8, k // 4 % 2, k // 2 % 2, k % 2
        d, dz = m % 4, m // 4
        far = ((1 - plan) * x + plan * y + 4 - d) % 4
        y_to, x_to = (1 - plan) * y + plan * far, (1 - plan) * far + plan * x
        to = device_of(y_to, (zh + dz * h) % 2, x_to, (zl + dz) % 2, (c0 + dc) % 2)
        seat = plan * 2 * OWNERS + (((1 - plan) * x + plan * y) * 4 + zl * 2 + c0) * 2 + h
        return pltpu.make_async_remote_copy(
            src_ref=fixed_ref.at[pl.ds(k * SEATS, SEATS)], dst_ref=back_ref.at[pl.ds(seat * SEATS, SEATS)],
            send_sem=given.at[k], recv_sem=taken.at[k], device_id=to, device_id_type=pl.DeviceIdType.MESH), seat

    def is_own(k):
        return jnp.logical_and(k < 8, k // 2 % 2 == 0)

    def pass_on(k):
        copy, seat = give(k)

        @pl.when(jnp.logical_not(is_own(k)))
        def _():
            copy.start()

        @pl.when(is_own(k))
        def _():
            back_ref[pl.ds(seat * SEATS, SEATS), :] = fixed_ref[pl.ds(k * SEATS, SEATS), :]

    row = lax.broadcasted_iota(jnp.int32, (8, 128), 0)

    def pick(k, _):
        @pl.when(k % (SLOTS // parts) == 0)
        def _():
            load(k // (SLOTS // parts)).wait()

        for j in range(SEATS):
            v = arr_ref[pl.ds(k * ROOM + j * FIELDS, 8), :]
            table = table_ref[pl.ds(pix_ref[k, j] * 5, 8), :]
            within = (v - jnp.floor(v * (1.0 / SRC)) * SRC).astype(jnp.int32)
            at = jnp.broadcast_to(lax.bitwise_and(within[6:7, :], 127), (8, 128))
            picked = jnp.take_along_axis(table, at, axis=1)
            terms = jnp.where(row < 5, v * picked, jnp.where(row == 5, -v, 0.0))
            fixed_ref[pl.ds(k * SEATS + j, 1), :] = -jnp.sum(terms, axis=0, keepdims=True)

        @pl.when(k > 0)
        def _():
            pass_on(k - 1)

        return 0

    lax.fori_loop(0, SLOTS, pick, 0)
    pass_on(SLOTS - 1)
    load_att.wait()

    def settle(k, _):
        @pl.when(jnp.logical_not(is_own(k)))
        def _():
            give(k)[0].wait()

        return 0

    lax.fori_loop(0, SLOTS, settle, 0)

    def fetch(g, _):
        for j in range(16):
            t = g * 16 + j
            settled_ref[pl.ds(t, 1), :] = back_ref[pl.ds(where_ref[t], 1), :]
        return 0

    lax.fori_loop(0, TILES // 16, fetch, 0)
    weight = w_ref[...]
    settled = settled_ref[...] / jnp.sqrt(weight)
    settled_ref[...] = settled
    hits = knot_hits(knot_ref[...], first_ref[0]).astype(BF16)
    lane = lax.broadcasted_iota(jnp.int32, (SPAN, 128), 1)
    total = quad_ref[...]
    scaled = weight * settled
    for m in range(4):
        for c in range(4):
            sums = split_dot(hits, scaled * att_ref[4 * m + c])
            at = 14 * m + 10 + c
            total = total + jnp.where(lane == at, jnp.sum(sums, axis=1, keepdims=True), 0.0)
    lane40 = lax.broadcasted_iota(jnp.int32, (SPAN + 8, 128), 1)
    padded = jnp.concatenate([total, jnp.zeros((8, 128), F32)], axis=0)
    moved = jnp.where(lane40 < 14, padded, 0.0)
    for m in range(1, 4):
        shifted = pltpu.roll(pltpu.roll(padded, m, 0), 128 - 14 * m, 1)
        moved = moved + jnp.where(lane40 < 14, shifted, 0.0)
    edge_ref[0] = moved[SPAN:]
    def onward(to):
        return pltpu.make_async_remote_copy(
            src_ref=edge_ref.at[0], dst_ref=edge_ref.at[1], send_sem=sent.at[0], recv_sem=landed.at[0],
            device_id=to, device_id_type=pl.DeviceIdType.MESH)

    def backward(to):
        return pltpu.make_async_remote_copy(
            src_ref=head_ref, dst_ref=next_ref, send_sem=sent.at[1], recv_sem=landed.at[1],
            device_id=to, device_id_type=pl.DeviceIdType.MESH)

    @pl.when(has_after)
    def _():
        onward(after).start()

    @pl.when(has_before)
    def _():
        onward(before).wait_recv()

    sums = jnp.concatenate([moved[:8] + edge_ref[1], moved[8:SPAN]], axis=0)

    def column(at):
        return jnp.broadcast_to(sums[:, at:at + 1], (SPAN, 128))

    entries = {pair: column(n) for n, pair in enumerate(KNOT_PAIRS)}
    answer = damped_solve(entries, [column(10 + c) for c in range(4)], 4)
    for c in range(4):
        head_ref[c] = answer[c][:8]

    @pl.when(has_before)
    def _():
        backward(before).start()

    row32 = lax.broadcasted_iota(jnp.int32, (SPAN, 128), 0)
    row8 = lax.broadcasted_iota(jnp.int32, (8, 128), 0)
    piece = jnp.zeros((8, 128), F32)
    for c in range(4):
        line = jnp.sum(jnp.where(lane == row32 + (sky % 4) * SPAN, answer[c], 0.0), axis=0, keepdims=True)
        piece = jnp.where(row8 == c, line, piece)
    piece_ref[...] = piece
    copies = [send(piece_ref, pieces_ref.at[sky], sent.at[1 + d], landed.at[1 + d], peers[d - 1])
              for d in range(1, OWNERS)]
    pieces_ref[sky] = piece

    @pl.when(has_after)
    def _():
        backward(after).wait_recv()

    fix = None
    for m in range(4):
        for c in range(4):
            both = jnp.concatenate([answer[c], next_ref[c]], axis=0)
            value = both[m:m + SPAN]
            high = value.astype(BF16)
            rest = value - high.astype(F32)
            middle = rest.astype(BF16)
            low = (rest - middle.astype(F32)).astype(BF16)
            table = jnp.concatenate([high, middle, low, jnp.zeros_like(high)], axis=0)
            term = att_ref[4 * m + c] * jnp.dot(hits_ref[...], table, preferred_element_type=F32)
            fix = term if fix is None else fix + term
    out_ref[...] = settled_ref[...] - fix
    for copy in copies:
        copy.wait()
    for j in range(4):
        total = pieces_ref[4 * j]
        for i in range(1, 4):
            total = total + pieces_ref[4 * j + i]
        attitude_ref[:, j * 128:(j + 1) * 128] = total[:4]

    @pl.when(has_after)
    def _():
        onward(after).wait_send()

    @pl.when(has_before)
    def _():
        backward(before).wait_send()


def apply_updates(pix, where, first, tiles, table, knots, weight, attitude, quad, hits):
    return pl.pallas_call(
        apply_kernel,
        out_shape=(
            jax.ShapeDtypeStruct((TILES, 128), F32),
            jax.ShapeDtypeStruct((4, SPAN * OWNERS), F32),
        ),
        in_specs=[SMEM, SMEM, SMEM, HBM, VMEM, VMEM, VMEM, HBM, VMEM, VMEM],
        out_specs=(VMEM, VMEM),
        scratch_shapes=[
            pltpu.VMEM((SLOTS * ROOM, 128), F32),
            pltpu.VMEM((SLOTS * SEATS, 128), F32),
            pltpu.VMEM((SLOTS * SEATS, 128), F32),
            pltpu.VMEM((16, TILES, 128), F32),
            pltpu.VMEM((TILES, 128), F32),
            pltpu.VMEM((2, 8, 128), F32),
            pltpu.VMEM((4, 8, 128), F32),
            pltpu.VMEM((4, 8, 128), F32),
            pltpu.VMEM((8, 128), F32),
            pltpu.VMEM((OWNERS, 8, 128), F32),
            pltpu.SemaphoreType.DMA((OWNERS + 1,)),
            pltpu.SemaphoreType.DMA((OWNERS + 1,)),
            pltpu.SemaphoreType.DMA((9,)),
            pltpu.SemaphoreType.DMA((SLOTS,)),
            pltpu.SemaphoreType.DMA((SLOTS,)),
        ],
        compiler_params=params(collective_id=4, has_side_effects=True),
        name="apply_updates",
    )(pix, where, first, tiles, table, knots, weight, attitude, quad, hits)


def emit_kernel(final_ref, attitude_ref, table_ref, final_out, attitude_out, update_out):
    final_out[...] = final_ref[...]
    attitude_out[...] = attitude_ref[...]
    for p in range(PIX):
        update_out[:, p * 128:(p + 1) * 128] = table_ref[p * 5:p * 5 + 5, :]


def emit(final, attitude, table):
    return pl.pallas_call(
        emit_kernel,
        out_shape=(
            jax.ShapeDtypeStruct((TILES, 128), F32),
            jax.ShapeDtypeStruct((4, SPAN * OWNERS), F32),
            jax.ShapeDtypeStruct((5, PIX * SRC), F32),
        ),
        in_specs=[VMEM, VMEM, VMEM],
        out_specs=(VMEM, VMEM, VMEM),
        compiler_params=params(),
        name="emit",
    )(final, attitude, table)


def body(residual, obs_weight, source_partials, attitude_partials, source_index,
         tile_pixel, tile_knot, pixel_slot):
    block = lax.axis_index("tm") * OWNERS + lax.axis_index("sky")
    first = (block * SPAN).reshape(1)
    knots = tile_knot.reshape(1, TILES)
    packed, where = pack(tile_pixel, pixel_slot, residual, obs_weight, source_partials, source_index)
    arrived, normals, pix, quad, hits = gather_tiles(packed, attitude_partials, obs_weight, knots, first)
    table = reduce_and_solve(normals)
    final, attitude_update = apply_updates(
        pix, where, first, arrived, table, knots, obs_weight, attitude_partials, quad, hits)
    final, attitude_update, source_update = emit(final, attitude_update, table)
    return final, source_update, attitude_update


def solution(mesh):
    in_specs = (
        P(("tm", "sky"), None),
        P(("tm", "sky"), None),
        P(None, ("tm", "sky"), None),
        P(None, ("tm", "sky"), None),
        P(("tm", "sky"), None),
        P(("tm", "sky")),
        P(("tm", "sky")),
        P(),
    )
    out_specs = (P(("tm", "sky"), None), P(None, "sky"), P(None, "tm"))
    return jax.shard_map(body, mesh=mesh, in_specs=in_specs, out_specs=out_specs, check_vma=False)
```

```python
import jax
import jax.numpy as jnp
from jax import lax
from jax.experimental import pallas as pl
from jax.experimental.pallas import tpu as pltpu
from jax.sharding import PartitionSpec as P

TILES = 512
OWNERS = 16
TIMES = 8
CAP = 96
PIX = 128
SRC = 128
FIELDS = 7
CLASSES = 2
SEATS = CAP // CLASSES
SLOTS = OWNERS * CLASSES
BLOCK_ROWS = SEATS * FIELDS
ROWS_IN = SLOTS * BLOCK_ROWS + 8
SPAN = 32
TERMS = 20
HALF = PIX // TIMES
HROWS = HALF * TERMS
KNOT_PAIRS = tuple((c, e) for c in range(4) for e in range(c, 4))
TERM_ROW = {
    (0, 0): 0, (1, 1): 1, (2, 2): 2, (3, 3): 3, (4, 4): 4, (0, 5): 5,
    (0, 1): 6, (1, 2): 7, (2, 3): 8, (3, 4): 9, (4, 5): 10, (0, 4): 11, (1, 5): 12,
    (0, 2): 13, (1, 3): 14, (2, 4): 15, (3, 5): 16, (0, 3): 17, (1, 4): 18, (2, 5): 19,
}
VMEM = pl.BlockSpec(memory_space=pltpu.VMEM)
SMEM = pl.BlockSpec(memory_space=pltpu.SMEM)
F32 = jnp.float32
BF16 = jnp.bfloat16


def params(**kw):
    return pltpu.CompilerParams(vmem_limit_bytes=60 * 1024 * 1024, **kw)


def pack_kernel(pixel_ref, slot_ref, res_ref, w_ref, part_ref, idx_ref,
                out_ref, where_ref, count_ref, stage_ref):
    for o in range(OWNERS):
        count_ref[o] = 0
    nothing = jnp.zeros((SEATS, 128), F32)

    def clear(b, _):
        base = pl.multiple_of(b * BLOCK_ROWS, 8)
        for i in range(FIELDS):
            out_ref[pl.ds(base + i * SEATS, SEATS), :] = nothing
        out_ref[pl.ds(base + 6, SEATS, stride=FIELDS), :] = nothing - 1.0
        return 0

    lax.fori_loop(0, SLOTS, clear, 0)

    def scale(g, _):
        rows = pl.ds(pl.multiple_of(g * 8, 8), 8)
        root = jnp.sqrt(w_ref[rows, :])
        for a in range(5):
            stage_ref[a, rows, :] = part_ref[a, rows, :] * root
        stage_ref[5, rows, :] = res_ref[rows, :] * root
        stage_ref[6, rows, :] = idx_ref[rows, :].astype(F32)
        return 0

    lax.fori_loop(0, TILES // 8, scale, 0, unroll=4)

    def place(g, _):
        for j in range(8):
            t = g * 8 + j
            seat = slot_ref[pixel_ref[t]]
            owner = lax.shift_right_logical(seat, 7)
            rank = count_ref[owner]
            count_ref[owner] = rank + 1
            block = owner * CLASSES + lax.bitwise_and(rank, 1)
            position = lax.shift_right_logical(rank, 1)
            where_ref[t] = block * SEATS + position
            base = block * BLOCK_ROWS + position * FIELDS
            for f in range(6):
                out_ref[pl.ds(base + f, 1), :] = stage_ref[f, pl.ds(t, 1), :]
            first = (lax.bitwise_and(seat, 127) * SRC).astype(F32)
            out_ref[pl.ds(base + 6, 1), :] = stage_ref[6, pl.ds(t, 1), :] + first
        return 0

    lax.fori_loop(0, TILES // 8, place, 0)


def pack(tile_pixel, pixel_slot, residual, weight, partials, index):
    return pl.pallas_call(
        pack_kernel,
        out_shape=(
            jax.ShapeDtypeStruct((ROWS_IN, 128), F32),
            jax.ShapeDtypeStruct((TILES,), jnp.int32),
        ),
        in_specs=[SMEM, SMEM, VMEM, VMEM, VMEM, VMEM],
        out_specs=(VMEM, SMEM),
        scratch_shapes=[pltpu.SMEM((OWNERS,), jnp.int32), pltpu.VMEM((FIELDS, TILES, 128), F32)],
        compiler_params=params(),
        name="pack",
    )(tile_pixel, pixel_slot, residual, weight, partials, index)


def place_of():
    tm, sky = lax.axis_index("tm"), lax.axis_index("sky")
    return tm // 2, tm % 2, sky // 4, (sky // 2) % 2, sky % 2


def device_of(y, zh, x, zl, c):
    return (y * 2 + zh, x * 4 + zl * 2 + c)


def send(src, dst, sent, landed, device):
    copy = pltpu.make_async_remote_copy(
        src_ref=src, dst_ref=dst, send_sem=sent, recv_sem=landed,
        device_id=device, device_id_type=pl.DeviceIdType.MESH)
    copy.start()
    return copy


def greet(devices):
    barrier = pltpu.get_barrier_semaphore()
    for device in devices:
        pl.semaphore_signal(barrier, inc=1, device_id=device, device_id_type=pl.DeviceIdType.MESH)
    pl.semaphore_wait(barrier, len(devices))


MOVES = [(m % 4, m // 4, dc, h) for m in range(8) for dc in range(2) for h in range(2)]
OWN = (0, 1)
CHUNK = 2
CHUNKS = SLOTS // CHUNK
STEP = 24
PITCH = 136
ROOM = BLOCK_ROWS + 8
HBM = pl.BlockSpec(memory_space=pltpu.HBM)


def routes_of():
    y, zh, x, zl, c = place_of()
    routes = []
    for d, dz, dc, h in MOVES:
        far, zl_to, c_to = (x + d) % 4, (zl + dz) % 2, (c + dc) % 2
        owner = far * 4 + zl_to * 2 + c_to
        routes.append((owner * CLASSES + h, device_of(y, (zh + dz * h) % 2, far, zl_to, c_to)))
    return routes


def pair_products(v, row):
    low5, low4 = row < 5, row < 4
    one = pltpu.roll(v, 1, 0)
    first = jnp.where(low5, v, pltpu.roll(v, 5, 0))
    second = jnp.where(low5, pltpu.roll(v, 7, 0), one)
    third = jnp.where(low4, v, pltpu.roll(v, 4, 0))
    fourth = jnp.where(low4, pltpu.roll(v, 6, 0), one)
    return jnp.concatenate([first * v, first * second, third * fourth], axis=0)


def left_side(v, row):
    products = pair_products(v, row)
    high = products.astype(BF16).astype(F32)
    return jnp.concatenate([high, products - high], axis=0).astype(BF16)


def landing(in_ref, arr_ref, sent, landed, k, to):
    return pltpu.make_async_remote_copy(
        src_ref=in_ref.at[pl.ds(k * BLOCK_ROWS, BLOCK_ROWS)],
        dst_ref=arr_ref.at[pl.ds(k * ROOM, BLOCK_ROWS)], send_sem=sent.at[k], recv_sem=landed.at[k],
        device_id=to, device_id_type=pl.DeviceIdType.MESH)


def gather_kernel(in_ref, att_hbm, w_hbm, knot_ref, first_ref,
                  keep_ref, sums_ref, pix_ref, quad_ref, hits_ref,
                  arr_ref, att_ref, w_ref, spread_ref, sent, landed, local, stored):
    routes = routes_of()
    load_att = pltpu.make_async_copy(att_hbm, att_ref, local.at[4])
    load_w = pltpu.make_async_copy(w_hbm, w_ref, local.at[5])
    load_att.start()
    load_w.start()
    greet([to for k, (_, to) in enumerate(routes) if k not in OWN])
    copies = []
    for k, (block, to) in enumerate(routes):
        if k not in OWN:
            copies.append(send(in_ref.at[pl.ds(block * BLOCK_ROWS, BLOCK_ROWS)],
                               arr_ref.at[pl.ds(k * ROOM, BLOCK_ROWS)], sent.at[k], landed.at[k], to))
    kept = []
    for i, k in enumerate(OWN):
        kept.append(pltpu.make_async_copy(in_ref.at[pl.ds(routes[k][0] * BLOCK_ROWS, BLOCK_ROWS)],
                                          arr_ref.at[pl.ds(k * ROOM, BLOCK_ROWS)], local.at[i]))
        kept[-1].start()

    def clear(g, _):
        spread_ref[pl.ds(pl.multiple_of(g * 8, 8), 8), :] = jnp.zeros((8, 128), F32)
        return 0

    lax.fori_loop(0, 24 * PITCH // 8, clear, 0, unroll=4)

    def clear_sums(g, _):
        sums_ref[pl.ds(pl.multiple_of(g * 16, 16), 16), :] = jnp.zeros((16, 128), F32)
        return 0

    lax.fori_loop(0, PIX * TERMS // 16, clear_sums, 0, unroll=4)
    load_att.wait()
    load_w.wait()
    quad_sums(knot_ref, first_ref, w_ref, att_ref, quad_ref, hits_ref)
    for move in kept:
        move.wait()
    row = lax.broadcasted_iota(jnp.int32, (8, 128), 0)
    sources = lax.broadcasted_iota(jnp.int32, (128, 128), 0).astype(F32)
    pixels = lax.broadcasted_iota(jnp.int32, (SEATS, 128), 1)
    seat_row = lax.broadcasted_iota(jnp.int32, (SEATS, 128), 0)
    blank = jnp.zeros((48, 128), BF16)

    def keep(k):
        return pltpu.make_async_copy(arr_ref.at[pl.ds(k * ROOM, BLOCK_ROWS)],
                                     keep_ref.at[pl.ds(k * ROOM, BLOCK_ROWS)], stored.at[k])

    def chunk_step(chunk, _):
        for i in range(CHUNK):
            k = chunk * CHUNK + i
            arrival = landing(in_ref, arr_ref, sent, landed, k, routes[2][1])

            @pl.when(chunk >= 1)
            def _():
                arrival.wait_recv()

            keep(k).start()

        def group(g, _):
            for j in range(0, STEP, 2):
                start = (chunk * CHUNK + g // 2) * ROOM + (g % 2 * STEP + j) * FIELDS
                lefts, hits = [], []
                for i in range(2):
                    v = arr_ref[pl.ds(start + i * FIELDS, 8), :]
                    within = v - jnp.floor(v * (1.0 / SRC)) * SRC
                    lefts.append(left_side(v, row))
                    hits.append((within[6:7, :] == sources).astype(F32).astype(BF16))
                left = jnp.concatenate([jnp.concatenate([lefts[0], blank], axis=1),
                                        jnp.concatenate([blank, lefts[1]], axis=1)], axis=0)
                out = lax.dot_general(left, jnp.concatenate(hits, axis=1), (((1,), (1,)), ((), ())),
                                      preferred_element_type=F32)
                for i in range(2):
                    both = out[48 * i:48 * i + 24] + out[48 * i + 24:48 * i + 48]
                    for n in range(3):
                        spread_ref[pl.ds(8 * n * PITCH + g * STEP + j + i, 8, stride=PITCH), :] = both[8 * n:8 * n + 8]
            return 0

        lax.fori_loop(0, CHUNK * SEATS // STEP, group, 0)
        places = []
        for i in range(CHUNK):
            k = chunk * CHUNK + i
            whole = arr_ref[pl.ds(k * ROOM + 6, SEATS, stride=FIELDS), :]
            pixel = jnp.floor(whole * (1.0 / SRC)).astype(jnp.int32)
            places.append((pixel == pixels).astype(F32))
            line = jnp.sum(jnp.where(pixels == seat_row, pixel, 0), axis=0, keepdims=True)
            pix_ref[pl.ds(k, 1), :] = jnp.maximum(line, 0)
        places.append(jnp.zeros((128 - CHUNK * SEATS, 128), F32))
        place = jnp.concatenate(places, axis=0).T.astype(BF16)
        place = jnp.concatenate([place, place], axis=1)
        for n in range(TERMS):
            at = n + (2 if n >= 6 else 0) + (1 if n >= 13 else 0)
            value = spread_ref[pl.ds(at * PITCH, 128), :]
            high = value.astype(BF16)
            low = (value - high.astype(F32)).astype(BF16)
            added = jnp.dot(place, jnp.concatenate([high, low], axis=0), preferred_element_type=F32)
            for part in range(TIMES):
                rows = pl.ds(part * HROWS + n * HALF, HALF)
                sums_ref[rows, :] = sums_ref[rows, :] + added[part * HALF:(part + 1) * HALF]
        return 0

    lax.fori_loop(0, CHUNKS, chunk_step, 0)
    for copy in copies:
        copy.wait_send()

    def kept_step(k, _):
        keep(k).wait()
        return 0

    lax.fori_loop(0, SLOTS, kept_step, 0)


def gather_tiles(packed, attitude, weight, knots, first):
    return pl.pallas_call(
        gather_kernel,
        out_shape=(
            jax.ShapeDtypeStruct((SLOTS * ROOM, 128), F32),
            jax.ShapeDtypeStruct((PIX * TERMS, 128), F32),
            jax.ShapeDtypeStruct((SLOTS, 128), jnp.int32),
            jax.ShapeDtypeStruct((SPAN, 128), F32),
            jax.ShapeDtypeStruct((TILES, 128), BF16),
        ),
        in_specs=[HBM, HBM, HBM, VMEM, SMEM],
        out_specs=(HBM, VMEM, VMEM, VMEM, VMEM),
        scratch_shapes=[
            pltpu.VMEM((SLOTS * ROOM, 128), F32),
            pltpu.VMEM((16, TILES, 128), F32),
            pltpu.VMEM((TILES, 128), F32),
            pltpu.VMEM((24 * PITCH, 128), F32),
            pltpu.SemaphoreType.DMA((SLOTS,)),
            pltpu.SemaphoreType.DMA((SLOTS,)),
            pltpu.SemaphoreType.DMA((6,)),
            pltpu.SemaphoreType.DMA((SLOTS,)),
        ],
        compiler_params=params(collective_id=1, has_side_effects=True),
        name="gather_tiles",
    )(packed, attitude, weight, knots, first)


def damped_solve(entries, target, order):
    factor = {}
    for column in range(order):
        pivot = entries[column, column] + 1.0
        for earlier in range(column):
            pivot = pivot - factor[column, earlier] * factor[column, earlier]
        pivot = jnp.sqrt(pivot)
        factor[column, column] = pivot
        for below in range(column + 1, order):
            current = entries[column, below]
            for earlier in range(column):
                current = current - factor[below, earlier] * factor[column, earlier]
            factor[below, column] = current / pivot
    forward = []
    for column in range(order):
        current = target[column]
        for earlier in range(column):
            current = current - factor[column, earlier] * forward[earlier]
        forward.append(current / factor[column, column])
    answer = [None] * order
    for column in reversed(range(order)):
        current = forward[column]
        for later in range(column + 1, order):
            current = current - factor[later, column] * answer[later]
        answer[column] = current / factor[column, column]
    return answer


def reduce_kernel(in_ref, table_ref, parts_ref, whole_ref, own_ref, sent1, landed1, sent2, landed2):
    y, zh, x, zl, c = place_of()
    tm = y * 2 + zh
    peers = [((y + d) % 4, (zh + z) % 2) for d, z in ((2, 1), (2, 0), (1, 1), (3, 1), (1, 0), (3, 0), (0, 1))]
    devices = [device_of(to_y, to_zh, x, zl, c) for to_y, to_zh in peers]
    greet(devices)
    copies = []
    for i, (to_y, to_zh) in enumerate(peers):
        copies.append(send(in_ref.at[pl.ds((to_y * 2 + to_zh) * HROWS, HROWS)], parts_ref.at[i],
                           sent1.at[i], landed1.at[i], devices[i]))
    for copy in copies:
        copy.wait()

    def add(g, _):
        rows = pl.ds(pl.multiple_of(g * 16, 16), 16)
        total = in_ref[pl.ds(tm * HROWS + pl.multiple_of(g * 16, 16), 16), :]
        for i in range(TIMES - 1):
            total = total + parts_ref[i, rows, :]
        whole_ref[rows, :] = total
        return 0

    lax.fori_loop(0, TERMS, add, 0, unroll=4)
    sums = [whole_ref[pl.ds(term * HALF, HALF), :] for term in range(TERMS)]
    entries = {key: sums[at] for key, at in TERM_ROW.items() if key[1] < 5}
    target = [sums[TERM_ROW[a, 5]] for a in range(5)]
    for a, value in enumerate(damped_solve(entries, target, 5)):
        own_ref[pl.ds(a, HALF, stride=5), :] = value
    part = pl.ds(tm * HALF * 5, HALF * 5)
    table_ref[part, :] = own_ref[...]
    copies = [send(own_ref, table_ref.at[part], sent2.at[i], landed2.at[i], device)
              for i, device in enumerate(devices)]
    for copy in copies:
        copy.wait()


def reduce_and_solve(normals):
    return pl.pallas_call(
        reduce_kernel,
        out_shape=jax.ShapeDtypeStruct((PIX * 5 + 8, 128), F32),
        in_specs=[VMEM],
        out_specs=VMEM,
        scratch_shapes=[
            pltpu.VMEM((TIMES - 1, HROWS, 128), F32),
            pltpu.VMEM((HROWS, 128), F32),
            pltpu.VMEM((HALF * 5, 128), F32),
            pltpu.SemaphoreType.DMA((TIMES - 1,)),
            pltpu.SemaphoreType.DMA((TIMES - 1,)),
            pltpu.SemaphoreType.DMA((TIMES - 1,)),
            pltpu.SemaphoreType.DMA((TIMES - 1,)),
        ],
        compiler_params=params(collective_id=2, has_side_effects=True),
        name="reduce",
    )(normals)


def knot_hits(knot_row, first):
    lane = lax.broadcasted_iota(jnp.int32, (SPAN, TILES), 0)
    return (lane == knot_row - first).astype(F32)


def split_dot(hits, value):
    high = value.astype(BF16)
    low = (value - high.astype(F32)).astype(BF16)
    return (jnp.dot(hits, high, preferred_element_type=F32)
            + jnp.dot(hits, low, preferred_element_type=F32))


def quad_sums(knot_ref, first_ref, w_ref, att_ref, out_ref, hits_ref):
    hits = knot_hits(knot_ref[...], first_ref[0])
    flipped = hits.T
    hits_ref[...] = jnp.concatenate([flipped] * 3 + [jnp.zeros_like(flipped)], axis=1).astype(BF16)
    hits = hits.astype(BF16)
    lane = lax.broadcasted_iota(jnp.int32, (SPAN, 128), 1)
    total = jnp.zeros((SPAN, 128), F32)
    weight = w_ref[...]
    for m in range(4):
        for c in range(4):
            scaled = weight * att_ref[4 * m + c]
            for e in range(c, 4):
                sums = split_dot(hits, scaled * att_ref[4 * m + e])
                at = 14 * m + KNOT_PAIRS.index((c, e))
                total = total + jnp.where(lane == at, jnp.sum(sums, axis=1, keepdims=True), 0.0)
    out_ref[...] = total


def apply_kernel(pix_ref, where_ref, first_ref, tiles_hbm, table_ref, knot_ref, w_ref, att_hbm, quad_ref, hits_ref,
                 out_ref, attitude_ref, arr_ref, fixed_ref, back_ref, att_ref,
                 settled_ref, edge_ref, head_ref, next_ref, piece_ref, pieces_ref,
                 sent, landed, loaded, given, taken):
    tm, sky = lax.axis_index("tm"), lax.axis_index("sky")
    y, zh, x, zl, c0 = place_of()
    block = tm * OWNERS + sky
    after = ((block + 1) // OWNERS % TIMES, (block + 1) % OWNERS)
    before = ((block + 127) // OWNERS % TIMES, (block + 127) % OWNERS)
    has_after, has_before = block < TIMES * OWNERS - 1, block > 0
    peers = [(tm, (sky + d) % OWNERS) for d in range(1, OWNERS)]
    parts = 8
    size = SLOTS // parts * ROOM

    def load(part):
        rows = pl.ds(part * size, size)
        return pltpu.make_async_copy(tiles_hbm.at[rows], arr_ref.at[rows], loaded.at[part])

    for part in range(parts):
        load(part).start()
    load_att = pltpu.make_async_copy(att_hbm, att_ref, loaded.at[parts])
    load_att.start()
    edge_ref[1] = jnp.zeros((8, 128), F32)
    next_ref[...] = jnp.zeros((4, 8, 128), F32)
    greet(peers + [after, before] + [to for k, (_, to) in enumerate(routes_of()) if k not in OWN])

    def give(k):
        m, dc, h = k // 4, k // 2 % 2, k % 2
        dz = m // 4
        to = device_of(y, (zh + dz * h) % 2, (x + 4 - m % 4) % 4, (zl + dz) % 2, (c0 + dc) % 2)
        seat = sky * CLASSES + h
        return pltpu.make_async_remote_copy(
            src_ref=fixed_ref.at[pl.ds(k * SEATS, SEATS)], dst_ref=back_ref.at[pl.ds(seat * SEATS, SEATS)],
            send_sem=given.at[k], recv_sem=taken.at[k], device_id=to, device_id_type=pl.DeviceIdType.MESH), seat

    def is_own(k):
        return k < 2

    def pass_on(k):
        copy, seat = give(k)

        @pl.when(jnp.logical_not(is_own(k)))
        def _():
            copy.start()

        @pl.when(is_own(k))
        def _():
            back_ref[pl.ds(seat * SEATS, SEATS), :] = fixed_ref[pl.ds(k * SEATS, SEATS), :]

    row = lax.broadcasted_iota(jnp.int32, (8, 128), 0)

    def pick(step, _):
        k, first = step // 2, step % 2 * STEP

        @pl.when(step % (2 * SLOTS // parts) == 0)
        def _():
            load(step // (2 * SLOTS // parts)).wait()

        for j in range(STEP):
            v = arr_ref[pl.ds(k * ROOM + (first + j) * FIELDS, 8), :]
            table = table_ref[pl.ds(pix_ref[k, first + j] * 5, 8), :]
            within = (v - jnp.floor(v * (1.0 / SRC)) * SRC).astype(jnp.int32)
            at = jnp.broadcast_to(lax.bitwise_and(within[6:7, :], 127), (8, 128))
            picked = jnp.take_along_axis(table, at, axis=1)
            terms = jnp.where(row < 5, v * picked, jnp.where(row == 5, -v, 0.0))
            fixed_ref[pl.ds(k * SEATS + first + j, 1), :] = -jnp.sum(terms, axis=0, keepdims=True)

        @pl.when(jnp.logical_and(first == 0, k > 0))
        def _():
            pass_on(k - 1)

        return 0

    lax.fori_loop(0, 2 * SLOTS, pick, 0)
    pass_on(SLOTS - 1)
    load_att.wait()

    def settle(k, _):
        @pl.when(jnp.logical_not(is_own(k)))
        def _():
            give(k)[0].wait()

        return 0

    lax.fori_loop(0, SLOTS, settle, 0)

    def fetch(g, _):
        for j in range(16):
            t = g * 16 + j
            settled_ref[pl.ds(t, 1), :] = back_ref[pl.ds(where_ref[t], 1), :]
        return 0

    lax.fori_loop(0, TILES // 16, fetch, 0)
    weight = w_ref[...]
    settled = settled_ref[...] / jnp.sqrt(weight)
    settled_ref[...] = settled
    hits = knot_hits(knot_ref[...], first_ref[0]).astype(BF16)
    lane = lax.broadcasted_iota(jnp.int32, (SPAN, 128), 1)
    total = quad_ref[...]
    scaled = weight * settled
    for m in range(4):
        for c in range(4):
            sums = split_dot(hits, scaled * att_ref[4 * m + c])
            at = 14 * m + 10 + c
            total = total + jnp.where(lane == at, jnp.sum(sums, axis=1, keepdims=True), 0.0)
    lane40 = lax.broadcasted_iota(jnp.int32, (SPAN + 8, 128), 1)
    padded = jnp.concatenate([total, jnp.zeros((8, 128), F32)], axis=0)
    moved = jnp.where(lane40 < 14, padded, 0.0)
    for m in range(1, 4):
        shifted = pltpu.roll(pltpu.roll(padded, m, 0), 128 - 14 * m, 1)
        moved = moved + jnp.where(lane40 < 14, shifted, 0.0)
    edge_ref[0] = moved[SPAN:]
    def onward(to):
        return pltpu.make_async_remote_copy(
            src_ref=edge_ref.at[0], dst_ref=edge_ref.at[1], send_sem=sent.at[0], recv_sem=landed.at[0],
            device_id=to, device_id_type=pl.DeviceIdType.MESH)

    def backward(to):
        return pltpu.make_async_remote_copy(
            src_ref=head_ref, dst_ref=next_ref, send_sem=sent.at[1], recv_sem=landed.at[1],
            device_id=to, device_id_type=pl.DeviceIdType.MESH)

    @pl.when(has_after)
    def _():
        onward(after).start()

    @pl.when(has_before)
    def _():
        onward(before).wait_recv()

    sums = jnp.concatenate([moved[:8] + edge_ref[1], moved[8:SPAN]], axis=0)

    def column(at):
        return jnp.broadcast_to(sums[:, at:at + 1], (SPAN, 128))

    entries = {pair: column(n) for n, pair in enumerate(KNOT_PAIRS)}
    answer = damped_solve(entries, [column(10 + c) for c in range(4)], 4)
    for c in range(4):
        head_ref[c] = answer[c][:8]

    @pl.when(has_before)
    def _():
        backward(before).start()

    row32 = lax.broadcasted_iota(jnp.int32, (SPAN, 128), 0)
    row8 = lax.broadcasted_iota(jnp.int32, (8, 128), 0)
    piece = jnp.zeros((8, 128), F32)
    for c in range(4):
        line = jnp.sum(jnp.where(lane == row32 + (sky % 4) * SPAN, answer[c], 0.0), axis=0, keepdims=True)
        piece = jnp.where(row8 == c, line, piece)
    piece_ref[...] = piece
    copies = [send(piece_ref, pieces_ref.at[sky], sent.at[1 + d], landed.at[1 + d], peers[d - 1])
              for d in range(1, OWNERS)]
    pieces_ref[sky] = piece

    @pl.when(has_after)
    def _():
        backward(after).wait_recv()

    fix = None
    for m in range(4):
        for c in range(4):
            both = jnp.concatenate([answer[c], next_ref[c]], axis=0)
            value = both[m:m + SPAN]
            high = value.astype(BF16)
            rest = value - high.astype(F32)
            middle = rest.astype(BF16)
            low = (rest - middle.astype(F32)).astype(BF16)
            table = jnp.concatenate([high, middle, low, jnp.zeros_like(high)], axis=0)
            term = att_ref[4 * m + c] * jnp.dot(hits_ref[...], table, preferred_element_type=F32)
            fix = term if fix is None else fix + term
    out_ref[...] = settled_ref[...] - fix
    for copy in copies:
        copy.wait()
    for j in range(4):
        total = pieces_ref[4 * j]
        for i in range(1, 4):
            total = total + pieces_ref[4 * j + i]
        attitude_ref[:, j * 128:(j + 1) * 128] = total[:4]

    @pl.when(has_after)
    def _():
        onward(after).wait_send()

    @pl.when(has_before)
    def _():
        backward(before).wait_send()


def apply_updates(pix, where, first, tiles, table, knots, weight, attitude, quad, hits):
    return pl.pallas_call(
        apply_kernel,
        out_shape=(
            jax.ShapeDtypeStruct((TILES, 128), F32),
            jax.ShapeDtypeStruct((4, SPAN * OWNERS), F32),
        ),
        in_specs=[SMEM, SMEM, SMEM, HBM, VMEM, VMEM, VMEM, HBM, VMEM, VMEM],
        out_specs=(VMEM, VMEM),
        scratch_shapes=[
            pltpu.VMEM((SLOTS * ROOM, 128), F32),
            pltpu.VMEM((SLOTS * SEATS, 128), F32),
            pltpu.VMEM((SLOTS * SEATS, 128), F32),
            pltpu.VMEM((16, TILES, 128), F32),
            pltpu.VMEM((TILES, 128), F32),
            pltpu.VMEM((2, 8, 128), F32),
            pltpu.VMEM((4, 8, 128), F32),
            pltpu.VMEM((4, 8, 128), F32),
            pltpu.VMEM((8, 128), F32),
            pltpu.VMEM((OWNERS, 8, 128), F32),
            pltpu.SemaphoreType.DMA((OWNERS + 1,)),
            pltpu.SemaphoreType.DMA((OWNERS + 1,)),
            pltpu.SemaphoreType.DMA((9,)),
            pltpu.SemaphoreType.DMA((SLOTS,)),
            pltpu.SemaphoreType.DMA((SLOTS,)),
        ],
        compiler_params=params(collective_id=4, has_side_effects=True),
        name="apply_updates",
    )(pix, where, first, tiles, table, knots, weight, attitude, quad, hits)


def emit_kernel(final_ref, attitude_ref, table_ref, final_out, attitude_out, update_out):
    final_out[...] = final_ref[...]
    attitude_out[...] = attitude_ref[...]
    for p in range(PIX):
        update_out[:, p * 128:(p + 1) * 128] = table_ref[p * 5:p * 5 + 5, :]


def emit(final, attitude, table):
    return pl.pallas_call(
        emit_kernel,
        out_shape=(
            jax.ShapeDtypeStruct((TILES, 128), F32),
            jax.ShapeDtypeStruct((4, SPAN * OWNERS), F32),
            jax.ShapeDtypeStruct((5, PIX * SRC), F32),
        ),
        in_specs=[VMEM, VMEM, VMEM],
        out_specs=(VMEM, VMEM, VMEM),
        compiler_params=params(),
        name="emit",
    )(final, attitude, table)


def body(residual, obs_weight, source_partials, attitude_partials, source_index,
         tile_pixel, tile_knot, pixel_slot):
    block = lax.axis_index("tm") * OWNERS + lax.axis_index("sky")
    first = (block * SPAN).reshape(1)
    knots = tile_knot.reshape(1, TILES)
    packed, where = pack(tile_pixel, pixel_slot, residual, obs_weight, source_partials, source_index)
    arrived, normals, pix, quad, hits = gather_tiles(packed, attitude_partials, obs_weight, knots, first)
    table = reduce_and_solve(normals)
    final, attitude_update = apply_updates(
        pix, where, first, arrived, table, knots, obs_weight, attitude_partials, quad, hits)
    final, attitude_update, source_update = emit(final, attitude_update, table)
    return final, source_update, attitude_update


def solution(mesh):
    in_specs = (
        P(("tm", "sky"), None),
        P(("tm", "sky"), None),
        P(None, ("tm", "sky"), None),
        P(None, ("tm", "sky"), None),
        P(("tm", "sky"), None),
        P(("tm", "sky")),
        P(("tm", "sky")),
        P(),
    )
    out_specs = (P(("tm", "sky"), None), P(None, "sky"), P(None, "tm"))
    return jax.shard_map(body, mesh=mesh, in_specs=in_specs, out_specs=out_specs, check_vma=False)
```

```python
import jax
import jax.numpy as jnp
from jax import lax
from jax.experimental import pallas as pl
from jax.experimental.pallas import tpu as pltpu
from jax.sharding import PartitionSpec as P

TILES = 512
OWNERS = 16
TIMES = 8
CAP = 96
PIX = 128
SRC = 128
FIELDS = 7
CLASSES = 2
SEATS = CAP // CLASSES
SLOTS = OWNERS * CLASSES
BLOCK_ROWS = SEATS * FIELDS
ROWS_IN = SLOTS * BLOCK_ROWS + 8
SPAN = 32
TERMS = 20
HALF = PIX // TIMES
HROWS = HALF * TERMS
KNOT_PAIRS = tuple((c, e) for c in range(4) for e in range(c, 4))
TERM_ROW = {
    (0, 0): 0, (1, 1): 1, (2, 2): 2, (3, 3): 3, (4, 4): 4, (0, 5): 5,
    (0, 1): 6, (1, 2): 7, (2, 3): 8, (3, 4): 9, (4, 5): 10, (0, 4): 11, (1, 5): 12,
    (0, 2): 13, (1, 3): 14, (2, 4): 15, (3, 5): 16, (0, 3): 17, (1, 4): 18, (2, 5): 19,
}
VMEM = pl.BlockSpec(memory_space=pltpu.VMEM)
SMEM = pl.BlockSpec(memory_space=pltpu.SMEM)
F32 = jnp.float32
BF16 = jnp.bfloat16


def params(**kw):
    return pltpu.CompilerParams(vmem_limit_bytes=60 * 1024 * 1024, **kw)


def pack_kernel(pixel_ref, slot_ref, res_ref, w_ref, part_ref, idx_ref,
                out_ref, where_ref, count_ref, stage_ref):
    for o in range(OWNERS):
        count_ref[o] = 0
    nothing = jnp.zeros((SEATS, 128), F32)

    def clear(b, _):
        base = pl.multiple_of(b * BLOCK_ROWS, 8)
        for i in range(FIELDS):
            out_ref[pl.ds(base + i * SEATS, SEATS), :] = nothing
        out_ref[pl.ds(base + 6, SEATS, stride=FIELDS), :] = nothing - 1.0
        return 0

    lax.fori_loop(0, SLOTS, clear, 0)

    def scale(g, _):
        rows = pl.ds(pl.multiple_of(g * 8, 8), 8)
        root = jnp.sqrt(w_ref[rows, :])
        for a in range(5):
            stage_ref[a, rows, :] = part_ref[a, rows, :] * root
        stage_ref[5, rows, :] = res_ref[rows, :] * root
        stage_ref[6, rows, :] = idx_ref[rows, :].astype(F32)
        return 0

    lax.fori_loop(0, TILES // 8, scale, 0, unroll=4)

    def place(g, _):
        for j in range(8):
            t = g * 8 + j
            seat = slot_ref[pixel_ref[t]]
            owner = lax.shift_right_logical(seat, 7)
            rank = count_ref[owner]
            count_ref[owner] = rank + 1
            block = owner * CLASSES + lax.bitwise_and(rank, 1)
            position = lax.shift_right_logical(rank, 1)
            where_ref[t] = block * SEATS + position
            base = block * BLOCK_ROWS + position * FIELDS
            for f in range(6):
                out_ref[pl.ds(base + f, 1), :] = stage_ref[f, pl.ds(t, 1), :]
            first = (lax.bitwise_and(seat, 127) * SRC).astype(F32)
            out_ref[pl.ds(base + 6, 1), :] = stage_ref[6, pl.ds(t, 1), :] + first
        return 0

    lax.fori_loop(0, TILES // 8, place, 0)


def pack(tile_pixel, pixel_slot, residual, weight, partials, index):
    return pl.pallas_call(
        pack_kernel,
        out_shape=(
            jax.ShapeDtypeStruct((ROWS_IN, 128), F32),
            jax.ShapeDtypeStruct((TILES,), jnp.int32),
        ),
        in_specs=[SMEM, SMEM, VMEM, VMEM, VMEM, VMEM],
        out_specs=(VMEM, SMEM),
        scratch_shapes=[pltpu.SMEM((OWNERS,), jnp.int32), pltpu.VMEM((FIELDS, TILES, 128), F32)],
        compiler_params=params(),
        name="pack",
    )(tile_pixel, pixel_slot, residual, weight, partials, index)


def place_of():
    tm, sky = lax.axis_index("tm"), lax.axis_index("sky")
    return tm // 2, tm % 2, sky // 4, (sky // 2) % 2, sky % 2


def device_of(y, zh, x, zl, c):
    return (y * 2 + zh, x * 4 + zl * 2 + c)


def send(src, dst, sent, landed, device):
    copy = pltpu.make_async_remote_copy(
        src_ref=src, dst_ref=dst, send_sem=sent, recv_sem=landed,
        device_id=device, device_id_type=pl.DeviceIdType.MESH)
    copy.start()
    return copy


def greet(devices):
    barrier = pltpu.get_barrier_semaphore()
    for device in devices:
        pl.semaphore_signal(barrier, inc=1, device_id=device, device_id_type=pl.DeviceIdType.MESH)
    pl.semaphore_wait(barrier, len(devices))


def move_of(k):
    far, step, turn = (k // 8 + 2) // 3, (k + 4) % 6, (k + 4) // 6 - 2
    u = step // 2
    d = far * (2 - u + 3 * (u // 2))
    dz = far * (1 - step % 2) + (1 - far) * (k // 4)
    dc = far * (turn // 2) + (1 - far) * (k // 2 % 2)
    h = far * (turn % 2) + (1 - far) * (k % 2)
    return d, dz, dc, h


MOVES = [move_of(k) for k in range(SLOTS)]
OWN = (0, 1)
CHUNK = 2
CHUNKS = SLOTS // CHUNK
STEP = 24
PITCH = 136
ROOM = BLOCK_ROWS + 8
HBM = pl.BlockSpec(memory_space=pltpu.HBM)


def routes_of():
    y, zh, x, zl, c = place_of()
    routes = []
    for d, dz, dc, h in MOVES:
        far, zl_to, c_to = (x + d) % 4, (zl + dz) % 2, (c + dc) % 2
        owner = far * 4 + zl_to * 2 + c_to
        routes.append((owner * CLASSES + h, device_of(y, (zh + dz * h) % 2, far, zl_to, c_to)))
    return routes


def pair_products(v, row):
    low5, low4 = row < 5, row < 4
    one = pltpu.roll(v, 1, 0)
    first = jnp.where(low5, v, pltpu.roll(v, 5, 0))
    second = jnp.where(low5, pltpu.roll(v, 7, 0), one)
    third = jnp.where(low4, v, pltpu.roll(v, 4, 0))
    fourth = jnp.where(low4, pltpu.roll(v, 6, 0), one)
    return jnp.concatenate([first * v, first * second, third * fourth], axis=0)


def left_side(v, row):
    products = pair_products(v, row)
    high = products.astype(BF16).astype(F32)
    return jnp.concatenate([high, products - high], axis=0).astype(BF16)


def landing(in_ref, arr_ref, sent, landed, k, to):
    return pltpu.make_async_remote_copy(
        src_ref=in_ref.at[pl.ds(k * BLOCK_ROWS, BLOCK_ROWS)],
        dst_ref=arr_ref.at[pl.ds(k * ROOM, BLOCK_ROWS)], send_sem=sent.at[k], recv_sem=landed.at[k],
        device_id=to, device_id_type=pl.DeviceIdType.MESH)


def gather_kernel(in_ref, att_hbm, w_hbm, knot_ref, first_ref,
                  keep_ref, sums_ref, pix_ref, quad_ref, hits_ref,
                  arr_ref, att_ref, w_ref, spread_ref, sent, landed, local, stored):
    routes = routes_of()
    load_att = pltpu.make_async_copy(att_hbm, att_ref, local.at[4])
    load_w = pltpu.make_async_copy(w_hbm, w_ref, local.at[5])
    load_att.start()
    load_w.start()
    greet([to for k, (_, to) in enumerate(routes) if k not in OWN])
    copies = []
    for k, (block, to) in enumerate(routes):
        if k not in OWN:
            copies.append(send(in_ref.at[pl.ds(block * BLOCK_ROWS, BLOCK_ROWS)],
                               arr_ref.at[pl.ds(k * ROOM, BLOCK_ROWS)], sent.at[k], landed.at[k], to))
    kept = []
    for i, k in enumerate(OWN):
        kept.append(pltpu.make_async_copy(in_ref.at[pl.ds(routes[k][0] * BLOCK_ROWS, BLOCK_ROWS)],
                                          arr_ref.at[pl.ds(k * ROOM, BLOCK_ROWS)], local.at[i]))
        kept[-1].start()

    def clear(g, _):
        spread_ref[pl.ds(pl.multiple_of(g * 8, 8), 8), :] = jnp.zeros((8, 128), F32)
        return 0

    lax.fori_loop(0, 24 * PITCH // 8, clear, 0, unroll=4)

    def clear_sums(g, _):
        sums_ref[pl.ds(pl.multiple_of(g * 16, 16), 16), :] = jnp.zeros((16, 128), F32)
        return 0

    lax.fori_loop(0, PIX * TERMS // 16, clear_sums, 0, unroll=4)
    load_att.wait()
    load_w.wait()
    quad_sums(knot_ref, first_ref, w_ref, att_ref, quad_ref, hits_ref)
    for move in kept:
        move.wait()
    row = lax.broadcasted_iota(jnp.int32, (8, 128), 0)
    sources = lax.broadcasted_iota(jnp.int32, (128, 128), 0).astype(F32)
    pixels = lax.broadcasted_iota(jnp.int32, (SEATS, 128), 1)
    seat_row = lax.broadcasted_iota(jnp.int32, (SEATS, 128), 0)
    blank = jnp.zeros((48, 128), BF16)

    def keep(k):
        return pltpu.make_async_copy(arr_ref.at[pl.ds(k * ROOM, BLOCK_ROWS)],
                                     keep_ref.at[pl.ds(k * ROOM, BLOCK_ROWS)], stored.at[k])

    def chunk_step(chunk, _):
        for i in range(CHUNK):
            k = chunk * CHUNK + i
            arrival = landing(in_ref, arr_ref, sent, landed, k, routes[2][1])

            @pl.when(chunk >= 1)
            def _():
                arrival.wait_recv()

            keep(k).start()

        def group(g, _):
            for j in range(0, STEP, 2):
                start = (chunk * CHUNK + g // 2) * ROOM + (g % 2 * STEP + j) * FIELDS
                lefts, hits = [], []
                for i in range(2):
                    v = arr_ref[pl.ds(start + i * FIELDS, 8), :]
                    within = v - jnp.floor(v * (1.0 / SRC)) * SRC
                    lefts.append(left_side(v, row))
                    hits.append((within[6:7, :] == sources).astype(F32).astype(BF16))
                left = jnp.concatenate([jnp.concatenate([lefts[0], blank], axis=1),
                                        jnp.concatenate([blank, lefts[1]], axis=1)], axis=0)
                out = lax.dot_general(left, jnp.concatenate(hits, axis=1), (((1,), (1,)), ((), ())),
                                      preferred_element_type=F32)
                for i in range(2):
                    both = out[48 * i:48 * i + 24] + out[48 * i + 24:48 * i + 48]
                    for n in range(3):
                        spread_ref[pl.ds(8 * n * PITCH + g * STEP + j + i, 8, stride=PITCH), :] = both[8 * n:8 * n + 8]
            return 0

        lax.fori_loop(0, CHUNK * SEATS // STEP, group, 0)
        places = []
        for i in range(CHUNK):
            k = chunk * CHUNK + i
            whole = arr_ref[pl.ds(k * ROOM + 6, SEATS, stride=FIELDS), :]
            pixel = jnp.floor(whole * (1.0 / SRC)).astype(jnp.int32)
            places.append((pixel == pixels).astype(F32))
            line = jnp.sum(jnp.where(pixels == seat_row, pixel, 0), axis=0, keepdims=True)
            pix_ref[pl.ds(k, 1), :] = jnp.maximum(line, 0)
        places.append(jnp.zeros((128 - CHUNK * SEATS, 128), F32))
        place = jnp.concatenate(places, axis=0).T.astype(BF16)
        place = jnp.concatenate([place, place], axis=1)
        for n in range(TERMS):
            at = n + (2 if n >= 6 else 0) + (1 if n >= 13 else 0)
            value = spread_ref[pl.ds(at * PITCH, 128), :]
            high = value.astype(BF16)
            low = (value - high.astype(F32)).astype(BF16)
            added = jnp.dot(place, jnp.concatenate([high, low], axis=0), preferred_element_type=F32)
            for part in range(TIMES):
                rows = pl.ds(part * HROWS + n * HALF, HALF)
                sums_ref[rows, :] = sums_ref[rows, :] + added[part * HALF:(part + 1) * HALF]
        return 0

    lax.fori_loop(0, CHUNKS, chunk_step, 0)
    for copy in copies:
        copy.wait_send()

    def kept_step(k, _):
        keep(k).wait()
        return 0

    lax.fori_loop(0, SLOTS, kept_step, 0)


def gather_tiles(packed, attitude, weight, knots, first):
    return pl.pallas_call(
        gather_kernel,
        out_shape=(
            jax.ShapeDtypeStruct((SLOTS * ROOM, 128), F32),
            jax.ShapeDtypeStruct((PIX * TERMS, 128), F32),
            jax.ShapeDtypeStruct((SLOTS, 128), jnp.int32),
            jax.ShapeDtypeStruct((SPAN, 128), F32),
            jax.ShapeDtypeStruct((TILES, 128), BF16),
        ),
        in_specs=[HBM, HBM, HBM, VMEM, SMEM],
        out_specs=(HBM, VMEM, VMEM, VMEM, VMEM),
        scratch_shapes=[
            pltpu.VMEM((SLOTS * ROOM, 128), F32),
            pltpu.VMEM((16, TILES, 128), F32),
            pltpu.VMEM((TILES, 128), F32),
            pltpu.VMEM((24 * PITCH, 128), F32),
            pltpu.SemaphoreType.DMA((SLOTS,)),
            pltpu.SemaphoreType.DMA((SLOTS,)),
            pltpu.SemaphoreType.DMA((6,)),
            pltpu.SemaphoreType.DMA((SLOTS,)),
        ],
        compiler_params=params(collective_id=1, has_side_effects=True),
        name="gather_tiles",
    )(packed, attitude, weight, knots, first)


def damped_solve(entries, target, order):
    factor = {}
    for column in range(order):
        pivot = entries[column, column] + 1.0
        for earlier in range(column):
            pivot = pivot - factor[column, earlier] * factor[column, earlier]
        pivot = jnp.sqrt(pivot)
        factor[column, column] = pivot
        for below in range(column + 1, order):
            current = entries[column, below]
            for earlier in range(column):
                current = current - factor[below, earlier] * factor[column, earlier]
            factor[below, column] = current / pivot
    forward = []
    for column in range(order):
        current = target[column]
        for earlier in range(column):
            current = current - factor[column, earlier] * forward[earlier]
        forward.append(current / factor[column, column])
    answer = [None] * order
    for column in reversed(range(order)):
        current = forward[column]
        for later in range(column + 1, order):
            current = current - factor[later, column] * answer[later]
        answer[column] = current / factor[column, column]
    return answer


def reduce_and_solve(in_ref, table_ref, parts_ref, whole_ref, own_ref, peers, devices, tm,
                     sent1, landed1, sent2, landed2):
    copies = []
    for i, (to_y, to_zh) in enumerate(peers):
        copies.append(send(in_ref.at[pl.ds((to_y * 2 + to_zh) * HROWS, HROWS)], parts_ref.at[i],
                           sent1.at[i], landed1.at[i], devices[i]))
    for copy in copies:
        copy.wait()

    def add(g, _):
        rows = pl.ds(pl.multiple_of(g * 16, 16), 16)
        total = in_ref[pl.ds(tm * HROWS + pl.multiple_of(g * 16, 16), 16), :]
        for i in range(TIMES - 1):
            total = total + parts_ref[i, rows, :]
        whole_ref[rows, :] = total
        return 0

    lax.fori_loop(0, TERMS, add, 0, unroll=4)
    sums = [whole_ref[pl.ds(term * HALF, HALF), :] for term in range(TERMS)]
    entries = {key: sums[at] for key, at in TERM_ROW.items() if key[1] < 5}
    target = [sums[TERM_ROW[a, 5]] for a in range(5)]
    for a, value in enumerate(damped_solve(entries, target, 5)):
        own_ref[pl.ds(a, HALF, stride=5), :] = value
    part = pl.ds(tm * HALF * 5, HALF * 5)
    table_ref[part, :] = own_ref[...]
    copies = [send(own_ref, table_ref.at[part], sent2.at[i], landed2.at[i], device)
              for i, device in enumerate(devices)]
    for copy in copies:
        copy.wait()


def knot_hits(knot_row, first):
    lane = lax.broadcasted_iota(jnp.int32, (SPAN, TILES), 0)
    return (lane == knot_row - first).astype(F32)


def split_dot(hits, value):
    high = value.astype(BF16)
    low = (value - high.astype(F32)).astype(BF16)
    return (jnp.dot(hits, high, preferred_element_type=F32)
            + jnp.dot(hits, low, preferred_element_type=F32))


def quad_sums(knot_ref, first_ref, w_ref, att_ref, out_ref, hits_ref):
    hits = knot_hits(knot_ref[...], first_ref[0])
    flipped = hits.T
    hits_ref[...] = jnp.concatenate([flipped] * 3 + [jnp.zeros_like(flipped)], axis=1).astype(BF16)
    hits = hits.astype(BF16)
    lane = lax.broadcasted_iota(jnp.int32, (SPAN, 128), 1)
    total = jnp.zeros((SPAN, 128), F32)
    weight = w_ref[...]
    for m in range(4):
        for c in range(4):
            scaled = weight * att_ref[4 * m + c]
            for e in range(c, 4):
                sums = split_dot(hits, scaled * att_ref[4 * m + e])
                at = 14 * m + KNOT_PAIRS.index((c, e))
                total = total + jnp.where(lane == at, jnp.sum(sums, axis=1, keepdims=True), 0.0)
    out_ref[...] = total


def apply_kernel(pix_ref, where_ref, first_ref, normals_ref, tiles_hbm, knot_ref, w_ref, att_hbm, quad_ref, hits_ref,
                 out_ref, attitude_ref, table_ref, parts_ref, whole_ref, own_ref, arr_ref, fixed_ref, back_ref, att_ref,
                 settled_ref, edge_ref, head_ref, next_ref, piece_ref, pieces_ref,
                 sent, landed, loaded, given, taken, sent1, landed1, sent2, landed2):
    tm, sky = lax.axis_index("tm"), lax.axis_index("sky")
    y, zh, x, zl, c0 = place_of()
    block = tm * OWNERS + sky
    after = ((block + 1) // OWNERS % TIMES, (block + 1) % OWNERS)
    before = ((block + 127) // OWNERS % TIMES, (block + 127) % OWNERS)
    has_after, has_before = block < TIMES * OWNERS - 1, block > 0
    peers = [(tm, (sky + d) % OWNERS) for d in range(1, OWNERS)]
    parts = 8
    size = SLOTS // parts * ROOM

    def load(part):
        rows = pl.ds(part * size, size)
        return pltpu.make_async_copy(tiles_hbm.at[rows], arr_ref.at[rows], loaded.at[part])

    for part in range(parts):
        load(part).start()
    load_att = pltpu.make_async_copy(att_hbm, att_ref, loaded.at[parts])
    load_att.start()
    edge_ref[1] = jnp.zeros((8, 128), F32)
    next_ref[...] = jnp.zeros((4, 8, 128), F32)
    times = [((y + d) % 4, (zh + z) % 2) for d, z in ((2, 1), (2, 0), (1, 1), (3, 1), (1, 0), (3, 0), (0, 1))]
    shards = [device_of(to_y, to_zh, x, zl, c0) for to_y, to_zh in times]
    greet(shards + peers + [after, before] + [to for k, (_, to) in enumerate(routes_of()) if k not in OWN])
    reduce_and_solve(normals_ref, table_ref, parts_ref, whole_ref, own_ref, times, shards, tm,
                     sent1, landed1, sent2, landed2)

    def give(k):
        d, dz, dc, h = move_of(k)
        to = device_of(y, (zh + dz * h) % 2, (x + 4 - d) % 4, (zl + dz) % 2, (c0 + dc) % 2)
        seat = sky * CLASSES + h
        return pltpu.make_async_remote_copy(
            src_ref=fixed_ref.at[pl.ds(k * SEATS, SEATS)], dst_ref=back_ref.at[pl.ds(seat * SEATS, SEATS)],
            send_sem=given.at[k], recv_sem=taken.at[k], device_id=to, device_id_type=pl.DeviceIdType.MESH), seat

    def is_own(k):
        return k < 2

    def pass_on(k):
        copy, seat = give(k)

        @pl.when(jnp.logical_not(is_own(k)))
        def _():
            copy.start()

        @pl.when(is_own(k))
        def _():
            back_ref[pl.ds(seat * SEATS, SEATS), :] = fixed_ref[pl.ds(k * SEATS, SEATS), :]

    row = lax.broadcasted_iota(jnp.int32, (8, 128), 0)

    def pick(step, _):
        k, first = step // 2, step % 2 * STEP

        @pl.when(step % (2 * SLOTS // parts) == 0)
        def _():
            load(step // (2 * SLOTS // parts)).wait()

        for j in range(STEP):
            v = arr_ref[pl.ds(k * ROOM + (first + j) * FIELDS, 8), :]
            table = table_ref[pl.ds(pix_ref[k, first + j] * 5, 8), :]
            within = (v - jnp.floor(v * (1.0 / SRC)) * SRC).astype(jnp.int32)
            at = jnp.broadcast_to(lax.bitwise_and(within[6:7, :], 127), (8, 128))
            picked = jnp.take_along_axis(table, at, axis=1)
            terms = jnp.where(row < 5, v * picked, jnp.where(row == 5, -v, 0.0))
            fixed_ref[pl.ds(k * SEATS + first + j, 1), :] = -jnp.sum(terms, axis=0, keepdims=True)

        @pl.when(jnp.logical_and(first == 0, k > 0))
        def _():
            pass_on(k - 1)

        return 0

    lax.fori_loop(0, 2 * SLOTS, pick, 0)
    pass_on(SLOTS - 1)
    load_att.wait()

    def settle(k, _):
        @pl.when(jnp.logical_not(is_own(k)))
        def _():
            give(k)[0].wait()

        return 0

    lax.fori_loop(0, SLOTS, settle, 0)

    def fetch(g, _):
        for j in range(16):
            t = g * 16 + j
            settled_ref[pl.ds(t, 1), :] = back_ref[pl.ds(where_ref[t], 1), :]
        return 0

    lax.fori_loop(0, TILES // 16, fetch, 0)
    weight = w_ref[...]
    settled = settled_ref[...] / jnp.sqrt(weight)
    settled_ref[...] = settled
    hits = knot_hits(knot_ref[...], first_ref[0]).astype(BF16)
    lane = lax.broadcasted_iota(jnp.int32, (SPAN, 128), 1)
    total = quad_ref[...]
    scaled = weight * settled
    for m in range(4):
        for c in range(4):
            sums = split_dot(hits, scaled * att_ref[4 * m + c])
            at = 14 * m + 10 + c
            total = total + jnp.where(lane == at, jnp.sum(sums, axis=1, keepdims=True), 0.0)
    lane40 = lax.broadcasted_iota(jnp.int32, (SPAN + 8, 128), 1)
    padded = jnp.concatenate([total, jnp.zeros((8, 128), F32)], axis=0)
    moved = jnp.where(lane40 < 14, padded, 0.0)
    for m in range(1, 4):
        shifted = pltpu.roll(pltpu.roll(padded, m, 0), 128 - 14 * m, 1)
        moved = moved + jnp.where(lane40 < 14, shifted, 0.0)
    edge_ref[0] = moved[SPAN:]
    def onward(to):
        return pltpu.make_async_remote_copy(
            src_ref=edge_ref.at[0], dst_ref=edge_ref.at[1], send_sem=sent.at[0], recv_sem=landed.at[0],
            device_id=to, device_id_type=pl.DeviceIdType.MESH)

    def backward(to):
        return pltpu.make_async_remote_copy(
            src_ref=head_ref, dst_ref=next_ref, send_sem=sent.at[1], recv_sem=landed.at[1],
            device_id=to, device_id_type=pl.DeviceIdType.MESH)

    @pl.when(has_after)
    def _():
        onward(after).start()

    @pl.when(has_before)
    def _():
        onward(before).wait_recv()

    sums = jnp.concatenate([moved[:8] + edge_ref[1], moved[8:SPAN]], axis=0)

    def column(at):
        return jnp.broadcast_to(sums[:, at:at + 1], (SPAN, 128))

    entries = {pair: column(n) for n, pair in enumerate(KNOT_PAIRS)}
    answer = damped_solve(entries, [column(10 + c) for c in range(4)], 4)
    for c in range(4):
        head_ref[c] = answer[c][:8]

    @pl.when(has_before)
    def _():
        backward(before).start()

    row32 = lax.broadcasted_iota(jnp.int32, (SPAN, 128), 0)
    row8 = lax.broadcasted_iota(jnp.int32, (8, 128), 0)
    piece = jnp.zeros((8, 128), F32)
    for c in range(4):
        line = jnp.sum(jnp.where(lane == row32 + (sky % 4) * SPAN, answer[c], 0.0), axis=0, keepdims=True)
        piece = jnp.where(row8 == c, line, piece)
    piece_ref[...] = piece
    copies = [send(piece_ref, pieces_ref.at[sky], sent.at[1 + d], landed.at[1 + d], peers[d - 1])
              for d in range(1, OWNERS)]
    pieces_ref[sky] = piece

    @pl.when(has_after)
    def _():
        backward(after).wait_recv()

    fix = None
    for m in range(4):
        for c in range(4):
            both = jnp.concatenate([answer[c], next_ref[c]], axis=0)
            value = both[m:m + SPAN]
            high = value.astype(BF16)
            rest = value - high.astype(F32)
            middle = rest.astype(BF16)
            low = (rest - middle.astype(F32)).astype(BF16)
            table = jnp.concatenate([high, middle, low, jnp.zeros_like(high)], axis=0)
            term = att_ref[4 * m + c] * jnp.dot(hits_ref[...], table, preferred_element_type=F32)
            fix = term if fix is None else fix + term
    out_ref[...] = settled_ref[...] - fix
    for copy in copies:
        copy.wait()
    for j in range(4):
        total = pieces_ref[4 * j]
        for i in range(1, 4):
            total = total + pieces_ref[4 * j + i]
        attitude_ref[:, j * 128:(j + 1) * 128] = total[:4]

    @pl.when(has_after)
    def _():
        onward(after).wait_send()

    @pl.when(has_before)
    def _():
        backward(before).wait_send()


def apply_updates(pix, where, first, normals, tiles, knots, weight, attitude, quad, hits):
    return pl.pallas_call(
        apply_kernel,
        out_shape=(
            jax.ShapeDtypeStruct((TILES, 128), F32),
            jax.ShapeDtypeStruct((4, SPAN * OWNERS), F32),
            jax.ShapeDtypeStruct((PIX * 5 + 8, 128), F32),
        ),
        in_specs=[SMEM, SMEM, SMEM, VMEM, HBM, VMEM, VMEM, HBM, VMEM, VMEM],
        out_specs=(VMEM, VMEM, VMEM),
        scratch_shapes=[
            pltpu.VMEM((TIMES - 1, HROWS, 128), F32),
            pltpu.VMEM((HROWS, 128), F32),
            pltpu.VMEM((HALF * 5, 128), F32),
            pltpu.VMEM((SLOTS * ROOM, 128), F32),
            pltpu.VMEM((SLOTS * SEATS, 128), F32),
            pltpu.VMEM((SLOTS * SEATS, 128), F32),
            pltpu.VMEM((16, TILES, 128), F32),
            pltpu.VMEM((TILES, 128), F32),
            pltpu.VMEM((2, 8, 128), F32),
            pltpu.VMEM((4, 8, 128), F32),
            pltpu.VMEM((4, 8, 128), F32),
            pltpu.VMEM((8, 128), F32),
            pltpu.VMEM((OWNERS, 8, 128), F32),
            pltpu.SemaphoreType.DMA((OWNERS + 1,)),
            pltpu.SemaphoreType.DMA((OWNERS + 1,)),
            pltpu.SemaphoreType.DMA((9,)),
            pltpu.SemaphoreType.DMA((SLOTS,)),
            pltpu.SemaphoreType.DMA((SLOTS,)),
            pltpu.SemaphoreType.DMA((TIMES - 1,)),
            pltpu.SemaphoreType.DMA((TIMES - 1,)),
            pltpu.SemaphoreType.DMA((TIMES - 1,)),
            pltpu.SemaphoreType.DMA((TIMES - 1,)),
        ],
        compiler_params=params(collective_id=4, has_side_effects=True),
        name="apply_updates",
    )(pix, where, first, normals, tiles, knots, weight, attitude, quad, hits)


def emit_kernel(final_ref, attitude_ref, table_ref, final_out, attitude_out, update_out):
    final_out[...] = final_ref[...]
    attitude_out[...] = attitude_ref[...]
    for p in range(PIX):
        update_out[:, p * 128:(p + 1) * 128] = table_ref[p * 5:p * 5 + 5, :]


def emit(final, attitude, table):
    return pl.pallas_call(
        emit_kernel,
        out_shape=(
            jax.ShapeDtypeStruct((TILES, 128), F32),
            jax.ShapeDtypeStruct((4, SPAN * OWNERS), F32),
            jax.ShapeDtypeStruct((5, PIX * SRC), F32),
        ),
        in_specs=[VMEM, VMEM, VMEM],
        out_specs=(VMEM, VMEM, VMEM),
        compiler_params=params(),
        name="emit",
    )(final, attitude, table)


def body(residual, obs_weight, source_partials, attitude_partials, source_index,
         tile_pixel, tile_knot, pixel_slot):
    block = lax.axis_index("tm") * OWNERS + lax.axis_index("sky")
    first = (block * SPAN).reshape(1)
    knots = tile_knot.reshape(1, TILES)
    packed, where = pack(tile_pixel, pixel_slot, residual, obs_weight, source_partials, source_index)
    arrived, normals, pix, quad, hits = gather_tiles(packed, attitude_partials, obs_weight, knots, first)
    final, attitude_update, table = apply_updates(
        pix, where, first, normals, arrived, knots, obs_weight, attitude_partials, quad, hits)
    final, attitude_update, source_update = emit(final, attitude_update, table)
    return final, source_update, attitude_update


def solution(mesh):
    in_specs = (
        P(("tm", "sky"), None),
        P(("tm", "sky"), None),
        P(None, ("tm", "sky"), None),
        P(None, ("tm", "sky"), None),
        P(("tm", "sky"), None),
        P(("tm", "sky")),
        P(("tm", "sky")),
        P(),
    )
    out_specs = (P(("tm", "sky"), None), P(None, "sky"), P(None, "tm"))
    return jax.shard_map(body, mesh=mesh, in_specs=in_specs, out_specs=out_specs, check_vma=False)
```

```python
import jax
import jax.numpy as jnp
from jax import lax
from jax.experimental import pallas as pl
from jax.experimental.pallas import tpu as pltpu
from jax.sharding import PartitionSpec as P

TILES = 512
OWNERS = 16
TIMES = 8
CAP = 96
PIX = 128
SRC = 128
FIELDS = 7
CLASSES = 2
SEATS = CAP // CLASSES
SLOTS = OWNERS * CLASSES
BLOCK_ROWS = SEATS * FIELDS
ROWS_IN = SLOTS * BLOCK_ROWS + 8
SPAN = 32
TERMS = 20
HALF = PIX // TIMES
HROWS = HALF * TERMS
KNOT_PAIRS = tuple((c, e) for c in range(4) for e in range(c, 4))
TERM_ROW = {
    (0, 0): 0, (1, 1): 1, (2, 2): 2, (3, 3): 3, (4, 4): 4, (0, 5): 5,
    (0, 1): 6, (1, 2): 7, (2, 3): 8, (3, 4): 9, (4, 5): 10, (0, 4): 11, (1, 5): 12,
    (0, 2): 13, (1, 3): 14, (2, 4): 15, (3, 5): 16, (0, 3): 17, (1, 4): 18, (2, 5): 19,
}
VMEM = pl.BlockSpec(memory_space=pltpu.VMEM)
SMEM = pl.BlockSpec(memory_space=pltpu.SMEM)
F32 = jnp.float32
BF16 = jnp.bfloat16


def params(**kw):
    return pltpu.CompilerParams(vmem_limit_bytes=60 * 1024 * 1024, **kw)


def pack_kernel(pixel_ref, slot_ref, res_ref, w_ref, part_ref, idx_ref,
                out_ref, where_ref, count_ref, stage_ref):
    for o in range(OWNERS):
        count_ref[o] = 0
    nothing = jnp.zeros((SEATS, 128), F32)

    def clear(b, _):
        base = pl.multiple_of(b * BLOCK_ROWS, 8)
        for i in range(FIELDS):
            out_ref[pl.ds(base + i * SEATS, SEATS), :] = nothing
        out_ref[pl.ds(base + 6, SEATS, stride=FIELDS), :] = nothing - 1.0
        return 0

    lax.fori_loop(0, SLOTS, clear, 0)

    def scale(g, _):
        rows = pl.ds(pl.multiple_of(g * 8, 8), 8)
        root = jnp.sqrt(w_ref[rows, :])
        for a in range(5):
            stage_ref[a, rows, :] = part_ref[a, rows, :] * root
        stage_ref[5, rows, :] = res_ref[rows, :] * root
        stage_ref[6, rows, :] = idx_ref[rows, :].astype(F32)
        return 0

    lax.fori_loop(0, TILES // 8, scale, 0, unroll=4)

    def place(g, _):
        for j in range(8):
            t = g * 8 + j
            seat = slot_ref[pixel_ref[t]]
            owner = lax.shift_right_logical(seat, 7)
            rank = count_ref[owner]
            count_ref[owner] = rank + 1
            block = owner * CLASSES + lax.bitwise_and(rank, 1)
            position = lax.shift_right_logical(rank, 1)
            where_ref[t] = block * SEATS + position
            base = block * BLOCK_ROWS + position * FIELDS
            for f in range(6):
                out_ref[pl.ds(base + f, 1), :] = stage_ref[f, pl.ds(t, 1), :]
            first = (lax.bitwise_and(seat, 127) * SRC).astype(F32)
            out_ref[pl.ds(base + 6, 1), :] = stage_ref[6, pl.ds(t, 1), :] + first
        return 0

    lax.fori_loop(0, TILES // 8, place, 0)


def pack(tile_pixel, pixel_slot, residual, weight, partials, index):
    return pl.pallas_call(
        pack_kernel,
        out_shape=(
            jax.ShapeDtypeStruct((ROWS_IN, 128), F32),
            jax.ShapeDtypeStruct((TILES,), jnp.int32),
        ),
        in_specs=[SMEM, SMEM, VMEM, VMEM, VMEM, VMEM],
        out_specs=(VMEM, SMEM),
        scratch_shapes=[pltpu.SMEM((OWNERS,), jnp.int32), pltpu.VMEM((FIELDS, TILES, 128), F32)],
        compiler_params=params(),
        name="pack",
    )(tile_pixel, pixel_slot, residual, weight, partials, index)


def place_of():
    tm, sky = lax.axis_index("tm"), lax.axis_index("sky")
    return tm // 2, tm % 2, sky // 4, (sky // 2) % 2, sky % 2


def device_of(y, zh, x, zl, c):
    return (y * 2 + zh, x * 4 + zl * 2 + c)


def send(src, dst, sent, landed, device):
    copy = pltpu.make_async_remote_copy(
        src_ref=src, dst_ref=dst, send_sem=sent, recv_sem=landed,
        device_id=device, device_id_type=pl.DeviceIdType.MESH)
    copy.start()
    return copy


def greet(devices):
    barrier = pltpu.get_barrier_semaphore()
    for device in devices:
        pl.semaphore_signal(barrier, inc=1, device_id=device, device_id_type=pl.DeviceIdType.MESH)
    pl.semaphore_wait(barrier, len(devices))


def move_of(k):
    rest, near = k // 16, (k // 8 + 1) % 2 * (1 - k // 16)
    d = rest * (1 + k % 2 * 2)
    dz = rest * (1 - k // 2 % 2) + (1 - rest) * (k // 4 % 2)
    dc = rest * (k // 8 % 2) + (1 - rest) * (k // 2 % 2)
    h = rest * (k // 4 % 2) + (1 - rest) * (k % 2)
    return d, dz, dc, h, near


MOVES = [move_of(k) for k in range(SLOTS)]
OWN = (0, 1, 8, 9)
CHUNK = 2
CHUNKS = SLOTS // CHUNK
STEP = 24
PITCH = 136
ROOM = BLOCK_ROWS + 8
HBM = pl.BlockSpec(memory_space=pltpu.HBM)


def routes_of():
    y, zh, x, zl, c = place_of()
    routes = []
    for d, dz, dc, h, pair in MOVES:
        far, zl_to, c_to = (x + d) % 4, (zl + dz) % 2, (c + dc) % 2
        owner = (far + 2 * pair) % 4 * 4 + zl_to * 2 + c_to
        routes.append((owner * CLASSES + h, device_of(y, (zh + dz * h) % 2, far, zl_to, c_to)))
    return routes


def times_of(y, zh):
    return [((y + d) % 4, (zh + z) % 2) for d, z in ((2, 1), (2, 0), (1, 1), (3, 1), (1, 0), (3, 0), (0, 1))]


def pair_products(v, row):
    low5, low4 = row < 5, row < 4
    one = pltpu.roll(v, 1, 0)
    first = jnp.where(low5, v, pltpu.roll(v, 5, 0))
    second = jnp.where(low5, pltpu.roll(v, 7, 0), one)
    third = jnp.where(low4, v, pltpu.roll(v, 4, 0))
    fourth = jnp.where(low4, pltpu.roll(v, 6, 0), one)
    return jnp.concatenate([first * v, first * second, third * fourth], axis=0)


def left_side(v, row):
    products = pair_products(v, row)
    high = products.astype(BF16).astype(F32)
    return jnp.concatenate([high, products - high], axis=0).astype(BF16)


def landing(in_ref, arr_ref, sent, landed, k, to):
    return pltpu.make_async_remote_copy(
        src_ref=in_ref.at[pl.ds(k * BLOCK_ROWS, BLOCK_ROWS)],
        dst_ref=arr_ref.at[pl.ds(k * ROOM, BLOCK_ROWS)], send_sem=sent.at[k], recv_sem=landed.at[k],
        device_id=to, device_id_type=pl.DeviceIdType.MESH)


def gather_kernel(in_ref, att_hbm, w_hbm, knot_ref, first_ref,
                  keep_ref, sums_ref, pix_ref, quad_ref, hits_ref,
                  arr_ref, att_ref, w_ref, spread_ref, parts_ref, pair_ref, across_ref,
                  sent, landed, local, stored, sent1, landed1, sent2, landed2):
    routes = routes_of()
    load_att = pltpu.make_async_copy(att_hbm, att_ref, local.at[4])
    load_w = pltpu.make_async_copy(w_hbm, w_ref, local.at[5])
    load_att.start()
    load_w.start()
    y, zh, x, zl, c = place_of()
    tm = y * 2 + zh
    times = times_of(y, zh)
    partner = device_of(y, zh, (x + 2) % 4, zl, c)
    shards = [device_of(to_y, to_zh, x, zl, c) for to_y, to_zh in times]
    greet([to for k, (_, to) in enumerate(routes) if k not in OWN] + shards + [partner])
    copies = []
    for k, (block, to) in enumerate(routes):
        if k not in OWN:
            copies.append(send(in_ref.at[pl.ds(block * BLOCK_ROWS, BLOCK_ROWS)],
                               arr_ref.at[pl.ds(k * ROOM, BLOCK_ROWS)], sent.at[k], landed.at[k], to))
    kept = []
    for i, k in enumerate(OWN):
        kept.append(pltpu.make_async_copy(in_ref.at[pl.ds(routes[k][0] * BLOCK_ROWS, BLOCK_ROWS)],
                                          arr_ref.at[pl.ds(k * ROOM, BLOCK_ROWS)], local.at[i]))
        kept[-1].start()

    def clear(g, _):
        spread_ref[pl.ds(pl.multiple_of(g * 8, 8), 8), :] = jnp.zeros((8, 128), F32)
        return 0

    lax.fori_loop(0, 24 * PITCH // 8, clear, 0, unroll=4)

    def clear_sums(g, _):
        sums_ref[pl.ds(pl.multiple_of(g * 16, 16), 16), :] = jnp.zeros((16, 128), F32)
        return 0

    lax.fori_loop(0, 2 * PIX * TERMS // 16, clear_sums, 0, unroll=4)
    load_att.wait()
    load_w.wait()
    quad_sums(knot_ref, first_ref, w_ref, att_ref, quad_ref, hits_ref)
    for move in kept:
        move.wait()
    row = lax.broadcasted_iota(jnp.int32, (8, 128), 0)
    sources = lax.broadcasted_iota(jnp.int32, (128, 128), 0).astype(F32)
    pixels = lax.broadcasted_iota(jnp.int32, (SEATS, 128), 1)
    seat_row = lax.broadcasted_iota(jnp.int32, (SEATS, 128), 0)
    blank = jnp.zeros((48, 128), BF16)

    def keep(k):
        return pltpu.make_async_copy(arr_ref.at[pl.ds(k * ROOM, BLOCK_ROWS)],
                                     keep_ref.at[pl.ds(k * ROOM, BLOCK_ROWS)], stored.at[k])

    def part_copy(i):
        to_y, to_zh = times[i]
        return pltpu.make_async_remote_copy(
            src_ref=sums_ref.at[pl.ds(PIX * TERMS + (to_y * 2 + to_zh) * HROWS, HROWS)], dst_ref=parts_ref.at[i],
            send_sem=sent1.at[i], recv_sem=landed1.at[i], device_id=shards[i], device_id_type=pl.DeviceIdType.MESH)

    def cross():
        return pltpu.make_async_remote_copy(
            src_ref=pair_ref, dst_ref=across_ref, send_sem=sent2.at[0], recv_sem=landed2.at[0],
            device_id=partner, device_id_type=pl.DeviceIdType.MESH)

    def chunk_step(chunk, _):
        pair = 1 - (chunk // 4 + 3) // 4

        @pl.when(chunk == 5)
        def _():
            for i in range(TIMES - 1):
                part_copy(i).start()

        @pl.when(chunk == 12)
        def _():
            for i in range(TIMES - 1):
                part_copy(i).wait()

            def add(g, _):
                at = pl.multiple_of(g * 16, 16)
                total = sums_ref[pl.ds(PIX * TERMS + tm * HROWS + at, 16), :]
                for i in range(TIMES - 1):
                    total = total + parts_ref[i, pl.ds(at, 16), :]
                pair_ref[pl.ds(at, 16), :] = total
                return 0

            lax.fori_loop(0, TERMS, add, 0)

        @pl.when(chunk == 13)
        def _():
            cross().start()

        for i in range(CHUNK):
            k = chunk * CHUNK + i
            arrival = landing(in_ref, arr_ref, sent, landed, k, routes[2][1])

            @pl.when(jnp.logical_and(chunk != 0, chunk != 4))
            def _():
                arrival.wait_recv()

            keep(k).start()

        def group(g, _):
            for j in range(0, STEP, 2):
                start = (chunk * CHUNK + g // 2) * ROOM + (g % 2 * STEP + j) * FIELDS
                lefts, hits = [], []
                for i in range(2):
                    v = arr_ref[pl.ds(start + i * FIELDS, 8), :]
                    within = v - jnp.floor(v * (1.0 / SRC)) * SRC
                    lefts.append(left_side(v, row))
                    hits.append((within[6:7, :] == sources).astype(F32).astype(BF16))
                left = jnp.concatenate([jnp.concatenate([lefts[0], blank], axis=1),
                                        jnp.concatenate([blank, lefts[1]], axis=1)], axis=0)
                out = lax.dot_general(left, jnp.concatenate(hits, axis=1), (((1,), (1,)), ((), ())),
                                      preferred_element_type=F32)
                for i in range(2):
                    both = out[48 * i:48 * i + 24] + out[48 * i + 24:48 * i + 48]
                    for n in range(3):
                        spread_ref[pl.ds(8 * n * PITCH + g * STEP + j + i, 8, stride=PITCH), :] = both[8 * n:8 * n + 8]
            return 0

        lax.fori_loop(0, CHUNK * SEATS // STEP, group, 0)
        places = []
        for i in range(CHUNK):
            k = chunk * CHUNK + i
            whole = arr_ref[pl.ds(k * ROOM + 6, SEATS, stride=FIELDS), :]
            pixel = jnp.floor(whole * (1.0 / SRC)).astype(jnp.int32)
            places.append((pixel == pixels).astype(F32))
            line = jnp.sum(jnp.where(pixels == seat_row, pixel, 0), axis=0, keepdims=True)
            pix_ref[pl.ds(k, 1), :] = jnp.maximum(line, 0) + pair * PIX
        places.append(jnp.zeros((128 - CHUNK * SEATS, 128), F32))
        place = jnp.concatenate(places, axis=0).T.astype(BF16)
        place = jnp.concatenate([place, place], axis=1)
        for n in range(TERMS):
            at = n + (2 if n >= 6 else 0) + (1 if n >= 13 else 0)
            value = spread_ref[pl.ds(at * PITCH, 128), :]
            high = value.astype(BF16)
            low = (value - high.astype(F32)).astype(BF16)
            added = jnp.dot(place, jnp.concatenate([high, low], axis=0), preferred_element_type=F32)
            for part in range(TIMES):
                rows = pl.ds(pair * (PIX * TERMS) + part * HROWS + n * HALF, HALF)
                sums_ref[rows, :] = sums_ref[rows, :] + added[part * HALF:(part + 1) * HALF]
        return 0

    lax.fori_loop(0, CHUNKS, chunk_step, 0)
    cross().wait()

    def take(g, _):
        at = pl.multiple_of(g * 16, 16)
        rows = pl.ds(tm * HROWS + at, 16)
        sums_ref[rows, :] = sums_ref[rows, :] + across_ref[pl.ds(at, 16), :]
        return 0

    lax.fori_loop(0, TERMS, take, 0)
    for copy in copies:
        copy.wait_send()

    def kept_step(k, _):
        keep(k).wait()
        return 0

    lax.fori_loop(0, SLOTS, kept_step, 0)


def gather_tiles(packed, attitude, weight, knots, first):
    return pl.pallas_call(
        gather_kernel,
        out_shape=(
            jax.ShapeDtypeStruct((SLOTS * ROOM, 128), F32),
            jax.ShapeDtypeStruct((2 * PIX * TERMS, 128), F32),
            jax.ShapeDtypeStruct((SLOTS, 128), jnp.int32),
            jax.ShapeDtypeStruct((SPAN, 128), F32),
            jax.ShapeDtypeStruct((TILES, 128), BF16),
        ),
        in_specs=[HBM, HBM, HBM, VMEM, SMEM],
        out_specs=(HBM, VMEM, VMEM, VMEM, VMEM),
        scratch_shapes=[
            pltpu.VMEM((SLOTS * ROOM, 128), F32),
            pltpu.VMEM((16, TILES, 128), F32),
            pltpu.VMEM((TILES, 128), F32),
            pltpu.VMEM((24 * PITCH, 128), F32),
            pltpu.VMEM((TIMES - 1, HROWS, 128), F32),
            pltpu.VMEM((HROWS, 128), F32),
            pltpu.VMEM((HROWS, 128), F32),
            pltpu.SemaphoreType.DMA((SLOTS,)),
            pltpu.SemaphoreType.DMA((SLOTS,)),
            pltpu.SemaphoreType.DMA((6,)),
            pltpu.SemaphoreType.DMA((SLOTS,)),
            pltpu.SemaphoreType.DMA((TIMES - 1,)),
            pltpu.SemaphoreType.DMA((TIMES - 1,)),
            pltpu.SemaphoreType.DMA((1,)),
            pltpu.SemaphoreType.DMA((1,)),
        ],
        compiler_params=params(collective_id=1, has_side_effects=True),
        name="gather_tiles",
    )(packed, attitude, weight, knots, first)


def damped_solve(entries, target, order):
    factor = {}
    for column in range(order):
        pivot = entries[column, column] + 1.0
        for earlier in range(column):
            pivot = pivot - factor[column, earlier] * factor[column, earlier]
        pivot = jnp.sqrt(pivot)
        factor[column, column] = pivot
        for below in range(column + 1, order):
            current = entries[column, below]
            for earlier in range(column):
                current = current - factor[below, earlier] * factor[column, earlier]
            factor[below, column] = current / pivot
    forward = []
    for column in range(order):
        current = target[column]
        for earlier in range(column):
            current = current - factor[column, earlier] * forward[earlier]
        forward.append(current / factor[column, column])
    answer = [None] * order
    for column in reversed(range(order)):
        current = forward[column]
        for later in range(column + 1, order):
            current = current - factor[later, column] * answer[later]
        answer[column] = current / factor[column, column]
    return answer


def reduce_and_solve(in_ref, table_ref, parts_ref, whole_ref, own_ref, peers, devices, opposite, tm,
                     sent1, landed1, sent2, landed2):
    copies = []
    for i, (to_y, to_zh) in enumerate(peers):
        copies.append(send(in_ref.at[pl.ds((to_y * 2 + to_zh) * HROWS, HROWS)], parts_ref.at[i],
                           sent1.at[i], landed1.at[i], devices[i]))
    for copy in copies:
        copy.wait()

    def add(g, _):
        rows = pl.ds(pl.multiple_of(g * 16, 16), 16)
        total = in_ref[pl.ds(tm * HROWS + pl.multiple_of(g * 16, 16), 16), :]
        for i in range(TIMES - 1):
            total = total + parts_ref[i, rows, :]
        whole_ref[rows, :] = total
        return 0

    lax.fori_loop(0, TERMS, add, 0, unroll=4)
    sums = [whole_ref[pl.ds(term * HALF, HALF), :] for term in range(TERMS)]
    entries = {key: sums[at] for key, at in TERM_ROW.items() if key[1] < 5}
    target = [sums[TERM_ROW[a, 5]] for a in range(5)]
    for a, value in enumerate(damped_solve(entries, target, 5)):
        own_ref[pl.ds(a, HALF, stride=5), :] = value
    part = pl.ds(tm * HALF * 5, HALF * 5)
    table_ref[part, :] = own_ref[...]
    pair = pl.ds(PIX * 5 + tm * HALF * 5, HALF * 5)
    copies = []
    for i, device in enumerate(opposite):
        copies.append(send(own_ref, table_ref.at[pair], sent2.at[TIMES + i], landed2.at[TIMES + i], device))
        if i < TIMES - 1:
            copies.append(send(own_ref, table_ref.at[part], sent2.at[i], landed2.at[i], devices[i]))
    for copy in copies:
        copy.wait()


def knot_hits(knot_row, first):
    lane = lax.broadcasted_iota(jnp.int32, (SPAN, TILES), 0)
    return (lane == knot_row - first).astype(F32)


def split_dot(hits, value):
    high = value.astype(BF16)
    low = (value - high.astype(F32)).astype(BF16)
    return (jnp.dot(hits, high, preferred_element_type=F32)
            + jnp.dot(hits, low, preferred_element_type=F32))


def quad_sums(knot_ref, first_ref, w_ref, att_ref, out_ref, hits_ref):
    hits = knot_hits(knot_ref[...], first_ref[0])
    flipped = hits.T
    hits_ref[...] = jnp.concatenate([flipped] * 3 + [jnp.zeros_like(flipped)], axis=1).astype(BF16)
    hits = hits.astype(BF16)
    lane = lax.broadcasted_iota(jnp.int32, (SPAN, 128), 1)
    total = jnp.zeros((SPAN, 128), F32)
    weight = w_ref[...]
    for m in range(4):
        for c in range(4):
            scaled = weight * att_ref[4 * m + c]
            for e in range(c, 4):
                sums = split_dot(hits, scaled * att_ref[4 * m + e])
                at = 14 * m + KNOT_PAIRS.index((c, e))
                total = total + jnp.where(lane == at, jnp.sum(sums, axis=1, keepdims=True), 0.0)
    out_ref[...] = total


def apply_kernel(pix_ref, where_ref, first_ref, normals_hbm, tiles_hbm, knot_ref, w_ref, att_hbm, quad_ref, hits_ref,
                 out_ref, attitude_ref, table_ref, normals_ref, parts_ref, whole_ref, own_ref, arr_ref, fixed_ref, back_ref, att_ref,
                 settled_ref, edge_ref, head_ref, next_ref, piece_ref, pieces_ref,
                 sent, landed, loaded, given, taken, sent1, landed1, sent2, landed2):
    tm, sky = lax.axis_index("tm"), lax.axis_index("sky")
    y, zh, x, zl, c0 = place_of()
    block = tm * OWNERS + sky
    after = ((block + 1) // OWNERS % TIMES, (block + 1) % OWNERS)
    before = ((block + 127) // OWNERS % TIMES, (block + 127) % OWNERS)
    has_after, has_before = block < TIMES * OWNERS - 1, block > 0
    peers = [(tm, (sky + d) % OWNERS) for d in range(1, OWNERS)]
    parts = 8
    size = SLOTS // parts * ROOM

    def load(part):
        rows = pl.ds(part * size, size)
        return pltpu.make_async_copy(tiles_hbm.at[rows], arr_ref.at[rows], loaded.at[part])

    load_sums = pltpu.make_async_copy(normals_hbm.at[pl.ds(0, PIX * TERMS)], normals_ref, loaded.at[parts + 1])
    load_sums.start()
    for part in range(parts):
        load(part).start()
    load_att = pltpu.make_async_copy(att_hbm, att_ref, loaded.at[parts])
    load_att.start()
    edge_ref[1] = jnp.zeros((8, 128), F32)
    next_ref[...] = jnp.zeros((4, 8, 128), F32)
    times = times_of(y, zh)
    others = times + [(y, zh)]
    opposite = [device_of(to_y, to_zh, (x + 2) % 4, zl, c0) for to_y, to_zh in others]
    shards = [device_of(to_y, to_zh, x, zl, c0) for to_y, to_zh in times]
    greet(shards + opposite + peers + [after, before] + [to for k, (_, to) in enumerate(routes_of()) if k not in OWN])
    load_sums.wait()
    reduce_and_solve(normals_ref, table_ref, parts_ref, whole_ref, own_ref, times, shards, opposite, tm,
                     sent1, landed1, sent2, landed2)

    def give(k):
        d, dz, dc, h, pair = move_of(k)
        to = device_of(y, (zh + dz * h) % 2, (x + 4 - d) % 4, (zl + dz) % 2, (c0 + dc) % 2)
        seat = ((x + 2 * pair) % 4 * 4 + zl * 2 + c0) * CLASSES + h
        return pltpu.make_async_remote_copy(
            src_ref=fixed_ref.at[pl.ds(k * SEATS, SEATS)], dst_ref=back_ref.at[pl.ds(seat * SEATS, SEATS)],
            send_sem=given.at[k], recv_sem=taken.at[k], device_id=to, device_id_type=pl.DeviceIdType.MESH), seat

    def is_own(k):
        return jnp.logical_and(k < 16, k % 8 < 2)

    def pass_on(k):
        copy, seat = give(k)

        @pl.when(jnp.logical_not(is_own(k)))
        def _():
            copy.start()

        @pl.when(is_own(k))
        def _():
            back_ref[pl.ds(seat * SEATS, SEATS), :] = fixed_ref[pl.ds(k * SEATS, SEATS), :]

    row = lax.broadcasted_iota(jnp.int32, (8, 128), 0)

    def pick(step, _):
        k, first = step // 2, step % 2 * STEP

        @pl.when(step % (2 * SLOTS // parts) == 0)
        def _():
            load(step // (2 * SLOTS // parts)).wait()

        for j in range(STEP):
            v = arr_ref[pl.ds(k * ROOM + (first + j) * FIELDS, 8), :]
            table = table_ref[pl.ds(pix_ref[k, first + j] * 5, 8), :]
            within = (v - jnp.floor(v * (1.0 / SRC)) * SRC).astype(jnp.int32)
            at = jnp.broadcast_to(lax.bitwise_and(within[6:7, :], 127), (8, 128))
            picked = jnp.take_along_axis(table, at, axis=1)
            terms = jnp.where(row < 5, v * picked, jnp.where(row == 5, -v, 0.0))
            fixed_ref[pl.ds(k * SEATS + first + j, 1), :] = -jnp.sum(terms, axis=0, keepdims=True)

        @pl.when(jnp.logical_and(first == 0, k > 0))
        def _():
            pass_on(k - 1)

        return 0

    lax.fori_loop(0, 2 * SLOTS, pick, 0)
    pass_on(SLOTS - 1)
    load_att.wait()

    def settle(k, _):
        @pl.when(jnp.logical_not(is_own(k)))
        def _():
            give(k)[0].wait()

        return 0

    lax.fori_loop(0, SLOTS, settle, 0)

    def fetch(g, _):
        for j in range(16):
            t = g * 16 + j
            settled_ref[pl.ds(t, 1), :] = back_ref[pl.ds(where_ref[t], 1), :]
        return 0

    lax.fori_loop(0, TILES // 16, fetch, 0)
    weight = w_ref[...]
    settled = settled_ref[...] / jnp.sqrt(weight)
    settled_ref[...] = settled
    hits = knot_hits(knot_ref[...], first_ref[0]).astype(BF16)
    lane = lax.broadcasted_iota(jnp.int32, (SPAN, 128), 1)
    total = quad_ref[...]
    scaled = weight * settled
    for m in range(4):
        for c in range(4):
            sums = split_dot(hits, scaled * att_ref[4 * m + c])
            at = 14 * m + 10 + c
            total = total + jnp.where(lane == at, jnp.sum(sums, axis=1, keepdims=True), 0.0)
    lane40 = lax.broadcasted_iota(jnp.int32, (SPAN + 8, 128), 1)
    padded = jnp.concatenate([total, jnp.zeros((8, 128), F32)], axis=0)
    moved = jnp.where(lane40 < 14, padded, 0.0)
    for m in range(1, 4):
        shifted = pltpu.roll(pltpu.roll(padded, m, 0), 128 - 14 * m, 1)
        moved = moved + jnp.where(lane40 < 14, shifted, 0.0)
    edge_ref[0] = moved[SPAN:]
    def onward(to):
        return pltpu.make_async_remote_copy(
            src_ref=edge_ref.at[0], dst_ref=edge_ref.at[1], send_sem=sent.at[0], recv_sem=landed.at[0],
            device_id=to, device_id_type=pl.DeviceIdType.MESH)

    def backward(to):
        return pltpu.make_async_remote_copy(
            src_ref=head_ref, dst_ref=next_ref, send_sem=sent.at[1], recv_sem=landed.at[1],
            device_id=to, device_id_type=pl.DeviceIdType.MESH)

    @pl.when(has_after)
    def _():
        onward(after).start()

    @pl.when(has_before)
    def _():
        onward(before).wait_recv()

    sums = jnp.concatenate([moved[:8] + edge_ref[1], moved[8:SPAN]], axis=0)

    def column(at):
        return jnp.broadcast_to(sums[:, at:at + 1], (SPAN, 128))

    entries = {pair: column(n) for n, pair in enumerate(KNOT_PAIRS)}
    answer = damped_solve(entries, [column(10 + c) for c in range(4)], 4)
    for c in range(4):
        head_ref[c] = answer[c][:8]

    @pl.when(has_before)
    def _():
        backward(before).start()

    row32 = lax.broadcasted_iota(jnp.int32, (SPAN, 128), 0)
    row8 = lax.broadcasted_iota(jnp.int32, (8, 128), 0)
    piece = jnp.zeros((8, 128), F32)
    for c in range(4):
        line = jnp.sum(jnp.where(lane == row32 + (sky % 4) * SPAN, answer[c], 0.0), axis=0, keepdims=True)
        piece = jnp.where(row8 == c, line, piece)
    piece_ref[...] = piece
    copies = [send(piece_ref, pieces_ref.at[sky], sent.at[1 + d], landed.at[1 + d], peers[d - 1])
              for d in range(1, OWNERS)]
    pieces_ref[sky] = piece

    @pl.when(has_after)
    def _():
        backward(after).wait_recv()

    fix = None
    for m in range(4):
        for c in range(4):
            both = jnp.concatenate([answer[c], next_ref[c]], axis=0)
            value = both[m:m + SPAN]
            high = value.astype(BF16)
            rest = value - high.astype(F32)
            middle = rest.astype(BF16)
            low = (rest - middle.astype(F32)).astype(BF16)
            table = jnp.concatenate([high, middle, low, jnp.zeros_like(high)], axis=0)
            term = att_ref[4 * m + c] * jnp.dot(hits_ref[...], table, preferred_element_type=F32)
            fix = term if fix is None else fix + term
    out_ref[...] = settled_ref[...] - fix
    for copy in copies:
        copy.wait()
    for j in range(4):
        total = pieces_ref[4 * j]
        for i in range(1, 4):
            total = total + pieces_ref[4 * j + i]
        attitude_ref[:, j * 128:(j + 1) * 128] = total[:4]

    @pl.when(has_after)
    def _():
        onward(after).wait_send()

    @pl.when(has_before)
    def _():
        backward(before).wait_send()


def apply_updates(pix, where, first, normals, tiles, knots, weight, attitude, quad, hits):
    return pl.pallas_call(
        apply_kernel,
        out_shape=(
            jax.ShapeDtypeStruct((TILES, 128), F32),
            jax.ShapeDtypeStruct((4, SPAN * OWNERS), F32),
            jax.ShapeDtypeStruct((2 * PIX * 5 + 8, 128), F32),
        ),
        in_specs=[SMEM, SMEM, SMEM, HBM, HBM, VMEM, VMEM, HBM, VMEM, VMEM],
        out_specs=(VMEM, VMEM, VMEM),
        scratch_shapes=[
            pltpu.VMEM((PIX * TERMS, 128), F32),
            pltpu.VMEM((TIMES - 1, HROWS, 128), F32),
            pltpu.VMEM((HROWS, 128), F32),
            pltpu.VMEM((HALF * 5, 128), F32),
            pltpu.VMEM((SLOTS * ROOM, 128), F32),
            pltpu.VMEM((SLOTS * SEATS, 128), F32),
            pltpu.VMEM((SLOTS * SEATS, 128), F32),
            pltpu.VMEM((16, TILES, 128), F32),
            pltpu.VMEM((TILES, 128), F32),
            pltpu.VMEM((2, 8, 128), F32),
            pltpu.VMEM((4, 8, 128), F32),
            pltpu.VMEM((4, 8, 128), F32),
            pltpu.VMEM((8, 128), F32),
            pltpu.VMEM((OWNERS, 8, 128), F32),
            pltpu.SemaphoreType.DMA((OWNERS + 1,)),
            pltpu.SemaphoreType.DMA((OWNERS + 1,)),
            pltpu.SemaphoreType.DMA((10,)),
            pltpu.SemaphoreType.DMA((SLOTS,)),
            pltpu.SemaphoreType.DMA((SLOTS,)),
            pltpu.SemaphoreType.DMA((TIMES - 1,)),
            pltpu.SemaphoreType.DMA((TIMES - 1,)),
            pltpu.SemaphoreType.DMA((2 * TIMES,)),
            pltpu.SemaphoreType.DMA((2 * TIMES,)),
        ],
        compiler_params=params(collective_id=4, has_side_effects=True),
        name="apply_updates",
    )(pix, where, first, normals, tiles, knots, weight, attitude, quad, hits)


def emit_kernel(final_ref, attitude_ref, table_ref, final_out, attitude_out, update_out):
    final_out[...] = final_ref[...]
    attitude_out[...] = attitude_ref[...]
    for p in range(PIX):
        update_out[:, p * 128:(p + 1) * 128] = table_ref[p * 5:p * 5 + 5, :]


def emit(final, attitude, table):
    return pl.pallas_call(
        emit_kernel,
        out_shape=(
            jax.ShapeDtypeStruct((TILES, 128), F32),
            jax.ShapeDtypeStruct((4, SPAN * OWNERS), F32),
            jax.ShapeDtypeStruct((5, PIX * SRC), F32),
        ),
        in_specs=[VMEM, VMEM, VMEM],
        out_specs=(VMEM, VMEM, VMEM),
        compiler_params=params(),
        name="emit",
    )(final, attitude, table)


def body(residual, obs_weight, source_partials, attitude_partials, source_index,
         tile_pixel, tile_knot, pixel_slot):
    block = lax.axis_index("tm") * OWNERS + lax.axis_index("sky")
    first = (block * SPAN).reshape(1)
    knots = tile_knot.reshape(1, TILES)
    packed, where = pack(tile_pixel, pixel_slot, residual, obs_weight, source_partials, source_index)
    arrived, normals, pix, quad, hits = gather_tiles(packed, attitude_partials, obs_weight, knots, first)
    final, attitude_update, table = apply_updates(
        pix, where, first, normals, arrived, knots, obs_weight, attitude_partials, quad, hits)
    final, attitude_update, source_update = emit(final, attitude_update, table)
    return final, source_update, attitude_update


def solution(mesh):
    in_specs = (
        P(("tm", "sky"), None),
        P(("tm", "sky"), None),
        P(None, ("tm", "sky"), None),
        P(None, ("tm", "sky"), None),
        P(("tm", "sky"), None),
        P(("tm", "sky")),
        P(("tm", "sky")),
        P(),
    )
    out_specs = (P(("tm", "sky"), None), P(None, "sky"), P(None, "tm"))
    return jax.shard_map(body, mesh=mesh, in_specs=in_specs, out_specs=out_specs, check_vma=False)
```

```python
import functools

import jax
import jax.numpy as jnp
from jax import lax
from jax.experimental import pallas as pl
from jax.experimental.pallas import tpu as pltpu
from jax.sharding import PartitionSpec as P

TILES = 512
OWNERS = 16
TIMES = 8
CAP = 96
PIX = 128
SRC = 128
FIELDS = 7
CLASSES = 2
SEATS = CAP // CLASSES
SLOTS = OWNERS * CLASSES
BLOCK_ROWS = SEATS * FIELDS
ROWS_IN = SLOTS * BLOCK_ROWS + 8
SPAN = 32
TERMS = 20
HALF = PIX // TIMES
HROWS = HALF * TERMS
KNOT_PAIRS = tuple((c, e) for c in range(4) for e in range(c, 4))
TERM_ROW = {
    (0, 0): 0, (1, 1): 1, (2, 2): 2, (3, 3): 3, (4, 4): 4, (0, 5): 5,
    (0, 1): 6, (1, 2): 7, (2, 3): 8, (3, 4): 9, (4, 5): 10, (0, 4): 11, (1, 5): 12,
    (0, 2): 13, (1, 3): 14, (2, 4): 15, (3, 5): 16, (0, 3): 17, (1, 4): 18, (2, 5): 19,
}
VMEM = pl.BlockSpec(memory_space=pltpu.VMEM)
SMEM = pl.BlockSpec(memory_space=pltpu.SMEM)
F32 = jnp.float32
BF16 = jnp.bfloat16


def params(**kw):
    return pltpu.CompilerParams(vmem_limit_bytes=60 * 1024 * 1024, **kw)


def pack_kernel(pixel_ref, slot_ref, res_ref, w_ref, part_ref, idx_ref,
                out_ref, where_ref, count_ref, stage_ref):
    for o in range(OWNERS):
        count_ref[o] = 0
    nothing = jnp.zeros((SEATS, 128), F32)

    def clear(b, _):
        base = pl.multiple_of(b * BLOCK_ROWS, 8)
        for i in range(FIELDS):
            out_ref[pl.ds(base + i * SEATS, SEATS), :] = nothing
        out_ref[pl.ds(base + 6, SEATS, stride=FIELDS), :] = nothing - 1.0
        return 0

    lax.fori_loop(0, SLOTS, clear, 0)

    def scale(g, _):
        rows = pl.ds(pl.multiple_of(g * 8, 8), 8)
        root = jnp.sqrt(w_ref[rows, :])
        for a in range(5):
            stage_ref[a, rows, :] = part_ref[a, rows, :] * root
        stage_ref[5, rows, :] = res_ref[rows, :] * root
        stage_ref[6, rows, :] = idx_ref[rows, :].astype(F32)
        return 0

    lax.fori_loop(0, TILES // 8, scale, 0, unroll=4)

    def place(g, _):
        for j in range(8):
            t = g * 8 + j
            seat = slot_ref[pixel_ref[t]]
            owner = lax.shift_right_logical(seat, 7)
            rank = count_ref[owner]
            count_ref[owner] = rank + 1
            block = owner * CLASSES + lax.bitwise_and(rank, 1)
            position = lax.shift_right_logical(rank, 1)
            where_ref[t] = block * SEATS + position
            base = block * BLOCK_ROWS + position * FIELDS
            for f in range(6):
                out_ref[pl.ds(base + f, 1), :] = stage_ref[f, pl.ds(t, 1), :]
            first = (lax.bitwise_and(seat, 127) * SRC).astype(F32)
            out_ref[pl.ds(base + 6, 1), :] = stage_ref[6, pl.ds(t, 1), :] + first
        return 0

    lax.fori_loop(0, TILES // 8, place, 0)


def pack(tile_pixel, pixel_slot, residual, weight, partials, index):
    return pl.pallas_call(
        pack_kernel,
        out_shape=(
            jax.ShapeDtypeStruct((ROWS_IN, 128), F32),
            jax.ShapeDtypeStruct((TILES,), jnp.int32),
        ),
        in_specs=[SMEM, SMEM, VMEM, VMEM, VMEM, VMEM],
        out_specs=(VMEM, SMEM),
        scratch_shapes=[pltpu.SMEM((OWNERS,), jnp.int32), pltpu.VMEM((FIELDS, TILES, 128), F32)],
        compiler_params=params(),
        name="pack",
    )(tile_pixel, pixel_slot, residual, weight, partials, index)


def place_of():
    tm, sky = lax.axis_index("tm"), lax.axis_index("sky")
    return tm // 2, tm % 2, sky // 4, (sky // 2) % 2, sky % 2


def device_of(y, zh, x, zl, c):
    return (y * 2 + zh, x * 4 + zl * 2 + c)


def send(src, dst, sent, landed, device):
    copy = pltpu.make_async_remote_copy(
        src_ref=src, dst_ref=dst, send_sem=sent, recv_sem=landed,
        device_id=device, device_id_type=pl.DeviceIdType.MESH)
    copy.start()
    return copy


def greet(devices):
    barrier = pltpu.get_barrier_semaphore()
    for device in devices:
        pl.semaphore_signal(barrier, inc=1, device_id=device, device_id_type=pl.DeviceIdType.MESH)
    pl.semaphore_wait(barrier, len(devices))


def move_of(k):
    rest, near = k // 16, (k // 8 + 1) % 2 * (1 - k // 16)
    d = rest * (1 + k % 2 * 2)
    dz = rest * (1 - k // 2 % 2) + (1 - rest) * (k // 4 % 2)
    dc = rest * (k // 8 % 2) + (1 - rest) * (k // 2 % 2)
    h = rest * (k // 4 % 2) + (1 - rest) * (k % 2)
    return d, dz, dc, h, near


MOVES = [move_of(k) for k in range(SLOTS)]
OWN = (0, 1, 8, 9)
CHUNK = 2
CHUNKS = SLOTS // CHUNK
STEP = 24
PITCH = 136
ROOM = BLOCK_ROWS + 8
HBM = pl.BlockSpec(memory_space=pltpu.HBM)


def routes_of():
    y, zh, x, zl, c = place_of()
    routes = []
    for d, dz, dc, h, pair in MOVES:
        far, zl_to, c_to = (x + d) % 4, (zl + dz) % 2, (c + dc) % 2
        owner = (far + 2 * pair) % 4 * 4 + zl_to * 2 + c_to
        routes.append((owner * CLASSES + h, device_of(y, (zh + dz * h) % 2, far, zl_to, c_to)))
    return routes


def times_of(y, zh):
    return [((y + d) % 4, (zh + z) % 2) for d, z in ((2, 1), (2, 0), (1, 1), (3, 1), (1, 0), (3, 0), (0, 1))]


def pair_products(v, row):
    low5, low4 = row < 5, row < 4
    one = pltpu.roll(v, 1, 0)
    first = jnp.where(low5, v, pltpu.roll(v, 5, 0))
    second = jnp.where(low5, pltpu.roll(v, 7, 0), one)
    third = jnp.where(low4, v, pltpu.roll(v, 4, 0))
    fourth = jnp.where(low4, pltpu.roll(v, 6, 0), one)
    return jnp.concatenate([first * v, first * second, third * fourth], axis=0)


def left_side(v, row):
    products = pair_products(v, row)
    high = products.astype(BF16).astype(F32)
    return jnp.concatenate([high, products - high], axis=0).astype(BF16)


def landing(in_ref, arr_ref, sent, landed, k, to):
    return pltpu.make_async_remote_copy(
        src_ref=in_ref.at[pl.ds(k * BLOCK_ROWS, BLOCK_ROWS)],
        dst_ref=arr_ref.at[pl.ds(k * ROOM, BLOCK_ROWS)], send_sem=sent.at[k], recv_sem=landed.at[k],
        device_id=to, device_id_type=pl.DeviceIdType.MESH)


def gather_kernel(in_ref, att_hbm, w_hbm, knot_ref, first_ref,
                  keep_ref, sums_ref, pix_ref, quad_ref, hits_ref,
                  arr_ref, att_ref, w_ref, spread_ref, parts_ref, pair_ref, across_ref,
                  sent, landed, local, stored, sent1, landed1, sent2, landed2):
    routes = routes_of()
    load_att = pltpu.make_async_copy(att_hbm, att_ref, local.at[4])
    load_w = pltpu.make_async_copy(w_hbm, w_ref, local.at[5])
    load_att.start()
    load_w.start()
    y, zh, x, zl, c = place_of()
    rows_y = [(y + d) % 4 for d in (2, 1, 3)]
    partner = device_of(y, zh, (x + 2) % 4, zl, c)
    shards = [device_of(to_y, zh, x, zl, c) for to_y in rows_y]
    greet([to for k, (_, to) in enumerate(routes) if k not in OWN] + shards + [partner])
    copies = []
    for k, (block, to) in enumerate(routes):
        if k not in OWN:
            copies.append(send(in_ref.at[pl.ds(block * BLOCK_ROWS, BLOCK_ROWS)],
                               arr_ref.at[pl.ds(k * ROOM, BLOCK_ROWS)], sent.at[k], landed.at[k], to))
    kept = []
    for i, k in enumerate(OWN):
        kept.append(pltpu.make_async_copy(in_ref.at[pl.ds(routes[k][0] * BLOCK_ROWS, BLOCK_ROWS)],
                                          arr_ref.at[pl.ds(k * ROOM, BLOCK_ROWS)], local.at[i]))
        kept[-1].start()

    def clear(g, _):
        spread_ref[pl.ds(pl.multiple_of(g * 8, 8), 8), :] = jnp.zeros((8, 128), F32)
        return 0

    lax.fori_loop(0, 24 * PITCH // 8, clear, 0, unroll=4)

    def clear_sums(g, _):
        sums_ref[pl.ds(pl.multiple_of(g * 16, 16), 16), :] = jnp.zeros((16, 128), F32)
        return 0

    lax.fori_loop(0, 2 * PIX * TERMS // 16, clear_sums, 0, unroll=4)
    load_att.wait()
    load_w.wait()
    quad_sums(knot_ref, first_ref, w_ref, att_ref, quad_ref, hits_ref)
    for move in kept:
        move.wait()
    row = lax.broadcasted_iota(jnp.int32, (8, 128), 0)
    sources = lax.broadcasted_iota(jnp.int32, (128, 128), 0).astype(F32)
    pixels = lax.broadcasted_iota(jnp.int32, (SEATS, 128), 1)
    seat_row = lax.broadcasted_iota(jnp.int32, (SEATS, 128), 0)
    blank = jnp.zeros((48, 128), BF16)

    def keep(k):
        return pltpu.make_async_copy(arr_ref.at[pl.ds(k * ROOM, BLOCK_ROWS)],
                                     keep_ref.at[pl.ds(k * ROOM, BLOCK_ROWS)], stored.at[k])

    def part_copy(i):
        return pltpu.make_async_remote_copy(
            src_ref=sums_ref.at[pl.ds(PIX * TERMS + rows_y[i] * 2 * HROWS, 2 * HROWS)], dst_ref=parts_ref.at[i],
            send_sem=sent1.at[i], recv_sem=landed1.at[i], device_id=shards[i], device_id_type=pl.DeviceIdType.MESH)

    def cross():
        return pltpu.make_async_remote_copy(
            src_ref=pair_ref, dst_ref=across_ref, send_sem=sent2.at[0], recv_sem=landed2.at[0],
            device_id=partner, device_id_type=pl.DeviceIdType.MESH)

    def chunk_step(chunk, _):
        pair = 1 - (chunk // 4 + 3) // 4

        @pl.when(chunk == 5)
        def _():
            for i in range(3):
                part_copy(i).start()

        @pl.when(chunk == 11)
        def _():
            for i in range(3):
                part_copy(i).wait()

            def add(g, _):
                at = pl.multiple_of(g * 16, 16)
                total = sums_ref[pl.ds(PIX * TERMS + y * 2 * HROWS + at, 16), :]
                for i in range(3):
                    total = total + parts_ref[i, pl.ds(at, 16), :]
                pair_ref[pl.ds(at, 16), :] = total
                return 0

            lax.fori_loop(0, 2 * TERMS, add, 0)

        @pl.when(chunk == 12)
        def _():
            cross().start()

        for i in range(CHUNK):
            k = chunk * CHUNK + i
            arrival = landing(in_ref, arr_ref, sent, landed, k, routes[2][1])

            @pl.when(jnp.logical_and(chunk != 0, chunk != 4))
            def _():
                arrival.wait_recv()

            keep(k).start()

        def group(g, _):
            for j in range(0, STEP, 2):
                start = (chunk * CHUNK + g // 2) * ROOM + (g % 2 * STEP + j) * FIELDS
                lefts, hits = [], []
                for i in range(2):
                    v = arr_ref[pl.ds(start + i * FIELDS, 8), :]
                    within = v - jnp.floor(v * (1.0 / SRC)) * SRC
                    lefts.append(left_side(v, row))
                    hits.append((within[6:7, :] == sources).astype(F32).astype(BF16))
                left = jnp.concatenate([jnp.concatenate([lefts[0], blank], axis=1),
                                        jnp.concatenate([blank, lefts[1]], axis=1)], axis=0)
                out = lax.dot_general(left, jnp.concatenate(hits, axis=1), (((1,), (1,)), ((), ())),
                                      preferred_element_type=F32)
                for i in range(2):
                    both = out[48 * i:48 * i + 24] + out[48 * i + 24:48 * i + 48]
                    for n in range(3):
                        spread_ref[pl.ds(8 * n * PITCH + g * STEP + j + i, 8, stride=PITCH), :] = both[8 * n:8 * n + 8]
            return 0

        lax.fori_loop(0, CHUNK * SEATS // STEP, group, 0)
        places = []
        for i in range(CHUNK):
            k = chunk * CHUNK + i
            whole = arr_ref[pl.ds(k * ROOM + 6, SEATS, stride=FIELDS), :]
            pixel = jnp.floor(whole * (1.0 / SRC)).astype(jnp.int32)
            places.append((pixel == pixels).astype(F32))
            line = jnp.sum(jnp.where(pixels == seat_row, pixel, 0), axis=0, keepdims=True)
            pix_ref[pl.ds(k, 1), :] = jnp.maximum(line, 0)
        places.append(jnp.zeros((128 - CHUNK * SEATS, 128), F32))
        place = jnp.concatenate(places, axis=0).T.astype(BF16)
        place = jnp.concatenate([place, place], axis=1)
        for n in range(TERMS):
            at = n + (2 if n >= 6 else 0) + (1 if n >= 13 else 0)
            value = spread_ref[pl.ds(at * PITCH, 128), :]
            high = value.astype(BF16)
            low = (value - high.astype(F32)).astype(BF16)
            added = jnp.dot(place, jnp.concatenate([high, low], axis=0), preferred_element_type=F32)
            for part in range(TIMES):
                rows = pl.ds(pair * (PIX * TERMS) + part * HROWS + n * HALF, HALF)
                sums_ref[rows, :] = sums_ref[rows, :] + added[part * HALF:(part + 1) * HALF]
        return 0

    lax.fori_loop(0, CHUNKS, chunk_step, 0)
    cross().wait()

    def take(g, _):
        at = pl.multiple_of(g * 16, 16)
        rows = pl.ds(y * 2 * HROWS + at, 16)
        sums_ref[rows, :] = sums_ref[rows, :] + across_ref[pl.ds(at, 16), :]
        return 0

    lax.fori_loop(0, 2 * TERMS, take, 0)
    for copy in copies:
        copy.wait_send()

    def kept_step(k, _):
        keep(k).wait()
        return 0

    lax.fori_loop(0, SLOTS, kept_step, 0)


def gather_tiles(packed, attitude, weight, knots, first):
    return pl.pallas_call(
        gather_kernel,
        out_shape=(
            jax.ShapeDtypeStruct((SLOTS * ROOM, 128), F32),
            jax.ShapeDtypeStruct((2 * PIX * TERMS, 128), F32),
            jax.ShapeDtypeStruct((SLOTS, 128), jnp.int32),
            jax.ShapeDtypeStruct((SPAN, 128), F32),
            jax.ShapeDtypeStruct((TILES, 128), BF16),
        ),
        in_specs=[HBM, HBM, HBM, VMEM, SMEM],
        out_specs=(HBM, VMEM, VMEM, VMEM, VMEM),
        scratch_shapes=[
            pltpu.VMEM((SLOTS * ROOM, 128), F32),
            pltpu.VMEM((16, TILES, 128), F32),
            pltpu.VMEM((TILES, 128), F32),
            pltpu.VMEM((24 * PITCH, 128), F32),
            pltpu.VMEM((3, 2 * HROWS, 128), F32),
            pltpu.VMEM((2 * HROWS, 128), F32),
            pltpu.VMEM((2 * HROWS, 128), F32),
            pltpu.SemaphoreType.DMA((SLOTS,)),
            pltpu.SemaphoreType.DMA((SLOTS,)),
            pltpu.SemaphoreType.DMA((6,)),
            pltpu.SemaphoreType.DMA((SLOTS,)),
            pltpu.SemaphoreType.DMA((3,)),
            pltpu.SemaphoreType.DMA((3,)),
            pltpu.SemaphoreType.DMA((1,)),
            pltpu.SemaphoreType.DMA((1,)),
        ],
        compiler_params=params(collective_id=1, has_side_effects=True),
        name="gather_tiles",
    )(packed, attitude, weight, knots, first)


def damped_solve(entries, target, order):
    factor = {}
    for column in range(order):
        pivot = entries[column, column] + 1.0
        for earlier in range(column):
            pivot = pivot - factor[column, earlier] * factor[column, earlier]
        pivot = jnp.sqrt(pivot)
        factor[column, column] = pivot
        for below in range(column + 1, order):
            current = entries[column, below]
            for earlier in range(column):
                current = current - factor[below, earlier] * factor[column, earlier]
            factor[below, column] = current / pivot
    forward = []
    for column in range(order):
        current = target[column]
        for earlier in range(column):
            current = current - factor[column, earlier] * forward[earlier]
        forward.append(current / factor[column, column])
    answer = [None] * order
    for column in reversed(range(order)):
        current = forward[column]
        for later in range(column + 1, order):
            current = current - factor[later, column] * answer[later]
        answer[column] = current / factor[column, column]
    return answer


def reduce_and_solve(in_ref, table_ref, second_ref, parts_ref, whole_ref, own_ref, peers, devices, opposite, tm,
                     sent1, landed1, sent2, landed2):
    copies = []
    for i, (to_y, to_zh) in enumerate(peers):
        copies.append(send(in_ref.at[pl.ds((to_y * 2 + to_zh) * HROWS, HROWS)], parts_ref.at[i],
                           sent1.at[i], landed1.at[i], devices[i]))
    for copy in copies:
        copy.wait()

    def add(g, _):
        rows = pl.ds(pl.multiple_of(g * 16, 16), 16)
        total = in_ref[pl.ds(tm * HROWS + pl.multiple_of(g * 16, 16), 16), :]
        for i in range(TIMES - 1):
            total = total + parts_ref[i, rows, :]
        whole_ref[rows, :] = total
        return 0

    lax.fori_loop(0, TERMS, add, 0, unroll=4)
    sums = [whole_ref[pl.ds(term * HALF, HALF), :] for term in range(TERMS)]
    entries = {key: sums[at] for key, at in TERM_ROW.items() if key[1] < 5}
    target = [sums[TERM_ROW[a, 5]] for a in range(5)]
    for a, value in enumerate(damped_solve(entries, target, 5)):
        own_ref[pl.ds(a, HALF, stride=5), :] = value
    part = pl.ds(tm * HALF * 5, HALF * 5)
    table_ref[part, :] = own_ref[...]
    copies = [send(own_ref, table_ref.at[part], sent2.at[i], landed2.at[i], device)
              for i, device in enumerate(devices)]

    def spread(i):
        return pltpu.make_async_remote_copy(
            src_ref=own_ref, dst_ref=second_ref.at[part], send_sem=sent2.at[TIMES + i], recv_sem=landed2.at[TIMES + i],
            device_id=opposite[i], device_id_type=pl.DeviceIdType.MESH)

    for i in range(TIMES):
        spread(i).start()
    for copy in copies:
        copy.wait()
    return spread


def knot_hits(knot_row, first):
    lane = lax.broadcasted_iota(jnp.int32, (SPAN, TILES), 0)
    return (lane == knot_row - first).astype(F32)


def split_dot(hits, value):
    high = value.astype(BF16)
    low = (value - high.astype(F32)).astype(BF16)
    return (jnp.dot(hits, high, preferred_element_type=F32)
            + jnp.dot(hits, low, preferred_element_type=F32))


def quad_sums(knot_ref, first_ref, w_ref, att_ref, out_ref, hits_ref):
    hits = knot_hits(knot_ref[...], first_ref[0])
    flipped = hits.T
    hits_ref[...] = jnp.concatenate([flipped] * 3 + [jnp.zeros_like(flipped)], axis=1).astype(BF16)
    hits = hits.astype(BF16)
    lane = lax.broadcasted_iota(jnp.int32, (SPAN, 128), 1)
    total = jnp.zeros((SPAN, 128), F32)
    weight = w_ref[...]
    for m in range(4):
        for c in range(4):
            scaled = weight * att_ref[4 * m + c]
            for e in range(c, 4):
                sums = split_dot(hits, scaled * att_ref[4 * m + e])
                at = 14 * m + KNOT_PAIRS.index((c, e))
                total = total + jnp.where(lane == at, jnp.sum(sums, axis=1, keepdims=True), 0.0)
    out_ref[...] = total


def apply_kernel(pix_ref, where_ref, first_ref, normals_hbm, tiles_hbm, knot_ref, w_ref, att_hbm, quad_ref, hits_ref,
                 out_ref, attitude_ref, table_ref, second_ref, normals_ref, parts_ref, whole_ref, own_ref, arr_ref, fixed_ref, back_ref, att_ref,
                 settled_ref, edge_ref, head_ref, next_ref, piece_ref, pieces_ref,
                 sent, landed, loaded, given, taken, sent1, landed1, sent2, landed2):
    tm, sky = lax.axis_index("tm"), lax.axis_index("sky")
    y, zh, x, zl, c0 = place_of()
    block = tm * OWNERS + sky
    after = ((block + 1) // OWNERS % TIMES, (block + 1) % OWNERS)
    before = ((block + 127) // OWNERS % TIMES, (block + 127) % OWNERS)
    has_after, has_before = block < TIMES * OWNERS - 1, block > 0
    peers = [(tm, (sky + d) % OWNERS) for d in range(1, OWNERS)]
    parts = 8
    size = SLOTS // parts * ROOM

    def load(part):
        rows = pl.ds(part * size, size)
        return pltpu.make_async_copy(tiles_hbm.at[rows], arr_ref.at[rows], loaded.at[part])

    load_sums = pltpu.make_async_copy(normals_hbm.at[pl.ds(0, PIX * TERMS)], normals_ref, loaded.at[parts + 1])
    load_sums.start()
    for part in range(parts):
        load((part + 2) % parts).start()
    load_att = pltpu.make_async_copy(att_hbm, att_ref, loaded.at[parts])
    load_att.start()
    edge_ref[1] = jnp.zeros((8, 128), F32)
    next_ref[...] = jnp.zeros((4, 8, 128), F32)
    times = times_of(y, zh)
    others = times + [(y, zh)]
    opposite = [device_of(to_y, to_zh, (x + 2) % 4, zl, c0) for to_y, to_zh in others]
    shards = [device_of(to_y, to_zh, x, zl, c0) for to_y, to_zh in times]
    greet(shards + opposite + peers + [after, before] + [to for k, (_, to) in enumerate(routes_of()) if k not in OWN])
    load_sums.wait()
    spread = reduce_and_solve(normals_ref, table_ref, second_ref, parts_ref, whole_ref, own_ref, times, shards, opposite, tm,
                              sent1, landed1, sent2, landed2)

    def give(k):
        d, dz, dc, h, pair = move_of(k)
        to = device_of(y, (zh + dz * h) % 2, (x + 4 - d) % 4, (zl + dz) % 2, (c0 + dc) % 2)
        seat = ((x + 2 * pair) % 4 * 4 + zl * 2 + c0) * CLASSES + h
        return pltpu.make_async_remote_copy(
            src_ref=fixed_ref.at[pl.ds(k * SEATS, SEATS)], dst_ref=back_ref.at[pl.ds(seat * SEATS, SEATS)],
            send_sem=given.at[k], recv_sem=taken.at[k], device_id=to, device_id_type=pl.DeviceIdType.MESH), seat

    def is_own(k):
        return jnp.logical_and(k < 16, k % 8 < 2)

    def pass_on(k):
        copy, seat = give(k)

        @pl.when(jnp.logical_not(is_own(k)))
        def _():
            copy.start()

        @pl.when(is_own(k))
        def _():
            back_ref[pl.ds(seat * SEATS, SEATS), :] = fixed_ref[pl.ds(k * SEATS, SEATS), :]

    row = lax.broadcasted_iota(jnp.int32, (8, 128), 0)

    def pick(rows_ref, step, _):
        k, first = (step // 2 + 8) % SLOTS, step % 2 * STEP

        @pl.when(step % (2 * SLOTS // parts) == 0)
        def _():
            load(k // (SLOTS // parts)).wait()

        for j in range(STEP):
            v = arr_ref[pl.ds(k * ROOM + (first + j) * FIELDS, 8), :]
            table = rows_ref[pl.ds(pix_ref[k, first + j] * 5, 8), :]
            within = (v - jnp.floor(v * (1.0 / SRC)) * SRC).astype(jnp.int32)
            at = jnp.broadcast_to(lax.bitwise_and(within[6:7, :], 127), (8, 128))
            picked = jnp.take_along_axis(table, at, axis=1)
            terms = jnp.where(row < 5, v * picked, jnp.where(row == 5, -v, 0.0))
            fixed_ref[pl.ds(k * SEATS + first + j, 1), :] = -jnp.sum(terms, axis=0, keepdims=True)

        @pl.when(jnp.logical_and(first == 0, step > 0))
        def _():
            pass_on((k + SLOTS - 1) % SLOTS)

        return 0

    lax.fori_loop(0, 2 * (SLOTS - 8), functools.partial(pick, table_ref), 0)
    for i in range(TIMES):
        spread(i).wait()
    lax.fori_loop(2 * (SLOTS - 8), 2 * SLOTS, functools.partial(pick, second_ref), 0)
    pass_on(7)
    load_att.wait()

    def settle(k, _):
        @pl.when(jnp.logical_not(is_own(k)))
        def _():
            give(k)[0].wait()

        return 0

    lax.fori_loop(0, SLOTS, settle, 0)

    def fetch(g, _):
        for j in range(16):
            t = g * 16 + j
            settled_ref[pl.ds(t, 1), :] = back_ref[pl.ds(where_ref[t], 1), :]
        return 0

    lax.fori_loop(0, TILES // 16, fetch, 0)
    weight = w_ref[...]
    settled = settled_ref[...] / jnp.sqrt(weight)
    settled_ref[...] = settled
    hits = knot_hits(knot_ref[...], first_ref[0]).astype(BF16)
    lane = lax.broadcasted_iota(jnp.int32, (SPAN, 128), 1)
    total = quad_ref[...]
    scaled = weight * settled
    for m in range(4):
        for c in range(4):
            sums = split_dot(hits, scaled * att_ref[4 * m + c])
            at = 14 * m + 10 + c
            total = total + jnp.where(lane == at, jnp.sum(sums, axis=1, keepdims=True), 0.0)
    lane40 = lax.broadcasted_iota(jnp.int32, (SPAN + 8, 128), 1)
    padded = jnp.concatenate([total, jnp.zeros((8, 128), F32)], axis=0)
    moved = jnp.where(lane40 < 14, padded, 0.0)
    for m in range(1, 4):
        shifted = pltpu.roll(pltpu.roll(padded, m, 0), 128 - 14 * m, 1)
        moved = moved + jnp.where(lane40 < 14, shifted, 0.0)
    edge_ref[0] = moved[SPAN:]
    def onward(to):
        return pltpu.make_async_remote_copy(
            src_ref=edge_ref.at[0], dst_ref=edge_ref.at[1], send_sem=sent.at[0], recv_sem=landed.at[0],
            device_id=to, device_id_type=pl.DeviceIdType.MESH)

    def backward(to):
        return pltpu.make_async_remote_copy(
            src_ref=head_ref, dst_ref=next_ref, send_sem=sent.at[1], recv_sem=landed.at[1],
            device_id=to, device_id_type=pl.DeviceIdType.MESH)

    @pl.when(has_after)
    def _():
        onward(after).start()

    @pl.when(has_before)
    def _():
        onward(before).wait_recv()

    sums = jnp.concatenate([moved[:8] + edge_ref[1], moved[8:SPAN]], axis=0)

    def column(at):
        return jnp.broadcast_to(sums[:, at:at + 1], (SPAN, 128))

    entries = {pair: column(n) for n, pair in enumerate(KNOT_PAIRS)}
    answer = damped_solve(entries, [column(10 + c) for c in range(4)], 4)
    for c in range(4):
        head_ref[c] = answer[c][:8]

    @pl.when(has_before)
    def _():
        backward(before).start()

    row32 = lax.broadcasted_iota(jnp.int32, (SPAN, 128), 0)
    row8 = lax.broadcasted_iota(jnp.int32, (8, 128), 0)
    piece = jnp.zeros((8, 128), F32)
    for c in range(4):
        line = jnp.sum(jnp.where(lane == row32 + (sky % 4) * SPAN, answer[c], 0.0), axis=0, keepdims=True)
        piece = jnp.where(row8 == c, line, piece)
    piece_ref[...] = piece
    copies = [send(piece_ref, pieces_ref.at[sky], sent.at[1 + d], landed.at[1 + d], peers[d - 1])
              for d in range(1, OWNERS)]
    pieces_ref[sky] = piece

    @pl.when(has_after)
    def _():
        backward(after).wait_recv()

    fix = None
    for m in range(4):
        for c in range(4):
            both = jnp.concatenate([answer[c], next_ref[c]], axis=0)
            value = both[m:m + SPAN]
            high = value.astype(BF16)
            rest = value - high.astype(F32)
            middle = rest.astype(BF16)
            low = (rest - middle.astype(F32)).astype(BF16)
            table = jnp.concatenate([high, middle, low, jnp.zeros_like(high)], axis=0)
            term = att_ref[4 * m + c] * jnp.dot(hits_ref[...], table, preferred_element_type=F32)
            fix = term if fix is None else fix + term
    out_ref[...] = settled_ref[...] - fix
    for copy in copies:
        copy.wait()
    for j in range(4):
        total = pieces_ref[4 * j]
        for i in range(1, 4):
            total = total + pieces_ref[4 * j + i]
        attitude_ref[:, j * 128:(j + 1) * 128] = total[:4]

    @pl.when(has_after)
    def _():
        onward(after).wait_send()

    @pl.when(has_before)
    def _():
        backward(before).wait_send()


def apply_updates(pix, where, first, normals, tiles, knots, weight, attitude, quad, hits):
    return pl.pallas_call(
        apply_kernel,
        out_shape=(
            jax.ShapeDtypeStruct((TILES, 128), F32),
            jax.ShapeDtypeStruct((4, SPAN * OWNERS), F32),
            jax.ShapeDtypeStruct((PIX * 5 + 8, 128), F32),
        ),
        in_specs=[SMEM, SMEM, SMEM, HBM, HBM, VMEM, VMEM, HBM, VMEM, VMEM],
        out_specs=(VMEM, VMEM, VMEM),
        scratch_shapes=[
            pltpu.VMEM((PIX * 5 + 8, 128), F32),
            pltpu.VMEM((PIX * TERMS, 128), F32),
            pltpu.VMEM((TIMES - 1, HROWS, 128), F32),
            pltpu.VMEM((HROWS, 128), F32),
            pltpu.VMEM((HALF * 5, 128), F32),
            pltpu.VMEM((SLOTS * ROOM, 128), F32),
            pltpu.VMEM((SLOTS * SEATS, 128), F32),
            pltpu.VMEM((SLOTS * SEATS, 128), F32),
            pltpu.VMEM((16, TILES, 128), F32),
            pltpu.VMEM((TILES, 128), F32),
            pltpu.VMEM((2, 8, 128), F32),
            pltpu.VMEM((4, 8, 128), F32),
            pltpu.VMEM((4, 8, 128), F32),
            pltpu.VMEM((8, 128), F32),
            pltpu.VMEM((OWNERS, 8, 128), F32),
            pltpu.SemaphoreType.DMA((OWNERS + 1,)),
            pltpu.SemaphoreType.DMA((OWNERS + 1,)),
            pltpu.SemaphoreType.DMA((10,)),
            pltpu.SemaphoreType.DMA((SLOTS,)),
            pltpu.SemaphoreType.DMA((SLOTS,)),
            pltpu.SemaphoreType.DMA((TIMES - 1,)),
            pltpu.SemaphoreType.DMA((TIMES - 1,)),
            pltpu.SemaphoreType.DMA((2 * TIMES,)),
            pltpu.SemaphoreType.DMA((2 * TIMES,)),
        ],
        compiler_params=params(collective_id=4, has_side_effects=True),
        name="apply_updates",
    )(pix, where, first, normals, tiles, knots, weight, attitude, quad, hits)


def emit_kernel(final_ref, attitude_ref, table_ref, final_out, attitude_out, update_out):
    final_out[...] = final_ref[...]
    attitude_out[...] = attitude_ref[...]
    for p in range(PIX):
        update_out[:, p * 128:(p + 1) * 128] = table_ref[p * 5:p * 5 + 5, :]


def emit(final, attitude, table):
    return pl.pallas_call(
        emit_kernel,
        out_shape=(
            jax.ShapeDtypeStruct((TILES, 128), F32),
            jax.ShapeDtypeStruct((4, SPAN * OWNERS), F32),
            jax.ShapeDtypeStruct((5, PIX * SRC), F32),
        ),
        in_specs=[VMEM, VMEM, VMEM],
        out_specs=(VMEM, VMEM, VMEM),
        compiler_params=params(),
        name="emit",
    )(final, attitude, table)


def body(residual, obs_weight, source_partials, attitude_partials, source_index,
         tile_pixel, tile_knot, pixel_slot):
    block = lax.axis_index("tm") * OWNERS + lax.axis_index("sky")
    first = (block * SPAN).reshape(1)
    knots = tile_knot.reshape(1, TILES)
    packed, where = pack(tile_pixel, pixel_slot, residual, obs_weight, source_partials, source_index)
    arrived, normals, pix, quad, hits = gather_tiles(packed, attitude_partials, obs_weight, knots, first)
    final, attitude_update, table = apply_updates(
        pix, where, first, normals, arrived, knots, obs_weight, attitude_partials, quad, hits)
    final, attitude_update, source_update = emit(final, attitude_update, table)
    return final, source_update, attitude_update


def solution(mesh):
    in_specs = (
        P(("tm", "sky"), None),
        P(("tm", "sky"), None),
        P(None, ("tm", "sky"), None),
        P(None, ("tm", "sky"), None),
        P(("tm", "sky"), None),
        P(("tm", "sky")),
        P(("tm", "sky")),
        P(),
    )
    out_specs = (P(("tm", "sky"), None), P(None, "sky"), P(None, "tm"))
    return jax.shard_map(body, mesh=mesh, in_specs=in_specs, out_specs=out_specs, check_vma=False)
```

```python
import functools

import jax
import jax.numpy as jnp
from jax import lax
from jax.experimental import pallas as pl
from jax.experimental.pallas import tpu as pltpu
from jax.sharding import PartitionSpec as P

TILES = 512
OWNERS = 16
TIMES = 8
CAP = 96
PIX = 128
SRC = 128
FIELDS = 7
CLASSES = 2
SEATS = CAP // CLASSES
SLOTS = OWNERS * CLASSES
BLOCK_ROWS = SEATS * FIELDS
ROWS_IN = SLOTS * BLOCK_ROWS + 8
SPAN = 32
TERMS = 20
HALF = PIX // TIMES
HROWS = HALF * TERMS
KNOT_PAIRS = tuple((c, e) for c in range(4) for e in range(c, 4))
TERM_ROW = {
    (0, 0): 0, (1, 1): 1, (2, 2): 2, (3, 3): 3, (4, 4): 4, (0, 5): 5,
    (0, 1): 6, (1, 2): 7, (2, 3): 8, (3, 4): 9, (4, 5): 10, (0, 4): 11, (1, 5): 12,
    (0, 2): 13, (1, 3): 14, (2, 4): 15, (3, 5): 16, (0, 3): 17, (1, 4): 18, (2, 5): 19,
}
VMEM = pl.BlockSpec(memory_space=pltpu.VMEM)
SMEM = pl.BlockSpec(memory_space=pltpu.SMEM)
F32 = jnp.float32
BF16 = jnp.bfloat16


def params(**kw):
    return pltpu.CompilerParams(vmem_limit_bytes=60 * 1024 * 1024, **kw)


def pack_kernel(pixel_ref, slot_ref, res_ref, w_ref, part_ref, idx_ref,
                out_ref, where_ref, count_ref, stage_ref):
    for o in range(OWNERS):
        count_ref[o] = 0
    nothing = jnp.zeros((SEATS, 128), F32)

    def clear(b, _):
        base = pl.multiple_of(b * BLOCK_ROWS, 8)
        for i in range(FIELDS):
            out_ref[pl.ds(base + i * SEATS, SEATS), :] = nothing
        out_ref[pl.ds(base + 6, SEATS, stride=FIELDS), :] = nothing - 1.0
        return 0

    lax.fori_loop(0, SLOTS, clear, 0)

    def scale(g, _):
        rows = pl.ds(pl.multiple_of(g * 8, 8), 8)
        root = jnp.sqrt(w_ref[rows, :])
        for a in range(5):
            stage_ref[a, rows, :] = part_ref[a, rows, :] * root
        stage_ref[5, rows, :] = res_ref[rows, :] * root
        stage_ref[6, rows, :] = idx_ref[rows, :].astype(F32)
        return 0

    lax.fori_loop(0, TILES // 8, scale, 0, unroll=4)

    def place(g, _):
        for j in range(16):
            t = g * 16 + j
            seat = slot_ref[pixel_ref[t]]
            owner = lax.shift_right_logical(seat, 7)
            rank = count_ref[owner]
            count_ref[owner] = rank + 1
            block = owner * CLASSES + lax.bitwise_and(rank, 1)
            position = lax.shift_right_logical(rank, 1)
            where_ref[t] = block * SEATS + position
            base = block * BLOCK_ROWS + position * FIELDS
            for f in range(6):
                out_ref[pl.ds(base + f, 1), :] = stage_ref[f, pl.ds(t, 1), :]
            first = (lax.bitwise_and(seat, 127) * SRC).astype(F32)
            out_ref[pl.ds(base + 6, 1), :] = stage_ref[6, pl.ds(t, 1), :] + first
        return 0

    lax.fori_loop(0, TILES // 16, place, 0)


def pack(tile_pixel, pixel_slot, residual, weight, partials, index):
    return pl.pallas_call(
        pack_kernel,
        out_shape=(
            jax.ShapeDtypeStruct((ROWS_IN, 128), F32),
            jax.ShapeDtypeStruct((TILES,), jnp.int32),
        ),
        in_specs=[SMEM, SMEM, VMEM, VMEM, VMEM, VMEM],
        out_specs=(VMEM, SMEM),
        scratch_shapes=[pltpu.SMEM((OWNERS,), jnp.int32), pltpu.VMEM((FIELDS, TILES, 128), F32)],
        compiler_params=params(),
        name="pack",
    )(tile_pixel, pixel_slot, residual, weight, partials, index)


def place_of():
    tm, sky = lax.axis_index("tm"), lax.axis_index("sky")
    return tm // 2, tm % 2, sky // 4, (sky // 2) % 2, sky % 2


def device_of(y, zh, x, zl, c):
    return (y * 2 + zh, x * 4 + zl * 2 + c)


def send(src, dst, sent, landed, device):
    copy = pltpu.make_async_remote_copy(
        src_ref=src, dst_ref=dst, send_sem=sent, recv_sem=landed,
        device_id=device, device_id_type=pl.DeviceIdType.MESH)
    copy.start()
    return copy


def greet(devices):
    barrier = pltpu.get_barrier_semaphore()
    for device in devices:
        pl.semaphore_signal(barrier, inc=1, device_id=device, device_id_type=pl.DeviceIdType.MESH)
    pl.semaphore_wait(barrier, len(devices))


def move_of(k):
    rest, near = k // 16, (k // 8 + 1) % 2 * (1 - k // 16)
    d = rest * (1 + k % 2 * 2)
    dz = rest * (1 - k // 2 % 2) + (1 - rest) * (k // 4 % 2)
    dc = rest * (k // 8 % 2) + (1 - rest) * (k // 2 % 2)
    h = rest * (k // 4 % 2) + (1 - rest) * (k % 2)
    return d, dz, dc, h, near


MOVES = [move_of(k) for k in range(SLOTS)]
OWN = (0, 1, 8, 9)
CHUNK = 2
CHUNKS = SLOTS // CHUNK
STEP = 48
PER = SEATS // STEP
PITCH = 136
ROOM = BLOCK_ROWS + 8
HBM = pl.BlockSpec(memory_space=pltpu.HBM)


def routes_of():
    y, zh, x, zl, c = place_of()
    routes = []
    for d, dz, dc, h, pair in MOVES:
        far, zl_to, c_to = (x + d) % 4, (zl + dz) % 2, (c + dc) % 2
        owner = (far + 2 * pair) % 4 * 4 + zl_to * 2 + c_to
        routes.append((owner * CLASSES + h, device_of(y, (zh + dz * h) % 2, far, zl_to, c_to)))
    return routes


def times_of(y, zh):
    return [((y + d) % 4, (zh + z) % 2) for d, z in ((2, 1), (2, 0), (1, 1), (3, 1), (1, 0), (3, 0), (0, 1))]


def pair_products(v, row):
    low5, low4 = row < 5, row < 4
    one = pltpu.roll(v, 1, 0)
    first = jnp.where(low5, v, pltpu.roll(v, 5, 0))
    second = jnp.where(low5, pltpu.roll(v, 7, 0), one)
    third = jnp.where(low4, v, pltpu.roll(v, 4, 0))
    fourth = jnp.where(low4, pltpu.roll(v, 6, 0), one)
    return jnp.concatenate([first * v, first * second, third * fourth], axis=0)


def left_side(v, row):
    products = pair_products(v, row)
    high = products.astype(BF16).astype(F32)
    return jnp.concatenate([high, products - high], axis=0).astype(BF16)


def landing(in_ref, arr_ref, sent, landed, k, to):
    return pltpu.make_async_remote_copy(
        src_ref=in_ref.at[pl.ds(k * BLOCK_ROWS, BLOCK_ROWS)],
        dst_ref=arr_ref.at[pl.ds(k * ROOM, BLOCK_ROWS)], send_sem=sent.at[k], recv_sem=landed.at[k],
        device_id=to, device_id_type=pl.DeviceIdType.MESH)


def gather_kernel(in_ref, att_hbm, w_hbm, knot_ref, first_ref,
                  keep_ref, sums_ref, pix_ref, quad_ref, hits_ref,
                  arr_ref, att_ref, w_ref, spread_ref, parts_ref, pair_ref, across_ref,
                  sent, landed, local, stored, sent1, landed1, sent2, landed2):
    routes = routes_of()
    load_att = pltpu.make_async_copy(att_hbm, att_ref, local.at[4])
    load_w = pltpu.make_async_copy(w_hbm, w_ref, local.at[5])
    load_att.start()
    load_w.start()
    y, zh, x, zl, c = place_of()
    rows_y = [(y + d) % 4 for d in (2, 1, 3)]
    partner = device_of(y, zh, (x + 2) % 4, zl, c)
    shards = [device_of(to_y, zh, x, zl, c) for to_y in rows_y]
    greet([to for k, (_, to) in enumerate(routes) if k not in OWN] + shards + [partner])
    copies = []
    for k, (block, to) in enumerate(routes):
        if k not in OWN:
            copies.append(send(in_ref.at[pl.ds(block * BLOCK_ROWS, BLOCK_ROWS)],
                               arr_ref.at[pl.ds(k * ROOM, BLOCK_ROWS)], sent.at[k], landed.at[k], to))
    kept = []
    for i, k in enumerate(OWN):
        kept.append(pltpu.make_async_copy(in_ref.at[pl.ds(routes[k][0] * BLOCK_ROWS, BLOCK_ROWS)],
                                          arr_ref.at[pl.ds(k * ROOM, BLOCK_ROWS)], local.at[i]))
        kept[-1].start()

    def clear(g, _):
        spread_ref[pl.ds(pl.multiple_of(g * 8, 8), 8), :] = jnp.zeros((8, 128), F32)
        return 0

    lax.fori_loop(0, 24 * PITCH // 8, clear, 0, unroll=4)

    def clear_sums(g, _):
        sums_ref[pl.ds(pl.multiple_of(g * 16, 16), 16), :] = jnp.zeros((16, 128), F32)
        return 0

    lax.fori_loop(0, 2 * PIX * TERMS // 16, clear_sums, 0, unroll=4)
    load_att.wait()
    load_w.wait()
    quad_sums(knot_ref, first_ref, w_ref, att_ref, quad_ref, hits_ref)
    for move in kept:
        move.wait()
    row = lax.broadcasted_iota(jnp.int32, (8, 128), 0)
    sources = lax.broadcasted_iota(jnp.int32, (128, 128), 0).astype(F32)
    pixels = lax.broadcasted_iota(jnp.int32, (SEATS, 128), 1)
    seat_row = lax.broadcasted_iota(jnp.int32, (SEATS, 128), 0)
    blank = jnp.zeros((48, 128), BF16)

    def keep(k):
        return pltpu.make_async_copy(arr_ref.at[pl.ds(k * ROOM, BLOCK_ROWS)],
                                     keep_ref.at[pl.ds(k * ROOM, BLOCK_ROWS)], stored.at[k])

    def part_copy(i):
        return pltpu.make_async_remote_copy(
            src_ref=sums_ref.at[pl.ds(PIX * TERMS + rows_y[i] * 2 * HROWS, 2 * HROWS)], dst_ref=parts_ref.at[i],
            send_sem=sent1.at[i], recv_sem=landed1.at[i], device_id=shards[i], device_id_type=pl.DeviceIdType.MESH)

    def cross():
        return pltpu.make_async_remote_copy(
            src_ref=pair_ref, dst_ref=across_ref, send_sem=sent2.at[0], recv_sem=landed2.at[0],
            device_id=partner, device_id_type=pl.DeviceIdType.MESH)

    def chunk_step(chunk, _):
        pair = 1 - (chunk // 4 + 3) // 4

        @pl.when(chunk == 5)
        def _():
            for i in range(3):
                part_copy(i).start()

        @pl.when(chunk == 11)
        def _():
            for i in range(3):
                part_copy(i).wait()

            def add(g, _):
                at = pl.multiple_of(g * 16, 16)
                total = sums_ref[pl.ds(PIX * TERMS + y * 2 * HROWS + at, 16), :]
                for i in range(3):
                    total = total + parts_ref[i, pl.ds(at, 16), :]
                pair_ref[pl.ds(at, 16), :] = total
                return 0

            lax.fori_loop(0, 2 * TERMS, add, 0)

        @pl.when(chunk == 12)
        def _():
            cross().start()

        for i in range(CHUNK):
            k = chunk * CHUNK + i
            arrival = landing(in_ref, arr_ref, sent, landed, k, routes[2][1])

            @pl.when(jnp.logical_and(chunk != 0, chunk != 4))
            def _():
                arrival.wait_recv()

            keep(k).start()

        def group(g, _):
            for j in range(0, STEP, 2):
                start = (chunk * CHUNK + g // PER) * ROOM + (g % PER * STEP + j) * FIELDS
                lefts, hits = [], []
                for i in range(2):
                    v = arr_ref[pl.ds(start + i * FIELDS, 8), :]
                    within = v - jnp.floor(v * (1.0 / SRC)) * SRC
                    lefts.append(left_side(v, row))
                    hits.append((within[6:7, :] == sources).astype(F32).astype(BF16))
                left = jnp.concatenate([jnp.concatenate([lefts[0], blank], axis=1),
                                        jnp.concatenate([blank, lefts[1]], axis=1)], axis=0)
                out = lax.dot_general(left, jnp.concatenate(hits, axis=1), (((1,), (1,)), ((), ())),
                                      preferred_element_type=F32)
                for i in range(2):
                    both = out[48 * i:48 * i + 24] + out[48 * i + 24:48 * i + 48]
                    for n in range(3):
                        spread_ref[pl.ds(8 * n * PITCH + g * STEP + j + i, 8, stride=PITCH), :] = both[8 * n:8 * n + 8]
            return 0

        lax.fori_loop(0, CHUNK * SEATS // STEP, group, 0)
        places = []
        for i in range(CHUNK):
            k = chunk * CHUNK + i
            whole = arr_ref[pl.ds(k * ROOM + 6, SEATS, stride=FIELDS), :]
            pixel = jnp.floor(whole * (1.0 / SRC)).astype(jnp.int32)
            places.append((pixel == pixels).astype(F32))
            line = jnp.sum(jnp.where(pixels == seat_row, pixel, 0), axis=0, keepdims=True)
            pix_ref[pl.ds(k, 1), :] = jnp.maximum(line, 0)
        places.append(jnp.zeros((128 - CHUNK * SEATS, 128), F32))
        place = jnp.concatenate(places, axis=0).T.astype(BF16)
        place = jnp.concatenate([place, place], axis=1)
        for n in range(TERMS):
            at = n + (2 if n >= 6 else 0) + (1 if n >= 13 else 0)
            value = spread_ref[pl.ds(at * PITCH, 128), :]
            high = value.astype(BF16)
            low = (value - high.astype(F32)).astype(BF16)
            added = jnp.dot(place, jnp.concatenate([high, low], axis=0), preferred_element_type=F32)
            for part in range(TIMES):
                rows = pl.ds(pair * (PIX * TERMS) + part * HROWS + n * HALF, HALF)
                sums_ref[rows, :] = sums_ref[rows, :] + added[part * HALF:(part + 1) * HALF]
        return 0

    lax.fori_loop(0, CHUNKS, chunk_step, 0)
    cross().wait()

    def take(g, _):
        at = pl.multiple_of(g * 16, 16)
        rows = pl.ds(y * 2 * HROWS + at, 16)
        sums_ref[rows, :] = sums_ref[rows, :] + across_ref[pl.ds(at, 16), :]
        return 0

    lax.fori_loop(0, 2 * TERMS, take, 0)
    for copy in copies:
        copy.wait_send()

    def kept_step(k, _):
        keep(k).wait()
        return 0

    lax.fori_loop(0, SLOTS, kept_step, 0)


def gather_tiles(packed, attitude, weight, knots, first):
    return pl.pallas_call(
        gather_kernel,
        out_shape=(
            jax.ShapeDtypeStruct((SLOTS * ROOM, 128), F32),
            jax.ShapeDtypeStruct((2 * PIX * TERMS, 128), F32),
            jax.ShapeDtypeStruct((SLOTS, 128), jnp.int32),
            jax.ShapeDtypeStruct((SPAN, 128), F32),
            jax.ShapeDtypeStruct((TILES, 128), BF16),
        ),
        in_specs=[HBM, HBM, HBM, VMEM, SMEM],
        out_specs=(HBM, VMEM, VMEM, VMEM, VMEM),
        scratch_shapes=[
            pltpu.VMEM((SLOTS * ROOM, 128), F32),
            pltpu.VMEM((16, TILES, 128), F32),
            pltpu.VMEM((TILES, 128), F32),
            pltpu.VMEM((24 * PITCH, 128), F32),
            pltpu.VMEM((3, 2 * HROWS, 128), F32),
            pltpu.VMEM((2 * HROWS, 128), F32),
            pltpu.VMEM((2 * HROWS, 128), F32),
            pltpu.SemaphoreType.DMA((SLOTS,)),
            pltpu.SemaphoreType.DMA((SLOTS,)),
            pltpu.SemaphoreType.DMA((6,)),
            pltpu.SemaphoreType.DMA((SLOTS,)),
            pltpu.SemaphoreType.DMA((3,)),
            pltpu.SemaphoreType.DMA((3,)),
            pltpu.SemaphoreType.DMA((1,)),
            pltpu.SemaphoreType.DMA((1,)),
        ],
        compiler_params=params(collective_id=1, has_side_effects=True),
        name="gather_tiles",
    )(packed, attitude, weight, knots, first)


def damped_solve(entries, target, order):
    factor = {}
    for column in range(order):
        pivot = entries[column, column] + 1.0
        for earlier in range(column):
            pivot = pivot - factor[column, earlier] * factor[column, earlier]
        pivot = jnp.sqrt(pivot)
        factor[column, column] = pivot
        for below in range(column + 1, order):
            current = entries[column, below]
            for earlier in range(column):
                current = current - factor[below, earlier] * factor[column, earlier]
            factor[below, column] = current / pivot
    forward = []
    for column in range(order):
        current = target[column]
        for earlier in range(column):
            current = current - factor[column, earlier] * forward[earlier]
        forward.append(current / factor[column, column])
    answer = [None] * order
    for column in reversed(range(order)):
        current = forward[column]
        for later in range(column + 1, order):
            current = current - factor[later, column] * answer[later]
        answer[column] = current / factor[column, column]
    return answer


def reduce_and_solve(in_ref, table_ref, second_ref, parts_ref, whole_ref, own_ref, peers, devices, opposite, tm,
                     sent1, landed1, sent2, landed2):
    copies = []
    for i, (to_y, to_zh) in enumerate(peers):
        copies.append(send(in_ref.at[pl.ds((to_y * 2 + to_zh) * HROWS, HROWS)], parts_ref.at[i],
                           sent1.at[i], landed1.at[i], devices[i]))
    for copy in copies:
        copy.wait()

    def add(g, _):
        rows = pl.ds(pl.multiple_of(g * 16, 16), 16)
        total = in_ref[pl.ds(tm * HROWS + pl.multiple_of(g * 16, 16), 16), :]
        for i in range(TIMES - 1):
            total = total + parts_ref[i, rows, :]
        whole_ref[rows, :] = total
        return 0

    lax.fori_loop(0, TERMS, add, 0, unroll=4)
    sums = [whole_ref[pl.ds(term * HALF, HALF), :] for term in range(TERMS)]
    entries = {key: sums[at] for key, at in TERM_ROW.items() if key[1] < 5}
    target = [sums[TERM_ROW[a, 5]] for a in range(5)]
    for a, value in enumerate(damped_solve(entries, target, 5)):
        own_ref[pl.ds(a, HALF, stride=5), :] = value
    part = pl.ds(tm * HALF * 5, HALF * 5)
    table_ref[part, :] = own_ref[...]
    copies = [send(own_ref, table_ref.at[part], sent2.at[i], landed2.at[i], device)
              for i, device in enumerate(devices)]

    def spread(i):
        return pltpu.make_async_remote_copy(
            src_ref=own_ref, dst_ref=second_ref.at[part], send_sem=sent2.at[TIMES + i], recv_sem=landed2.at[TIMES + i],
            device_id=opposite[i], device_id_type=pl.DeviceIdType.MESH)

    for i in range(TIMES):
        spread(i).start()
    for copy in copies:
        copy.wait()
    return spread


def knot_hits(knot_row, first):
    lane = lax.broadcasted_iota(jnp.int32, (SPAN, TILES), 0)
    return (lane == knot_row - first).astype(F32)


def split_dot(hits, value):
    high = value.astype(BF16)
    low = (value - high.astype(F32)).astype(BF16)
    return (jnp.dot(hits, high, preferred_element_type=F32)
            + jnp.dot(hits, low, preferred_element_type=F32))


def quad_sums(knot_ref, first_ref, w_ref, att_ref, out_ref, hits_ref):
    hits = knot_hits(knot_ref[...], first_ref[0])
    flipped = hits.T
    hits_ref[...] = jnp.concatenate([flipped] * 3 + [jnp.zeros_like(flipped)], axis=1).astype(BF16)
    hits = hits.astype(BF16)
    lane = lax.broadcasted_iota(jnp.int32, (SPAN, 128), 1)
    total = jnp.zeros((SPAN, 128), F32)
    weight = w_ref[...]
    for m in range(4):
        for c in range(4):
            scaled = weight * att_ref[4 * m + c]
            for e in range(c, 4):
                sums = split_dot(hits, scaled * att_ref[4 * m + e])
                at = 14 * m + KNOT_PAIRS.index((c, e))
                total = total + jnp.where(lane == at, jnp.sum(sums, axis=1, keepdims=True), 0.0)
    out_ref[...] = total


def apply_kernel(pix_ref, where_ref, first_ref, normals_hbm, tiles_hbm, knot_ref, w_ref, att_hbm, quad_ref, hits_ref,
                 out_ref, attitude_ref, table_ref, second_ref, normals_ref, parts_ref, whole_ref, own_ref, arr_ref, fixed_ref, back_ref, att_ref,
                 settled_ref, edge_ref, head_ref, next_ref, piece_ref, pieces_ref,
                 sent, landed, loaded, given, taken, sent1, landed1, sent2, landed2):
    tm, sky = lax.axis_index("tm"), lax.axis_index("sky")
    y, zh, x, zl, c0 = place_of()
    block = tm * OWNERS + sky
    after = ((block + 1) // OWNERS % TIMES, (block + 1) % OWNERS)
    before = ((block + 127) // OWNERS % TIMES, (block + 127) % OWNERS)
    has_after, has_before = block < TIMES * OWNERS - 1, block > 0
    peers = [(tm, (sky + d) % OWNERS) for d in range(1, OWNERS)]
    parts = 8
    size = SLOTS // parts * ROOM

    def load(part):
        rows = pl.ds(part * size, size)
        return pltpu.make_async_copy(tiles_hbm.at[rows], arr_ref.at[rows], loaded.at[part])

    load_sums = pltpu.make_async_copy(normals_hbm.at[pl.ds(0, PIX * TERMS)], normals_ref, loaded.at[parts + 1])
    load_sums.start()
    for part in range(parts):
        load((part + 2) % parts).start()
    load_att = pltpu.make_async_copy(att_hbm, att_ref, loaded.at[parts])
    load_att.start()
    edge_ref[1] = jnp.zeros((8, 128), F32)
    next_ref[...] = jnp.zeros((4, 8, 128), F32)
    times = times_of(y, zh)
    others = times + [(y, zh)]
    opposite = [device_of(to_y, to_zh, (x + 2) % 4, zl, c0) for to_y, to_zh in others]
    shards = [device_of(to_y, to_zh, x, zl, c0) for to_y, to_zh in times]
    greet(shards + opposite + peers + [after, before] + [to for k, (_, to) in enumerate(routes_of()) if k not in OWN])
    load_sums.wait()
    spread = reduce_and_solve(normals_ref, table_ref, second_ref, parts_ref, whole_ref, own_ref, times, shards, opposite, tm,
                              sent1, landed1, sent2, landed2)

    def give(k):
        d, dz, dc, h, pair = move_of(k)
        to = device_of(y, (zh + dz * h) % 2, (x + 4 - d) % 4, (zl + dz) % 2, (c0 + dc) % 2)
        seat = ((x + 2 * pair) % 4 * 4 + zl * 2 + c0) * CLASSES + h
        return pltpu.make_async_remote_copy(
            src_ref=fixed_ref.at[pl.ds(k * SEATS, SEATS)], dst_ref=back_ref.at[pl.ds(seat * SEATS, SEATS)],
            send_sem=given.at[k], recv_sem=taken.at[k], device_id=to, device_id_type=pl.DeviceIdType.MESH), seat

    def is_own(k):
        return jnp.logical_and(k < 16, k % 8 < 2)

    def pass_on(k):
        copy, seat = give(k)

        @pl.when(jnp.logical_not(is_own(k)))
        def _():
            copy.start()

        @pl.when(is_own(k))
        def _():
            back_ref[pl.ds(seat * SEATS, SEATS), :] = fixed_ref[pl.ds(k * SEATS, SEATS), :]

    row = lax.broadcasted_iota(jnp.int32, (8, 128), 0)

    def pick(rows_ref, step, _):
        k, first = (step // PER + 8) % SLOTS, step % PER * STEP

        @pl.when(step % (PER * SLOTS // parts) == 0)
        def _():
            load(k // (SLOTS // parts)).wait()

        for j in range(STEP):
            v = arr_ref[pl.ds(k * ROOM + (first + j) * FIELDS, 8), :]
            table = rows_ref[pl.ds(pix_ref[k, first + j] * 5, 8), :]
            within = (v - jnp.floor(v * (1.0 / SRC)) * SRC).astype(jnp.int32)
            at = jnp.broadcast_to(lax.bitwise_and(within[6:7, :], 127), (8, 128))
            picked = jnp.take_along_axis(table, at, axis=1)
            terms = jnp.where(row < 5, v * picked, jnp.where(row == 5, -v, 0.0))
            fixed_ref[pl.ds(k * SEATS + first + j, 1), :] = -jnp.sum(terms, axis=0, keepdims=True)

        @pl.when(jnp.logical_and(first == 0, step > 0))
        def _():
            pass_on((k + SLOTS - 1) % SLOTS)

        return 0

    lax.fori_loop(0, PER * (SLOTS - 8), functools.partial(pick, table_ref), 0)
    for i in range(TIMES):
        spread(i).wait()
    lax.fori_loop(PER * (SLOTS - 8), PER * SLOTS, functools.partial(pick, second_ref), 0)
    pass_on(7)
    load_att.wait()

    def settle(k, _):
        @pl.when(jnp.logical_not(is_own(k)))
        def _():
            give(k)[0].wait()

        return 0

    lax.fori_loop(0, SLOTS, settle, 0)

    def fetch(g, _):
        for j in range(16):
            t = g * 16 + j
            settled_ref[pl.ds(t, 1), :] = back_ref[pl.ds(where_ref[t], 1), :]
        return 0

    lax.fori_loop(0, TILES // 16, fetch, 0)
    weight = w_ref[...]
    settled = settled_ref[...] / jnp.sqrt(weight)
    settled_ref[...] = settled
    hits = knot_hits(knot_ref[...], first_ref[0]).astype(BF16)
    lane = lax.broadcasted_iota(jnp.int32, (SPAN, 128), 1)
    total = quad_ref[...]
    scaled = weight * settled
    for m in range(4):
        for c in range(4):
            sums = split_dot(hits, scaled * att_ref[4 * m + c])
            at = 14 * m + 10 + c
            total = total + jnp.where(lane == at, jnp.sum(sums, axis=1, keepdims=True), 0.0)
    lane40 = lax.broadcasted_iota(jnp.int32, (SPAN + 8, 128), 1)
    padded = jnp.concatenate([total, jnp.zeros((8, 128), F32)], axis=0)
    moved = jnp.where(lane40 < 14, padded, 0.0)
    for m in range(1, 4):
        shifted = pltpu.roll(pltpu.roll(padded, m, 0), 128 - 14 * m, 1)
        moved = moved + jnp.where(lane40 < 14, shifted, 0.0)
    edge_ref[0] = moved[SPAN:]
    def onward(to):
        return pltpu.make_async_remote_copy(
            src_ref=edge_ref.at[0], dst_ref=edge_ref.at[1], send_sem=sent.at[0], recv_sem=landed.at[0],
            device_id=to, device_id_type=pl.DeviceIdType.MESH)

    def backward(to):
        return pltpu.make_async_remote_copy(
            src_ref=head_ref, dst_ref=next_ref, send_sem=sent.at[1], recv_sem=landed.at[1],
            device_id=to, device_id_type=pl.DeviceIdType.MESH)

    @pl.when(has_after)
    def _():
        onward(after).start()

    @pl.when(has_before)
    def _():
        onward(before).wait_recv()

    sums = jnp.concatenate([moved[:8] + edge_ref[1], moved[8:SPAN]], axis=0)

    def column(at):
        return jnp.broadcast_to(sums[:, at:at + 1], (SPAN, 128))

    entries = {pair: column(n) for n, pair in enumerate(KNOT_PAIRS)}
    answer = damped_solve(entries, [column(10 + c) for c in range(4)], 4)
    for c in range(4):
        head_ref[c] = answer[c][:8]

    @pl.when(has_before)
    def _():
        backward(before).start()

    row32 = lax.broadcasted_iota(jnp.int32, (SPAN, 128), 0)
    row8 = lax.broadcasted_iota(jnp.int32, (8, 128), 0)
    piece = jnp.zeros((8, 128), F32)
    for c in range(4):
        line = jnp.sum(jnp.where(lane == row32 + (sky % 4) * SPAN, answer[c], 0.0), axis=0, keepdims=True)
        piece = jnp.where(row8 == c, line, piece)
    piece_ref[...] = piece
    copies = [send(piece_ref, pieces_ref.at[sky], sent.at[1 + d], landed.at[1 + d], peers[d - 1])
              for d in range(1, OWNERS)]
    pieces_ref[sky] = piece

    @pl.when(has_after)
    def _():
        backward(after).wait_recv()

    fix = None
    for m in range(4):
        for c in range(4):
            both = jnp.concatenate([answer[c], next_ref[c]], axis=0)
            value = both[m:m + SPAN]
            high = value.astype(BF16)
            rest = value - high.astype(F32)
            middle = rest.astype(BF16)
            low = (rest - middle.astype(F32)).astype(BF16)
            table = jnp.concatenate([high, middle, low, jnp.zeros_like(high)], axis=0)
            term = att_ref[4 * m + c] * jnp.dot(hits_ref[...], table, preferred_element_type=F32)
            fix = term if fix is None else fix + term
    out_ref[...] = settled_ref[...] - fix
    for copy in copies:
        copy.wait()
    for j in range(4):
        total = pieces_ref[4 * j]
        for i in range(1, 4):
            total = total + pieces_ref[4 * j + i]
        attitude_ref[:, j * 128:(j + 1) * 128] = total[:4]

    @pl.when(has_after)
    def _():
        onward(after).wait_send()

    @pl.when(has_before)
    def _():
        backward(before).wait_send()


def apply_updates(pix, where, first, normals, tiles, knots, weight, attitude, quad, hits):
    return pl.pallas_call(
        apply_kernel,
        out_shape=(
            jax.ShapeDtypeStruct((TILES, 128), F32),
            jax.ShapeDtypeStruct((4, SPAN * OWNERS), F32),
            jax.ShapeDtypeStruct((PIX * 5 + 8, 128), F32),
        ),
        in_specs=[SMEM, SMEM, SMEM, HBM, HBM, VMEM, VMEM, HBM, VMEM, VMEM],
        out_specs=(VMEM, VMEM, VMEM),
        scratch_shapes=[
            pltpu.VMEM((PIX * 5 + 8, 128), F32),
            pltpu.VMEM((PIX * TERMS, 128), F32),
            pltpu.VMEM((TIMES - 1, HROWS, 128), F32),
            pltpu.VMEM((HROWS, 128), F32),
            pltpu.VMEM((HALF * 5, 128), F32),
            pltpu.VMEM((SLOTS * ROOM, 128), F32),
            pltpu.VMEM((SLOTS * SEATS, 128), F32),
            pltpu.VMEM((SLOTS * SEATS, 128), F32),
            pltpu.VMEM((16, TILES, 128), F32),
            pltpu.VMEM((TILES, 128), F32),
            pltpu.VMEM((2, 8, 128), F32),
            pltpu.VMEM((4, 8, 128), F32),
            pltpu.VMEM((4, 8, 128), F32),
            pltpu.VMEM((8, 128), F32),
            pltpu.VMEM((OWNERS, 8, 128), F32),
            pltpu.SemaphoreType.DMA((OWNERS + 1,)),
            pltpu.SemaphoreType.DMA((OWNERS + 1,)),
            pltpu.SemaphoreType.DMA((10,)),
            pltpu.SemaphoreType.DMA((SLOTS,)),
            pltpu.SemaphoreType.DMA((SLOTS,)),
            pltpu.SemaphoreType.DMA((TIMES - 1,)),
            pltpu.SemaphoreType.DMA((TIMES - 1,)),
            pltpu.SemaphoreType.DMA((2 * TIMES,)),
            pltpu.SemaphoreType.DMA((2 * TIMES,)),
        ],
        compiler_params=params(collective_id=4, has_side_effects=True),
        name="apply_updates",
    )(pix, where, first, normals, tiles, knots, weight, attitude, quad, hits)


def emit_kernel(final_ref, attitude_ref, table_ref, final_out, attitude_out, update_out):
    final_out[...] = final_ref[...]
    attitude_out[...] = attitude_ref[...]
    for p in range(PIX):
        update_out[:, p * 128:(p + 1) * 128] = table_ref[p * 5:p * 5 + 5, :]


def emit(final, attitude, table):
    return pl.pallas_call(
        emit_kernel,
        out_shape=(
            jax.ShapeDtypeStruct((TILES, 128), F32),
            jax.ShapeDtypeStruct((4, SPAN * OWNERS), F32),
            jax.ShapeDtypeStruct((5, PIX * SRC), F32),
        ),
        in_specs=[VMEM, VMEM, VMEM],
        out_specs=(VMEM, VMEM, VMEM),
        compiler_params=params(),
        name="emit",
    )(final, attitude, table)


def body(residual, obs_weight, source_partials, attitude_partials, source_index,
         tile_pixel, tile_knot, pixel_slot):
    block = lax.axis_index("tm") * OWNERS + lax.axis_index("sky")
    first = (block * SPAN).reshape(1)
    knots = tile_knot.reshape(1, TILES)
    packed, where = pack(tile_pixel, pixel_slot, residual, obs_weight, source_partials, source_index)
    arrived, normals, pix, quad, hits = gather_tiles(packed, attitude_partials, obs_weight, knots, first)
    final, attitude_update, table = apply_updates(
        pix, where, first, normals, arrived, knots, obs_weight, attitude_partials, quad, hits)
    final, attitude_update, source_update = emit(final, attitude_update, table)
    return final, source_update, attitude_update


def solution(mesh):
    in_specs = (
        P(("tm", "sky"), None),
        P(("tm", "sky"), None),
        P(None, ("tm", "sky"), None),
        P(None, ("tm", "sky"), None),
        P(("tm", "sky"), None),
        P(("tm", "sky")),
        P(("tm", "sky")),
        P(),
    )
    out_specs = (P(("tm", "sky"), None), P(None, "sky"), P(None, "tm"))
    return jax.shard_map(body, mesh=mesh, in_specs=in_specs, out_specs=out_specs, check_vma=False)
```

```python
import functools

import jax
import jax.numpy as jnp
from jax import lax
from jax.experimental import pallas as pl
from jax.experimental.pallas import tpu as pltpu
from jax.sharding import PartitionSpec as P

TILES = 512
OWNERS = 16
TIMES = 8
CAP = 96
PIX = 128
SRC = 128
FIELDS = 7
CLASSES = 2
SEATS = CAP // CLASSES
SLOTS = OWNERS * CLASSES
BLOCK_ROWS = SEATS * FIELDS
ROWS_IN = SLOTS * BLOCK_ROWS + 8
SPAN = 32
TERMS = 20
HALF = PIX // TIMES
HROWS = HALF * TERMS
KNOT_PAIRS = tuple((c, e) for c in range(4) for e in range(c, 4))
TERM_ROW = {
    (0, 0): 0, (1, 1): 1, (2, 2): 2, (3, 3): 3, (4, 4): 4, (0, 5): 5,
    (0, 1): 6, (1, 2): 7, (2, 3): 8, (3, 4): 9, (4, 5): 10, (0, 4): 11, (1, 5): 12,
    (0, 2): 13, (1, 3): 14, (2, 4): 15, (3, 5): 16, (0, 3): 17, (1, 4): 18, (2, 5): 19,
}
VMEM = pl.BlockSpec(memory_space=pltpu.VMEM)
SMEM = pl.BlockSpec(memory_space=pltpu.SMEM)
F32 = jnp.float32
BF16 = jnp.bfloat16


def params(**kw):
    return pltpu.CompilerParams(vmem_limit_bytes=60 * 1024 * 1024, **kw)


def pack_kernel(pixel_ref, slot_ref, res_ref, w_ref, part_ref, idx_ref,
                out_ref, where_ref, count_ref, stage_ref):
    for o in range(OWNERS):
        count_ref[o] = 0
    nothing = jnp.zeros((SEATS, 128), F32)

    def clear(b, _):
        base = pl.multiple_of(b * BLOCK_ROWS, 8)
        for i in range(FIELDS):
            out_ref[pl.ds(base + i * SEATS, SEATS), :] = nothing
        out_ref[pl.ds(base + 6, SEATS, stride=FIELDS), :] = nothing - 1.0
        return 0

    lax.fori_loop(0, SLOTS, clear, 0)

    def scale(g, _):
        rows = pl.ds(pl.multiple_of(g * 8, 8), 8)
        root = jnp.sqrt(w_ref[rows, :])
        for a in range(5):
            stage_ref[a, rows, :] = part_ref[a, rows, :] * root
        stage_ref[5, rows, :] = res_ref[rows, :] * root
        stage_ref[6, rows, :] = idx_ref[rows, :].astype(F32)
        return 0

    lax.fori_loop(0, TILES // 8, scale, 0, unroll=4)

    def place(g, _):
        for j in range(16):
            t = g * 16 + j
            seat = slot_ref[pixel_ref[t]]
            owner = lax.shift_right_logical(seat, 7)
            rank = count_ref[owner]
            count_ref[owner] = rank + 1
            block = owner * CLASSES + lax.bitwise_and(rank, 1)
            position = lax.shift_right_logical(rank, 1)
            where_ref[t] = block * SEATS + position
            base = block * BLOCK_ROWS + position * FIELDS
            for f in range(6):
                out_ref[pl.ds(base + f, 1), :] = stage_ref[f, pl.ds(t, 1), :]
            first = (lax.bitwise_and(seat, 127) * SRC).astype(F32)
            out_ref[pl.ds(base + 6, 1), :] = stage_ref[6, pl.ds(t, 1), :] + first
        return 0

    lax.fori_loop(0, TILES // 16, place, 0)


def pack(tile_pixel, pixel_slot, residual, weight, partials, index):
    return pl.pallas_call(
        pack_kernel,
        out_shape=(
            jax.ShapeDtypeStruct((ROWS_IN, 128), F32),
            jax.ShapeDtypeStruct((TILES,), jnp.int32),
        ),
        in_specs=[SMEM, SMEM, VMEM, VMEM, VMEM, VMEM],
        out_specs=(VMEM, SMEM),
        scratch_shapes=[pltpu.SMEM((OWNERS,), jnp.int32), pltpu.VMEM((FIELDS, TILES, 128), F32)],
        compiler_params=params(),
        name="pack",
    )(tile_pixel, pixel_slot, residual, weight, partials, index)


def place_of():
    tm, sky = lax.axis_index("tm"), lax.axis_index("sky")
    return tm // 2, tm % 2, sky // 4, (sky // 2) % 2, sky % 2


def device_of(y, zh, x, zl, c):
    return (y * 2 + zh, x * 4 + zl * 2 + c)


def send(src, dst, sent, landed, device):
    copy = pltpu.make_async_remote_copy(
        src_ref=src, dst_ref=dst, send_sem=sent, recv_sem=landed,
        device_id=device, device_id_type=pl.DeviceIdType.MESH)
    copy.start()
    return copy


def greet(devices):
    barrier = pltpu.get_barrier_semaphore()
    for device in devices:
        pl.semaphore_signal(barrier, inc=1, device_id=device, device_id_type=pl.DeviceIdType.MESH)
    pl.semaphore_wait(barrier, len(devices))


def move_of(k):
    rest, near = k // 16, (k // 8 + 1) % 2 * (1 - k // 16)
    d = rest * (1 + k % 2 * 2)
    dz = rest * (1 - k // 2 % 2) + (1 - rest) * (k // 4 % 2)
    dc = rest * (k // 8 % 2) + (1 - rest) * (k // 2 % 2)
    h = rest * (k // 4 % 2) + (1 - rest) * (k % 2)
    return d, dz, dc, h, near


MOVES = [move_of(k) for k in range(SLOTS)]
OWN = (0, 1, 8, 9)
CHUNK = 2
CHUNKS = SLOTS // CHUNK
STEP = 48
PER = SEATS // STEP
PITCH = 136
ROOM = BLOCK_ROWS + 8
HBM = pl.BlockSpec(memory_space=pltpu.HBM)


def routes_of():
    y, zh, x, zl, c = place_of()
    routes = []
    for d, dz, dc, h, pair in MOVES:
        far, zl_to, c_to = (x + d) % 4, (zl + dz) % 2, (c + dc) % 2
        owner = (far + 2 * pair) % 4 * 4 + zl_to * 2 + c_to
        routes.append((owner * CLASSES + h, device_of(y, (zh + dz * h) % 2, far, zl_to, c_to)))
    return routes


def times_of(y, zh):
    return [((y + d) % 4, (zh + z) % 2) for d, z in ((2, 1), (2, 0), (1, 1), (3, 1), (1, 0), (3, 0), (0, 1))]


def pair_products(v, row):
    low5, low4 = row < 5, row < 4
    one = pltpu.roll(v, 1, 0)
    first = jnp.where(low5, v, pltpu.roll(v, 5, 0))
    second = jnp.where(low5, pltpu.roll(v, 7, 0), one)
    third = jnp.where(low4, v, pltpu.roll(v, 4, 0))
    fourth = jnp.where(low4, pltpu.roll(v, 6, 0), one)
    return jnp.concatenate([first * v, first * second, third * fourth], axis=0)


def left_side(v, row):
    products = pair_products(v, row)
    high = products.astype(BF16).astype(F32)
    return jnp.concatenate([high, products - high], axis=0).astype(BF16)


def landing(in_ref, arr_ref, sent, landed, k, to):
    return pltpu.make_async_remote_copy(
        src_ref=in_ref.at[pl.ds(k * BLOCK_ROWS, BLOCK_ROWS)],
        dst_ref=arr_ref.at[pl.ds(k * ROOM, BLOCK_ROWS)], send_sem=sent.at[k], recv_sem=landed.at[k],
        device_id=to, device_id_type=pl.DeviceIdType.MESH)


def gather_kernel(in_ref, att_hbm, w_hbm, knot_ref, first_ref,
                  keep_ref, sums_ref, pix_ref, quad_ref, hits_ref,
                  arr_ref, att_ref, w_ref, spread_ref, parts_ref, pair_ref, across_ref,
                  sent, landed, local, stored, sent1, landed1, sent2, landed2):
    routes = routes_of()
    load_att = pltpu.make_async_copy(att_hbm, att_ref, local.at[4])
    load_w = pltpu.make_async_copy(w_hbm, w_ref, local.at[5])
    load_att.start()
    load_w.start()
    y, zh, x, zl, c = place_of()
    rows_y = [(y + d) % 4 for d in (2, 1, 3)]
    partner = device_of(y, zh, (x + 2) % 4, zl, c)
    shards = [device_of(to_y, zh, x, zl, c) for to_y in rows_y]
    greet([to for k, (_, to) in enumerate(routes) if k not in OWN] + shards + [partner])
    copies = []
    for k, (block, to) in enumerate(routes):
        if k not in OWN:
            copies.append(send(in_ref.at[pl.ds(block * BLOCK_ROWS, BLOCK_ROWS)],
                               arr_ref.at[pl.ds(k * ROOM, BLOCK_ROWS)], sent.at[k], landed.at[k], to))
    kept = []
    for i, k in enumerate(OWN):
        kept.append(pltpu.make_async_copy(in_ref.at[pl.ds(routes[k][0] * BLOCK_ROWS, BLOCK_ROWS)],
                                          arr_ref.at[pl.ds(k * ROOM, BLOCK_ROWS)], local.at[i]))
        kept[-1].start()

    def clear(g, _):
        spread_ref[pl.ds(pl.multiple_of(g * 8, 8), 8), :] = jnp.zeros((8, 128), F32)
        return 0

    lax.fori_loop(0, 24 * PITCH // 8, clear, 0, unroll=4)

    def clear_sums(g, _):
        sums_ref[pl.ds(pl.multiple_of(g * 16, 16), 16), :] = jnp.zeros((16, 128), F32)
        return 0

    lax.fori_loop(0, 2 * PIX * TERMS // 16, clear_sums, 0, unroll=4)
    load_att.wait()
    load_w.wait()
    quad_sums(knot_ref, first_ref, w_ref, att_ref, quad_ref, hits_ref)
    for move in kept:
        move.wait()
    row = lax.broadcasted_iota(jnp.int32, (8, 128), 0)
    sources = lax.broadcasted_iota(jnp.int32, (128, 128), 0).astype(F32)
    pixels = lax.broadcasted_iota(jnp.int32, (SEATS, 128), 1)
    seat_row = lax.broadcasted_iota(jnp.int32, (SEATS, 128), 0)
    blank = jnp.zeros((48, 128), BF16)

    def keep(k):
        return pltpu.make_async_copy(arr_ref.at[pl.ds(k * ROOM, BLOCK_ROWS)],
                                     keep_ref.at[pl.ds(k * ROOM, BLOCK_ROWS)], stored.at[k])

    def part_copy(i):
        return pltpu.make_async_remote_copy(
            src_ref=sums_ref.at[pl.ds(PIX * TERMS + rows_y[i] * 2 * HROWS, 2 * HROWS)], dst_ref=parts_ref.at[i],
            send_sem=sent1.at[i], recv_sem=landed1.at[i], device_id=shards[i], device_id_type=pl.DeviceIdType.MESH)

    def cross():
        return pltpu.make_async_remote_copy(
            src_ref=pair_ref, dst_ref=across_ref, send_sem=sent2.at[0], recv_sem=landed2.at[0],
            device_id=partner, device_id_type=pl.DeviceIdType.MESH)

    def chunk_step(chunk, _):
        pair = 1 - (chunk // 4 + 3) // 4

        @pl.when(chunk == 5)
        def _():
            for i in range(3):
                part_copy(i).start()

        @pl.when(chunk == 11)
        def _():
            for i in range(3):
                part_copy(i).wait()

            def add(g, _):
                at = pl.multiple_of(g * 16, 16)
                total = sums_ref[pl.ds(PIX * TERMS + y * 2 * HROWS + at, 16), :]
                for i in range(3):
                    total = total + parts_ref[i, pl.ds(at, 16), :]
                pair_ref[pl.ds(at, 16), :] = total
                return 0

            lax.fori_loop(0, 2 * TERMS, add, 0)

        @pl.when(chunk == 12)
        def _():
            cross().start()

        for i in range(CHUNK):
            k = chunk * CHUNK + i
            arrival = landing(in_ref, arr_ref, sent, landed, k, routes[2][1])

            @pl.when(jnp.logical_and(chunk != 0, chunk != 4))
            def _():
                arrival.wait_recv()

            keep(k).start()

        def group(g, _):
            for j in range(0, STEP, 2):
                start = (chunk * CHUNK + g // PER) * ROOM + (g % PER * STEP + j) * FIELDS
                lefts, hits = [], []
                for i in range(2):
                    v = arr_ref[pl.ds(start + i * FIELDS, 8), :]
                    within = v - jnp.floor(v * (1.0 / SRC)) * SRC
                    lefts.append(left_side(v, row))
                    hits.append((within[6:7, :] == sources).astype(F32).astype(BF16))
                left = jnp.concatenate([jnp.concatenate([lefts[0], blank], axis=1),
                                        jnp.concatenate([blank, lefts[1]], axis=1)], axis=0)
                out = lax.dot_general(left, jnp.concatenate(hits, axis=1), (((1,), (1,)), ((), ())),
                                      preferred_element_type=F32)
                for i in range(2):
                    both = out[48 * i:48 * i + 24] + out[48 * i + 24:48 * i + 48]
                    for n in range(3):
                        spread_ref[pl.ds(8 * n * PITCH + g * STEP + j + i, 8, stride=PITCH), :] = both[8 * n:8 * n + 8]
            return 0

        for g in range(CHUNK * SEATS // STEP):
            group(g, 0)
        places = []
        for i in range(CHUNK):
            k = chunk * CHUNK + i
            whole = arr_ref[pl.ds(k * ROOM + 6, SEATS, stride=FIELDS), :]
            pixel = jnp.floor(whole * (1.0 / SRC)).astype(jnp.int32)
            places.append((pixel == pixels).astype(F32))
            line = jnp.sum(jnp.where(pixels == seat_row, pixel, 0), axis=0, keepdims=True)
            pix_ref[pl.ds(k, 1), :] = jnp.maximum(line, 0)
        places.append(jnp.zeros((128 - CHUNK * SEATS, 128), F32))
        place = jnp.concatenate(places, axis=0).T.astype(BF16)
        place = jnp.concatenate([place, place], axis=1)
        for n in range(TERMS):
            at = n + (2 if n >= 6 else 0) + (1 if n >= 13 else 0)
            value = spread_ref[pl.ds(at * PITCH, 128), :]
            high = value.astype(BF16)
            low = (value - high.astype(F32)).astype(BF16)
            added = jnp.dot(place, jnp.concatenate([high, low], axis=0), preferred_element_type=F32)
            for part in range(TIMES):
                rows = pl.ds(pair * (PIX * TERMS) + part * HROWS + n * HALF, HALF)
                sums_ref[rows, :] = sums_ref[rows, :] + added[part * HALF:(part + 1) * HALF]
        return 0

    lax.fori_loop(0, CHUNKS, chunk_step, 0)
    cross().wait()

    def take(g, _):
        at = pl.multiple_of(g * 16, 16)
        rows = pl.ds(y * 2 * HROWS + at, 16)
        sums_ref[rows, :] = sums_ref[rows, :] + across_ref[pl.ds(at, 16), :]
        return 0

    lax.fori_loop(0, 2 * TERMS, take, 0)
    for copy in copies:
        copy.wait_send()

    def kept_step(k, _):
        keep(k).wait()
        return 0

    lax.fori_loop(0, SLOTS, kept_step, 0)


def gather_tiles(packed, attitude, weight, knots, first):
    return pl.pallas_call(
        gather_kernel,
        out_shape=(
            jax.ShapeDtypeStruct((SLOTS * ROOM, 128), F32),
            jax.ShapeDtypeStruct((2 * PIX * TERMS, 128), F32),
            jax.ShapeDtypeStruct((SLOTS, 128), jnp.int32),
            jax.ShapeDtypeStruct((SPAN, 128), F32),
            jax.ShapeDtypeStruct((TILES, 128), BF16),
        ),
        in_specs=[HBM, HBM, HBM, VMEM, SMEM],
        out_specs=(HBM, VMEM, VMEM, VMEM, VMEM),
        scratch_shapes=[
            pltpu.VMEM((SLOTS * ROOM, 128), F32),
            pltpu.VMEM((16, TILES, 128), F32),
            pltpu.VMEM((TILES, 128), F32),
            pltpu.VMEM((24 * PITCH, 128), F32),
            pltpu.VMEM((3, 2 * HROWS, 128), F32),
            pltpu.VMEM((2 * HROWS, 128), F32),
            pltpu.VMEM((2 * HROWS, 128), F32),
            pltpu.SemaphoreType.DMA((SLOTS,)),
            pltpu.SemaphoreType.DMA((SLOTS,)),
            pltpu.SemaphoreType.DMA((6,)),
            pltpu.SemaphoreType.DMA((SLOTS,)),
            pltpu.SemaphoreType.DMA((3,)),
            pltpu.SemaphoreType.DMA((3,)),
            pltpu.SemaphoreType.DMA((1,)),
            pltpu.SemaphoreType.DMA((1,)),
        ],
        compiler_params=params(collective_id=1, has_side_effects=True),
        name="gather_tiles",
    )(packed, attitude, weight, knots, first)


def damped_solve(entries, target, order):
    factor = {}
    for column in range(order):
        pivot = entries[column, column] + 1.0
        for earlier in range(column):
            pivot = pivot - factor[column, earlier] * factor[column, earlier]
        pivot = jnp.sqrt(pivot)
        factor[column, column] = pivot
        for below in range(column + 1, order):
            current = entries[column, below]
            for earlier in range(column):
                current = current - factor[below, earlier] * factor[column, earlier]
            factor[below, column] = current / pivot
    forward = []
    for column in range(order):
        current = target[column]
        for earlier in range(column):
            current = current - factor[column, earlier] * forward[earlier]
        forward.append(current / factor[column, column])
    answer = [None] * order
    for column in reversed(range(order)):
        current = forward[column]
        for later in range(column + 1, order):
            current = current - factor[later, column] * answer[later]
        answer[column] = current / factor[column, column]
    return answer


def reduce_and_solve(in_ref, table_ref, second_ref, parts_ref, whole_ref, own_ref, peers, devices, opposite, tm,
                     sent1, landed1, sent2, landed2):
    copies = []
    for i, (to_y, to_zh) in enumerate(peers):
        copies.append(send(in_ref.at[pl.ds((to_y * 2 + to_zh) * HROWS, HROWS)], parts_ref.at[i],
                           sent1.at[i], landed1.at[i], devices[i]))
    for copy in copies:
        copy.wait()

    def add(g, _):
        rows = pl.ds(pl.multiple_of(g * 16, 16), 16)
        total = in_ref[pl.ds(tm * HROWS + pl.multiple_of(g * 16, 16), 16), :]
        for i in range(TIMES - 1):
            total = total + parts_ref[i, rows, :]
        whole_ref[rows, :] = total
        return 0

    lax.fori_loop(0, TERMS, add, 0, unroll=4)
    sums = [whole_ref[pl.ds(term * HALF, HALF), :] for term in range(TERMS)]
    entries = {key: sums[at] for key, at in TERM_ROW.items() if key[1] < 5}
    target = [sums[TERM_ROW[a, 5]] for a in range(5)]
    for a, value in enumerate(damped_solve(entries, target, 5)):
        own_ref[pl.ds(a, HALF, stride=5), :] = value
    part = pl.ds(tm * HALF * 5, HALF * 5)
    table_ref[part, :] = own_ref[...]
    copies = [send(own_ref, table_ref.at[part], sent2.at[i], landed2.at[i], device)
              for i, device in enumerate(devices)]

    def spread(i):
        return pltpu.make_async_remote_copy(
            src_ref=own_ref, dst_ref=second_ref.at[part], send_sem=sent2.at[TIMES + i], recv_sem=landed2.at[TIMES + i],
            device_id=opposite[i], device_id_type=pl.DeviceIdType.MESH)

    for i in range(TIMES):
        spread(i).start()
    for copy in copies:
        copy.wait()
    return spread


def knot_hits(knot_row, first):
    lane = lax.broadcasted_iota(jnp.int32, (SPAN, TILES), 0)
    return (lane == knot_row - first).astype(F32)


def split_dot(hits, value):
    high = value.astype(BF16)
    low = (value - high.astype(F32)).astype(BF16)
    return (jnp.dot(hits, high, preferred_element_type=F32)
            + jnp.dot(hits, low, preferred_element_type=F32))


def quad_sums(knot_ref, first_ref, w_ref, att_ref, out_ref, hits_ref):
    hits = knot_hits(knot_ref[...], first_ref[0])
    flipped = hits.T
    hits_ref[...] = jnp.concatenate([flipped] * 3 + [jnp.zeros_like(flipped)], axis=1).astype(BF16)
    hits = hits.astype(BF16)
    lane = lax.broadcasted_iota(jnp.int32, (SPAN, 128), 1)
    total = jnp.zeros((SPAN, 128), F32)
    weight = w_ref[...]
    for m in range(4):
        for c in range(4):
            scaled = weight * att_ref[4 * m + c]
            for e in range(c, 4):
                sums = split_dot(hits, scaled * att_ref[4 * m + e])
                at = 14 * m + KNOT_PAIRS.index((c, e))
                total = total + jnp.where(lane == at, jnp.sum(sums, axis=1, keepdims=True), 0.0)
    out_ref[...] = total


def apply_kernel(pix_ref, where_ref, first_ref, normals_hbm, tiles_hbm, knot_ref, w_ref, att_hbm, quad_ref, hits_ref,
                 out_ref, attitude_ref, table_ref, second_ref, normals_ref, parts_ref, whole_ref, own_ref, arr_ref, fixed_ref, back_ref, att_ref,
                 settled_ref, edge_ref, head_ref, next_ref, piece_ref, pieces_ref,
                 sent, landed, loaded, given, taken, sent1, landed1, sent2, landed2):
    tm, sky = lax.axis_index("tm"), lax.axis_index("sky")
    y, zh, x, zl, c0 = place_of()
    block = tm * OWNERS + sky
    after = ((block + 1) // OWNERS % TIMES, (block + 1) % OWNERS)
    before = ((block + 127) // OWNERS % TIMES, (block + 127) % OWNERS)
    has_after, has_before = block < TIMES * OWNERS - 1, block > 0
    peers = [(tm, (sky + d) % OWNERS) for d in range(1, OWNERS)]
    parts = 8
    size = SLOTS // parts * ROOM

    def load(part):
        rows = pl.ds(part * size, size)
        return pltpu.make_async_copy(tiles_hbm.at[rows], arr_ref.at[rows], loaded.at[part])

    load_sums = pltpu.make_async_copy(normals_hbm.at[pl.ds(0, PIX * TERMS)], normals_ref, loaded.at[parts + 1])
    load_sums.start()
    for part in range(parts):
        load((part + 2) % parts).start()
    load_att = pltpu.make_async_copy(att_hbm, att_ref, loaded.at[parts])
    load_att.start()
    edge_ref[1] = jnp.zeros((8, 128), F32)
    next_ref[...] = jnp.zeros((4, 8, 128), F32)
    times = times_of(y, zh)
    others = times + [(y, zh)]
    opposite = [device_of(to_y, to_zh, (x + 2) % 4, zl, c0) for to_y, to_zh in others]
    shards = [device_of(to_y, to_zh, x, zl, c0) for to_y, to_zh in times]
    greet(shards + opposite + peers + [after, before] + [to for k, (_, to) in enumerate(routes_of()) if k not in OWN])
    load_sums.wait()
    spread = reduce_and_solve(normals_ref, table_ref, second_ref, parts_ref, whole_ref, own_ref, times, shards, opposite, tm,
                              sent1, landed1, sent2, landed2)

    def give(k):
        d, dz, dc, h, pair = move_of(k)
        to = device_of(y, (zh + dz * h) % 2, (x + 4 - d) % 4, (zl + dz) % 2, (c0 + dc) % 2)
        seat = ((x + 2 * pair) % 4 * 4 + zl * 2 + c0) * CLASSES + h
        return pltpu.make_async_remote_copy(
            src_ref=fixed_ref.at[pl.ds(k * SEATS, SEATS)], dst_ref=back_ref.at[pl.ds(seat * SEATS, SEATS)],
            send_sem=given.at[k], recv_sem=taken.at[k], device_id=to, device_id_type=pl.DeviceIdType.MESH), seat

    def is_own(k):
        return jnp.logical_and(k < 16, k % 8 < 2)

    def pass_on(k):
        copy, seat = give(k)

        @pl.when(jnp.logical_not(is_own(k)))
        def _():
            copy.start()

        @pl.when(is_own(k))
        def _():
            back_ref[pl.ds(seat * SEATS, SEATS), :] = fixed_ref[pl.ds(k * SEATS, SEATS), :]

    row = lax.broadcasted_iota(jnp.int32, (8, 128), 0)

    def pick(rows_ref, step, _):
        k, first = (step // PER + 8) % SLOTS, step % PER * STEP

        @pl.when(step % (PER * SLOTS // parts) == 0)
        def _():
            load(k // (SLOTS // parts)).wait()

        for j in range(STEP):
            v = arr_ref[pl.ds(k * ROOM + (first + j) * FIELDS, 8), :]
            table = rows_ref[pl.ds(pix_ref[k, first + j] * 5, 8), :]
            within = (v - jnp.floor(v * (1.0 / SRC)) * SRC).astype(jnp.int32)
            at = jnp.broadcast_to(lax.bitwise_and(within[6:7, :], 127), (8, 128))
            picked = jnp.take_along_axis(table, at, axis=1)
            terms = jnp.where(row < 5, v * picked, jnp.where(row == 5, -v, 0.0))
            fixed_ref[pl.ds(k * SEATS + first + j, 1), :] = -jnp.sum(terms, axis=0, keepdims=True)

        @pl.when(jnp.logical_and(first == 0, step > 0))
        def _():
            pass_on((k + SLOTS - 1) % SLOTS)

        return 0

    lax.fori_loop(0, PER * (SLOTS - 8), functools.partial(pick, table_ref), 0)
    for i in range(TIMES):
        spread(i).wait()
    lax.fori_loop(PER * (SLOTS - 8), PER * SLOTS, functools.partial(pick, second_ref), 0)
    pass_on(7)
    load_att.wait()

    def settle(k, _):
        @pl.when(jnp.logical_not(is_own(k)))
        def _():
            give(k)[0].wait()

        return 0

    lax.fori_loop(0, SLOTS, settle, 0)

    def fetch(g, _):
        for j in range(32):
            t = g * 32 + j
            settled_ref[pl.ds(t, 1), :] = back_ref[pl.ds(where_ref[t], 1), :]
        return 0

    lax.fori_loop(0, TILES // 32, fetch, 0)
    weight = w_ref[...]
    settled = settled_ref[...] / jnp.sqrt(weight)
    settled_ref[...] = settled
    hits = knot_hits(knot_ref[...], first_ref[0]).astype(BF16)
    lane = lax.broadcasted_iota(jnp.int32, (SPAN, 128), 1)
    total = quad_ref[...]
    scaled = weight * settled
    for m in range(4):
        for c in range(4):
            sums = split_dot(hits, scaled * att_ref[4 * m + c])
            at = 14 * m + 10 + c
            total = total + jnp.where(lane == at, jnp.sum(sums, axis=1, keepdims=True), 0.0)
    lane40 = lax.broadcasted_iota(jnp.int32, (SPAN + 8, 128), 1)
    padded = jnp.concatenate([total, jnp.zeros((8, 128), F32)], axis=0)
    moved = jnp.where(lane40 < 14, padded, 0.0)
    for m in range(1, 4):
        shifted = pltpu.roll(pltpu.roll(padded, m, 0), 128 - 14 * m, 1)
        moved = moved + jnp.where(lane40 < 14, shifted, 0.0)
    edge_ref[0] = moved[SPAN:]
    def onward(to):
        return pltpu.make_async_remote_copy(
            src_ref=edge_ref.at[0], dst_ref=edge_ref.at[1], send_sem=sent.at[0], recv_sem=landed.at[0],
            device_id=to, device_id_type=pl.DeviceIdType.MESH)

    def backward(to):
        return pltpu.make_async_remote_copy(
            src_ref=head_ref, dst_ref=next_ref, send_sem=sent.at[1], recv_sem=landed.at[1],
            device_id=to, device_id_type=pl.DeviceIdType.MESH)

    @pl.when(has_after)
    def _():
        onward(after).start()

    @pl.when(has_before)
    def _():
        onward(before).wait_recv()

    sums = jnp.concatenate([moved[:8] + edge_ref[1], moved[8:SPAN]], axis=0)

    def column(at):
        return jnp.broadcast_to(sums[:, at:at + 1], (SPAN, 128))

    entries = {pair: column(n) for n, pair in enumerate(KNOT_PAIRS)}
    answer = damped_solve(entries, [column(10 + c) for c in range(4)], 4)
    for c in range(4):
        head_ref[c] = answer[c][:8]

    @pl.when(has_before)
    def _():
        backward(before).start()

    row32 = lax.broadcasted_iota(jnp.int32, (SPAN, 128), 0)
    row8 = lax.broadcasted_iota(jnp.int32, (8, 128), 0)
    piece = jnp.zeros((8, 128), F32)
    for c in range(4):
        line = jnp.sum(jnp.where(lane == row32 + (sky % 4) * SPAN, answer[c], 0.0), axis=0, keepdims=True)
        piece = jnp.where(row8 == c, line, piece)
    piece_ref[...] = piece
    copies = [send(piece_ref, pieces_ref.at[sky], sent.at[1 + d], landed.at[1 + d], peers[d - 1])
              for d in range(1, OWNERS)]
    pieces_ref[sky] = piece

    @pl.when(has_after)
    def _():
        backward(after).wait_recv()

    fix = None
    for m in range(4):
        for c in range(4):
            both = jnp.concatenate([answer[c], next_ref[c]], axis=0)
            value = both[m:m + SPAN]
            high = value.astype(BF16)
            rest = value - high.astype(F32)
            middle = rest.astype(BF16)
            low = (rest - middle.astype(F32)).astype(BF16)
            table = jnp.concatenate([high, middle, low, jnp.zeros_like(high)], axis=0)
            term = att_ref[4 * m + c] * jnp.dot(hits_ref[...], table, preferred_element_type=F32)
            fix = term if fix is None else fix + term
    out_ref[...] = settled_ref[...] - fix
    for copy in copies:
        copy.wait()
    for j in range(4):
        total = pieces_ref[4 * j]
        for i in range(1, 4):
            total = total + pieces_ref[4 * j + i]
        attitude_ref[:, j * 128:(j + 1) * 128] = total[:4]

    @pl.when(has_after)
    def _():
        onward(after).wait_send()

    @pl.when(has_before)
    def _():
        backward(before).wait_send()


def apply_updates(pix, where, first, normals, tiles, knots, weight, attitude, quad, hits):
    return pl.pallas_call(
        apply_kernel,
        out_shape=(
            jax.ShapeDtypeStruct((TILES, 128), F32),
            jax.ShapeDtypeStruct((4, SPAN * OWNERS), F32),
            jax.ShapeDtypeStruct((PIX * 5 + 8, 128), F32),
        ),
        in_specs=[SMEM, SMEM, SMEM, HBM, HBM, VMEM, VMEM, HBM, VMEM, VMEM],
        out_specs=(VMEM, VMEM, VMEM),
        scratch_shapes=[
            pltpu.VMEM((PIX * 5 + 8, 128), F32),
            pltpu.VMEM((PIX * TERMS, 128), F32),
            pltpu.VMEM((TIMES - 1, HROWS, 128), F32),
            pltpu.VMEM((HROWS, 128), F32),
            pltpu.VMEM((HALF * 5, 128), F32),
            pltpu.VMEM((SLOTS * ROOM, 128), F32),
            pltpu.VMEM((SLOTS * SEATS, 128), F32),
            pltpu.VMEM((SLOTS * SEATS, 128), F32),
            pltpu.VMEM((16, TILES, 128), F32),
            pltpu.VMEM((TILES, 128), F32),
            pltpu.VMEM((2, 8, 128), F32),
            pltpu.VMEM((4, 8, 128), F32),
            pltpu.VMEM((4, 8, 128), F32),
            pltpu.VMEM((8, 128), F32),
            pltpu.VMEM((OWNERS, 8, 128), F32),
            pltpu.SemaphoreType.DMA((OWNERS + 1,)),
            pltpu.SemaphoreType.DMA((OWNERS + 1,)),
            pltpu.SemaphoreType.DMA((10,)),
            pltpu.SemaphoreType.DMA((SLOTS,)),
            pltpu.SemaphoreType.DMA((SLOTS,)),
            pltpu.SemaphoreType.DMA((TIMES - 1,)),
            pltpu.SemaphoreType.DMA((TIMES - 1,)),
            pltpu.SemaphoreType.DMA((2 * TIMES,)),
            pltpu.SemaphoreType.DMA((2 * TIMES,)),
        ],
        compiler_params=params(collective_id=4, has_side_effects=True),
        name="apply_updates",
    )(pix, where, first, normals, tiles, knots, weight, attitude, quad, hits)


def emit_kernel(final_ref, attitude_ref, table_ref, final_out, attitude_out, update_out):
    final_out[...] = final_ref[...]
    attitude_out[...] = attitude_ref[...]
    for p in range(PIX):
        update_out[:, p * 128:(p + 1) * 128] = table_ref[p * 5:p * 5 + 5, :]


def emit(final, attitude, table):
    return pl.pallas_call(
        emit_kernel,
        out_shape=(
            jax.ShapeDtypeStruct((TILES, 128), F32),
            jax.ShapeDtypeStruct((4, SPAN * OWNERS), F32),
            jax.ShapeDtypeStruct((5, PIX * SRC), F32),
        ),
        in_specs=[VMEM, VMEM, VMEM],
        out_specs=(VMEM, VMEM, VMEM),
        compiler_params=params(),
        name="emit",
    )(final, attitude, table)


def body(residual, obs_weight, source_partials, attitude_partials, source_index,
         tile_pixel, tile_knot, pixel_slot):
    block = lax.axis_index("tm") * OWNERS + lax.axis_index("sky")
    first = (block * SPAN).reshape(1)
    knots = tile_knot.reshape(1, TILES)
    packed, where = pack(tile_pixel, pixel_slot, residual, obs_weight, source_partials, source_index)
    arrived, normals, pix, quad, hits = gather_tiles(packed, attitude_partials, obs_weight, knots, first)
    final, attitude_update, table = apply_updates(
        pix, where, first, normals, arrived, knots, obs_weight, attitude_partials, quad, hits)
    final, attitude_update, source_update = emit(final, attitude_update, table)
    return final, source_update, attitude_update


def solution(mesh):
    in_specs = (
        P(("tm", "sky"), None),
        P(("tm", "sky"), None),
        P(None, ("tm", "sky"), None),
        P(None, ("tm", "sky"), None),
        P(("tm", "sky"), None),
        P(("tm", "sky")),
        P(("tm", "sky")),
        P(),
    )
    out_specs = (P(("tm", "sky"), None), P(None, "sky"), P(None, "tm"))
    return jax.shard_map(body, mesh=mesh, in_specs=in_specs, out_specs=out_specs, check_vma=False)
```
